128 devices in a mesh: col: 2 (over core), row: 64 (over z, y, x).
Axes of the slice: x: 4, y: 4, z: 4, core: 2. Of those that a mesh axis runs over, the one named last changes fastest.
Arguments:
- inter_mask: int32 [32768, 8192], P('row', 'col')
- user_emb: bfloat16 [32768, 64], P(('row', 'col'))
- item_emb: bfloat16 [8192, 64], P(('col', 'row'))
- triples: int32 [2048, 3], replicated
Outputs:
- output 1: bfloat16 [32768, 64], P(('row', 'col'))
- output 2: bfloat16 [8192, 64], P(('col', 'row'))
- output 3: float32 [], replicated
- output 4: float32 [32768, 64], P(('row', 'col'))
- output 5: float32 [8192, 64], P(('col', 'row'))
All inputs are finite; a program needn't handle non-finite values.
Results may differ from the reference program's by a relative error of at most 0.0191124.
Values are sent between devices in bfloat16 or wider.
A program may use at most 1 GiB of HBM per device.

```python
import jax
import jax.numpy as jnp
from jax import lax

NUM_USERS = 32768
NUM_ITEMS = 8192
EMBED_DIM = 64
BATCH_SIZE = 2048
LAYERS = 3


def setup_inputs(seed: int = 0) -> dict:
    base_key = jax.random.key(seed)
    key_list = jax.random.split(base_key, 10)
    act_user = jax.random.randint(key_list[0], (NUM_USERS,), 1, 5)
    act_item = jax.random.randint(key_list[1], (NUM_ITEMS,), 1, 5)
    draw_vals = jax.random.randint(key_list[2], (NUM_USERS, NUM_ITEMS), 0, 2 * NUM_ITEMS)
    inter_mask = (draw_vals < act_user[:, None] * act_item[None, :] * 10).astype(jnp.int32)
    emb_scale = EMBED_DIM ** -0.25
    mean_user = jax.random.normal(key_list[3], (EMBED_DIM,), jnp.float32)
    mean_item = jax.random.normal(key_list[4], (EMBED_DIM,), jnp.float32)
    noise_user = jax.random.normal(key_list[5], (NUM_USERS, EMBED_DIM), jnp.float32)
    noise_item = jax.random.normal(key_list[6], (NUM_ITEMS, EMBED_DIM), jnp.float32)
    user_emb = ((mean_user[None, :] + noise_user) * emb_scale).astype(jnp.bfloat16)
    item_emb = ((mean_item[None, :] + noise_item) * emb_scale).astype(jnp.bfloat16)
    user_ids = jax.random.randint(key_list[7], (BATCH_SIZE,), 0, NUM_USERS)
    user_ids = user_ids.at[0].set(NUM_USERS - 1).at[1].set(0)
    pos_ids = jax.random.randint(key_list[8], (BATCH_SIZE,), 0, NUM_ITEMS)
    pos_ids = pos_ids.at[0].set(NUM_ITEMS - 1).at[1].set(0)
    neg_ids = jax.random.randint(key_list[9], (BATCH_SIZE,), 0, NUM_ITEMS)
    neg_ids = neg_ids.at[0].set(0).at[1].set(NUM_ITEMS - 1)
    triples = jnp.stack([user_ids, pos_ids, neg_ids], axis=1).astype(jnp.int32)
    return {'inter_mask': inter_mask, 'user_emb': user_emb, 'item_emb': item_emb, 'triples': triples}


def reference(inter_mask, user_emb, item_emb, triples):
    deg_user = jnp.maximum(jnp.sum(inter_mask, axis=1, dtype=jnp.int32), 1)
    deg_item = jnp.maximum(jnp.sum(inter_mask, axis=0, dtype=jnp.int32), 1)
    scale_user = lax.rsqrt(deg_user.astype(jnp.float32))
    scale_item = lax.rsqrt(deg_item.astype(jnp.float32))
    adj_mat = (scale_user[:, None] * inter_mask.astype(jnp.float32) * scale_item[None, :]).astype(jnp.bfloat16)

    def to_users(item_side):
        return jnp.dot(adj_mat, item_side, preferred_element_type=jnp.float32)

    def to_items(user_side):
        return lax.dot_general(adj_mat, user_side, (((0,), (0,)), ((), ())), preferred_element_type=jnp.float32)

    user_cur = user_emb
    item_cur = item_emb
    user_acc = user_emb.astype(jnp.float32)
    item_acc = item_emb.astype(jnp.float32)
    for _ in range(LAYERS):
        user_next = to_users(item_cur).astype(jnp.bfloat16)
        item_next = to_items(user_cur).astype(jnp.bfloat16)
        user_acc = user_acc + user_next.astype(jnp.float32)
        item_acc = item_acc + item_next.astype(jnp.float32)
        user_cur, item_cur = user_next, item_next
    user_out = (user_acc / (LAYERS + 1)).astype(jnp.bfloat16)
    item_out = (item_acc / (LAYERS + 1)).astype(jnp.bfloat16)

    def score_loss(user_table, item_table):
        e_user = jnp.take(user_table, triples[:, 0], axis=0)
        e_pos = jnp.take(item_table, triples[:, 1], axis=0)
        e_neg = jnp.take(item_table, triples[:, 2], axis=0)
        margin = jnp.sum(e_user * e_pos, axis=1) - jnp.sum(e_user * e_neg, axis=1)
        return jnp.mean(jax.nn.softplus(-margin))

    bpr_loss, pullback = jax.vjp(score_loss, user_out.astype(jnp.float32), item_out.astype(jnp.float32))
    grad_user_out, grad_item_out = pullback(jnp.ones_like(bpr_loss))
    src_user = grad_user_out / (LAYERS + 1)
    src_item = grad_item_out / (LAYERS + 1)
    cot_user = src_user.astype(jnp.bfloat16)
    cot_item = src_item.astype(jnp.bfloat16)
    for _ in range(LAYERS - 1):
        new_user = (src_user + to_users(cot_item)).astype(jnp.bfloat16)
        new_item = (src_item + to_items(cot_user)).astype(jnp.bfloat16)
        cot_user, cot_item = new_user, new_item
    grad_user = src_user + to_users(cot_item)
    grad_item = src_item + to_items(cot_user)
    return user_out, item_out, bpr_loss, grad_user, grad_item
```

```python
import jax
import jax.numpy as jnp
from jax import lax
from jax.experimental import pallas as pl
from jax.experimental.pallas import tpu as pltpu
from jax.sharding import PartitionSpec as P

SIDE = 4
STRIDE = (16, 4, 1)
EMB = 64
CHUNK = 256
NCHUNK = 16
LAYERS = 3
STAGES = 2 * LAYERS
RS_ORDER = ((0, 1, 2), (2, 1, 0))
F32 = jnp.float32
BF16 = jnp.bfloat16
NSEM = 480
NT = (((1,), (1,)), ((), ()))
MESH = pl.DeviceIdType.MESH


def block_rows(part, q):
    return slice(32 * part + 16 * (q // 2), 32 * part + 16 * (q // 2) + 16)


def block_lanes(q):
    return slice(128 * (q % 2), 128 * (q % 2) + 128)


def join_blocks(get):
    rows = []
    for part in range(2):
        for half in range(2):
            rows.append(jnp.concatenate([get(part, 2 * half), get(part, 2 * half + 1)], axis=1))
    return jnp.concatenate(rows, axis=0)


def kernel(mask_hbm, user_ref, item_ref, ids_ref,
           fu_ref, fi_ref, loss_ref, gu_ref, gi_ref,
           mask, adj, rowsum, rowsum_in, scale_u, colsum, colsum_in, scale_i,
           ut, up, up_in, u_acc, s_user,
           nat, it, part_sum, q1, q2, r1, r2, r3, i_acc, s_item,
           fin_b, fin_f, nat_f,
           sel, sel_in, w0, w1, w2, in1, in2, in3, rows_all, grad_u, grad_i, prod_u, prod_i,
           mask_sem, send_sem, recv_sem):
    row = lax.axis_index('row')
    col = lax.axis_index('col')
    pos = (row // 16, (row // 4) % 4, row % 4)
    z, y, x = pos
    users = user_ref.shape[0]
    n_batch = ids_ref.shape[1]

    def peer(axis, k):
        return {'row': row + ((pos[axis] + k) % SIDE - pos[axis]) * STRIDE[axis]}

    partner = {'col': 1 - col}

    copies = []
    for j in range(NCHUNK):
        cp = pltpu.make_async_copy(mask_hbm.at[:, pl.ds(j * CHUNK, CHUNK)], mask.at[j], mask_sem.at[j])
        cp.start()
        copies.append(cp)

    barrier = pltpu.get_barrier_semaphore()
    for axis in range(3):
        for k in range(1, SIDE):
            pl.semaphore_signal(barrier, inc=1, device_id=peer(axis, k), device_id_type=MESH)
    pl.semaphore_signal(barrier, inc=1, device_id=partner, device_id_type=MESH)
    pl.semaphore_wait(barrier, 10)

    sent = []

    def send(src, dst, device):
        i = len(sent)
        cp = pltpu.make_async_remote_copy(src_ref=src, dst_ref=dst, send_sem=send_sem.at[i], recv_sem=recv_sem.at[i],
                                          device_id=device, device_id_type=MESH)
        cp.start()
        sent.append(cp)
        return cp

    def send_axis(axis, src, dst):
        return [send(src((pos[axis] + k) % SIDE), dst(k - 1), peer(axis, k)) for k in range(1, SIDE)]

    def arrive(cps):
        for cp in cps:
            cp.wait_recv()

    ut[0, col] = user_ref[...].astype(F32).T.astype(BF16)
    u_first = [send(ut.at[0, col], ut.at[0, col], partner)]
    nat[x] = item_ref[...]
    i_first = send_axis(2, lambda t: nat.at[x], lambda k: nat.at[x])

    rowsum[...] = jnp.zeros_like(rowsum)
    for j in range(NCHUNK):
        copies[j].wait()
        m = mask[j]
        rowsum[...] += m[:, :128] + m[:, 128:]
        s = jnp.sum(m, axis=0, keepdims=True)
        colsum[0, 2 * j:2 * j + 1, :] = s[:, :128]
        colsum[0, 2 * j + 1:2 * j + 2, :] = s[:, 128:]
    rs_cp = [send(rowsum, rowsum_in, partner)]
    cs_cp = send_axis(0, lambda t: colsum.at[0], lambda k: colsum_in.at[0, k])

    arrive(i_first)
    chunk0 = jnp.concatenate([nat[k].astype(F32) for k in range(SIDE)], axis=0).T
    for part in range(2):
        for q in range(SIDE):
            it[0, part, z, y, q] = chunk0[block_rows(part, q), block_lanes(q)].astype(BF16)

    def gather_start(s, axis):
        if axis == 2:
            ref = it.at[s, :, z, y, x]
        elif axis == 0:
            ref = it.at[s, :, z, y]
        else:
            ref = it.at[s, :, :, y]
        return send_axis(axis, lambda t: ref, lambda k: ref)

    ag = gather_start(0, 0)
    arrive(rs_cp)
    deg_u = jnp.maximum(jnp.sum(rowsum[...] + rowsum_in[...], axis=1, keepdims=True), 1)
    scale_u[...] = jnp.broadcast_to(lax.rsqrt(deg_u.astype(F32)), scale_u.shape)
    arrive(cs_cp)
    colsum[1] = colsum[0] + colsum_in[0, 0] + colsum_in[0, 1] + colsum_in[0, 2]
    cs_cp = send_axis(1, lambda t: colsum.at[1], lambda k: colsum_in.at[1, k])
    arrive(ag)
    ag = gather_start(0, 1)
    arrive(cs_cp)
    colsum[2] = colsum[1] + colsum_in[1, 0] + colsum_in[1, 1] + colsum_in[1, 2]
    cs_cp = send_axis(2, lambda t: colsum.at[2], lambda k: colsum_in.at[2, k])
    arrive(cs_cp)
    deg_i = jnp.maximum(colsum[2] + colsum_in[2, 0] + colsum_in[2, 1] + colsum_in[2, 2], 1)
    scale_i[...] = lax.rsqrt(deg_i.astype(F32))
    for j in range(NCHUNK):
        su = scale_u[...]
        m = mask[j].astype(F32)
        adj[j, :, :128] = (su * m[:, :128] * scale_i[2 * j:2 * j + 1, :]).astype(BF16)
        adj[j, :, 128:] = (su * m[:, 128:] * scale_i[2 * j + 1:2 * j + 2, :]).astype(BF16)

    def item_product(s):
        lhs = jnp.concatenate([ut[s, 0], ut[s, 1]], axis=1)

        def body(zz, _):
            for yy in range(SIDE):
                out = jnp.dot(lhs, adj[zz * SIDE + yy], preferred_element_type=F32)
                for part in range(2):
                    for q in range(SIDE):
                        part_sum[s, part, zz, yy, q] = out[block_rows(part, q), block_lanes(q)]
            return 0

        lax.fori_loop(0, SIDE, body, 0)

    def user_product(s):
        def body(zz, acc):
            for yy in range(SIDE):
                lhs = join_blocks(lambda part, q: it[s, part, zz, yy, q])
                acc = acc + lax.dot_general(lhs, adj[zz * SIDE + yy], NT, preferred_element_type=F32)
            return acc

        acc = lax.fori_loop(0, SIDE, body, jnp.zeros((EMB, 2 * users), F32))
        up[s, 0] = acc[:, :users]
        up[s, 1] = acc[:, users:]
        return [send(up.at[s], up_in.at[s], partner)]

    def at(ref, axis, t):
        return ref.at[(slice(None),) * axis + (t,)]

    def scatter_start(s):
        return [send_axis(RS_ORDER[p][0],
                          lambda t, p=p: at(part_sum.at[s, p], RS_ORDER[p][0], t),
                          lambda k, p=p: r1.at[s, p, k]) for p in range(2)]

    def scatter_mid(s, cps):
        out = []
        for p in range(2):
            a0, a1, _ = RS_ORDER[p]
            arrive(cps[p])
            q1[s, p] = at(part_sum.at[s, p], a0, pos[a0])[...] + r1[s, p, 0] + r1[s, p, 1] + r1[s, p, 2]
            rest = [a for a in range(3) if a != a0]
            out.append(send_axis(a1, lambda t, p=p: at(q1.at[s, p], rest.index(a1), t), lambda k, p=p: r2.at[s, p, k]))
        return out

    def scatter_last(s, cps):
        out = []
        for p in range(2):
            a0, a1, a2 = RS_ORDER[p]
            rest = [a for a in range(3) if a != a0]
            arrive(cps[p])
            q2[s, p] = at(q1.at[s, p], rest.index(a1), pos[a1])[...] + r2[s, p, 0] + r2[s, p, 1] + r2[s, p, 2]
            out.append(send_axis(a2, lambda t, p=p: q2.at[s, p, t], lambda k, p=p: r3.at[s, p, k]))
        return out

    def scatter_end(s, cps):
        out = []
        for p in range(2):
            arrive(cps[p])
            out.append(q2[s, p, pos[RS_ORDER[p][2]]] + r3[s, p, 0] + r3[s, p, 1] + r3[s, p, 2])
        return out

    for p in range(2):
        i_acc[p] = it[0, p, z, y, x].astype(F32)
    arrive(u_first)
    for h in range(2):
        u_acc[h] = ut[0, h].astype(F32)

    item_product(0)
    rs = scatter_start(0)
    for s in range(LAYERS):
        if s > 0:
            arrive(ag)
            ag = gather_start(s, 0)
            arrive(ag)
            ag = gather_start(s, 1)
        rs = scatter_mid(s, rs)
        arrive(ag)
        ux = user_product(s)
        rs = scatter_last(s, rs)
        arrive(ux)
        for h in range(2):
            nxt = (up[s, h] + up_in[s, h]).astype(BF16)
            u_acc[h] += nxt.astype(F32)
            if s + 1 < LAYERS:
                ut[s + 1, h] = nxt
        if s + 1 < LAYERS:
            item_product(s + 1)
            rs_next = scatter_start(s + 1)
        new = scatter_end(s, rs)
        for p in range(2):
            nxt = new[p].astype(BF16)
            i_acc[p] += nxt.astype(F32)
            if s + 1 < LAYERS:
                it[s + 1, p, z, y, x] = nxt
        if s + 1 < LAYERS:
            ag = gather_start(s + 1, 2)
            rs = rs_next

    for p in range(2):
        fin_b[p, x] = (i_acc[p] * 0.25).astype(BF16)
    fb = send_axis(2, lambda t: fin_b.at[:, x], lambda k: fin_b.at[:, x])
    for h in range(2):
        ut[LAYERS, h] = (u_acc[h] * 0.25).astype(BF16)
    own_u = ut[LAYERS, col]
    fu_ref[...] = own_u.astype(F32).T.astype(BF16)

    tiles = n_batch // CHUNK
    iota = lax.broadcasted_iota(jnp.int32, (users, CHUNK), 0)

    def put_rows(group, t, picked):
        for r in range(4):
            rt = 4 * group + r
            for l in range(2):
                lt = 2 * t + l
                sel[lt // 8, (lt % 8) // 4, lt % 4, rt // 3, rt % 3] = picked[16 * r:16 * r + 16, 128 * l:128 * l + 128].astype(BF16)

    base_u = (2 * row + col) * users
    for t in range(tiles):
        ids = ids_ref[0:1, t * CHUNK:(t + 1) * CHUNK]
        hot = jnp.where(iota == ids - base_u, 1.0, 0.0).astype(BF16)
        put_rows(0, t, jnp.dot(own_u, hot, preferred_element_type=F32))
    arrive(fb)
    fin_chunk = join_blocks(lambda part, q: fin_b[part, q])
    nat_f[...] = fin_chunk.astype(F32).T
    own = pl.ds(pl.multiple_of(x * EMB, EMB), EMB)
    fi_ref[...] = nat_f[own, :].astype(BF16)
    base_i = (col * NCHUNK + z * SIDE + y) * CHUNK
    iota_i = lax.broadcasted_iota(jnp.int32, (CHUNK, CHUNK), 0)
    for g in range(1, 3):
        for t in range(tiles):
            rel = ids_ref[g:g + 1, t * CHUNK:(t + 1) * CHUNK] - base_i
            rel = jnp.where((rel >= x * EMB) & (rel < x * EMB + EMB), rel, -1)
            hot = jnp.where(iota_i == rel, 1.0, 0.0).astype(BF16)
            put_rows(g, t, jnp.dot(fin_chunk, hot, preferred_element_type=F32))

    sx = [send(sel.at[1 - col], sel_in, partner)]
    arrive(sx)
    w0[...] = sel[col] + sel_in[...]
    ax0, ax2 = (0, 2), (2, 0)
    cps = [send_axis(ax0[p], lambda t, p=p: w0.at[p, t], lambda k, p=p: in1.at[p, k]) for p in range(2)]
    nxt_cps = []
    for p in range(2):
        arrive(cps[p])
        w1[p] = w0[p, pos[ax0[p]]] + in1[p, 0] + in1[p, 1] + in1[p, 2]
        nxt_cps.append(send_axis(1, lambda t, p=p: w1.at[p, t], lambda k, p=p: in2.at[p, k]))
    cps, nxt_cps = nxt_cps, []
    for p in range(2):
        arrive(cps[p])
        w2[p] = w1[p, y] + in2[p, 0] + in2[p, 1] + in2[p, 2]
        nxt_cps.append(send_axis(ax2[p], lambda t, p=p: w2.at[p], lambda k, p=p: in3.at[p, k]))
    cps, nxt_cps = nxt_cps, []
    for p in range(2):
        arrive(cps[p])
        a = pos[ax0[p]]
        rows_all[col, p, a, y] = w2[p] + in3[p, 0] + in3[p, 1] + in3[p, 2]
        ref = rows_all.at[col, p, a, y]
        nxt_cps.append(send_axis(1, lambda t, ref=ref: ref, lambda k, ref=ref: ref))
    cps, nxt_cps = nxt_cps, []
    for p in range(2):
        arrive(cps[p])
        ref = rows_all.at[col, p, pos[ax0[p]]]
        nxt_cps.append(send_axis(ax0[p], lambda t, ref=ref: ref, lambda k, ref=ref: ref))
    for p in range(2):
        arrive(nxt_cps[p])
    arrive([send(rows_all.at[col], rows_all.at[col], partner)])

    total = jnp.zeros((1, 128), F32)
    for lt in range(n_batch // 128):
        def rows_of(group):
            return jnp.concatenate([rows_all[lt // 8, (lt % 8) // 4, lt % 4, rt // 3, rt % 3].astype(F32)
                                    for rt in range(4 * group, 4 * group + 4)], axis=0)
        e_user, e_pos, e_neg = rows_of(0), rows_of(1), rows_of(2)
        margin = jnp.sum(e_user * e_pos, axis=0, keepdims=True) - jnp.sum(e_user * e_neg, axis=0, keepdims=True)
        soft = jnp.maximum(-margin, 0.0) + jnp.log1p(jnp.exp(-jnp.abs(margin)))
        total = total + soft
        coef = -jax.nn.sigmoid(-margin) / n_batch
        lanes = slice(lt * 128, lt * 128 + 128)
        for ref, g in ((grad_u, coef * (e_pos - e_neg)), (grad_i, coef * e_user)):
            hi = g.astype(BF16)
            left = g - hi.astype(F32)
            mid = left.astype(BF16)
            ref[0:EMB, lanes] = hi
            ref[EMB:2 * EMB, lanes] = mid
            ref[2 * EMB:3 * EMB, lanes] = (left - mid.astype(F32)).astype(BF16)
    loss_ref[...] = jnp.sum(total, axis=1, keepdims=True) / n_batch

    iota2 = lax.broadcasted_iota(jnp.int32, (2 * users, CHUNK), 0)
    prod_i[...] = jnp.zeros_like(prod_i)
    prod_u[...] = jnp.zeros_like(prod_u)
    for t in range(tiles):
        cut = slice(t * CHUNK, (t + 1) * CHUNK)
        plus = jnp.where(iota_i == ids_ref[1:2, cut] - base_i, 1.0, 0.0)
        minus = jnp.where(iota_i == ids_ref[2:3, cut] - base_i, 1.0, 0.0)
        prod_i[...] += lax.dot_general(grad_i[:, cut], (plus - minus).astype(BF16), NT, preferred_element_type=F32)
    seed = (prod_i[0:EMB, :] + prod_i[EMB:2 * EMB, :] + prod_i[2 * EMB:3 * EMB, :]) * 0.25
    s0 = LAYERS
    for part in range(2):
        for q in range(SIDE):
            block = seed[block_rows(part, q), block_lanes(q)]
            s_item[part, q] = block
            it[s0, part, z, y, q] = block.astype(BF16)
    ag = gather_start(s0, 0)
    for t in range(tiles):
        cut = slice(t * CHUNK, (t + 1) * CHUNK)
        hot = jnp.where(iota2 == ids_ref[0:1, cut] - row * (2 * users), 1.0, 0.0).astype(BF16)
        prod_u[...] += lax.dot_general(grad_u[:, cut], hot, NT, preferred_element_type=F32)
    seed = (prod_u[0:EMB, :] + prod_u[EMB:2 * EMB, :] + prod_u[2 * EMB:3 * EMB, :]) * 0.25
    for h in range(2):
        s_user[h] = seed[:, h * users:(h + 1) * users]
        ut[s0, h] = seed[:, h * users:(h + 1) * users].astype(BF16)

    item_product(s0)
    rs = scatter_start(s0)
    for s in range(s0, STAGES):
        arrive(ag)
        if s > s0:
            ag = gather_start(s, 0)
            arrive(ag)
        ag = gather_start(s, 1)
        rs = scatter_mid(s, rs)
        arrive(ag)
        ux = user_product(s)
        rs = scatter_last(s, rs)
        arrive(ux)
        if s + 1 < STAGES:
            for h in range(2):
                ut[s + 1, h] = (s_user[h] + (up[s, h] + up_in[s, h])).astype(BF16)
            item_product(s + 1)
            rs_next = scatter_start(s + 1)
        else:
            gu_ref[...] = (s_user[col] + (up[s, col] + up_in[s, col])).T
        new = scatter_end(s, rs)
        for p in range(2):
            nxt = s_item[p, x] + new[p]
            if s + 1 < STAGES:
                it[s + 1, p, z, y, x] = nxt.astype(BF16)
            else:
                fin_f[p, x] = nxt
        if s + 1 < STAGES:
            ag = gather_start(s + 1, 2)
            rs = rs_next
    ff = send_axis(2, lambda t: fin_f.at[:, x], lambda k: fin_f.at[:, x])
    arrive(ff)
    nat_f[...] = join_blocks(lambda part, q: fin_f[part, q]).T
    gi_ref[...] = nat_f[own, :]
    for cp in sent:
        cp.wait_send()


def solution(mesh):
    def local_fn(mask_blk, user_emb, item_emb, triples):
        n_u, n_b = mask_blk.shape[0], triples.shape[0]
        half = n_u // 2
        vm = pltpu.VMEM
        outs = (jax.ShapeDtypeStruct((half, EMB), BF16), jax.ShapeDtypeStruct((EMB, EMB), BF16),
                jax.ShapeDtypeStruct((1, 1), F32), jax.ShapeDtypeStruct((half, EMB), F32),
                jax.ShapeDtypeStruct((EMB, EMB), F32))
        tile = (16, 128)
        S = SIDE
        scratch = [
            vm((NCHUNK, n_u, CHUNK), jnp.int32), vm((NCHUNK, n_u, CHUNK), BF16),
            vm((n_u, 128), jnp.int32), vm((n_u, 128), jnp.int32), vm((n_u, 128), F32),
            vm((3, 32, 128), jnp.int32), vm((3, 3, 32, 128), jnp.int32), vm((32, 128), F32),
            vm((STAGES, 2, EMB, half), BF16), vm((STAGES, 2, EMB, half), F32), vm((STAGES, 2, EMB, half), F32),
            vm((2, EMB, half), F32), vm((2, EMB, half), F32),
            vm((S, EMB, EMB), BF16), vm((STAGES, 2, S, S, S) + tile, BF16), vm((STAGES, 2, S, S, S) + tile, F32),
            vm((STAGES, 2, S, S) + tile, F32), vm((STAGES, 2, S) + tile, F32),
            vm((STAGES, 2, 3, S, S) + tile, F32), vm((STAGES, 2, 3, S) + tile, F32), vm((STAGES, 2, 3) + tile, F32),
            vm((2,) + tile, F32), vm((2, S) + tile, F32),
            vm((2, S) + tile, BF16), vm((2, S) + tile, F32), vm((CHUNK, EMB), F32),
            vm((2, 2, S, S, 3) + tile, BF16), vm((2, S, S, 3) + tile, BF16), vm((2, S, S, 3) + tile, BF16),
            vm((2, S, 3) + tile, BF16), vm((2, 3) + tile, BF16),
            vm((2, 3, S, 3) + tile, BF16), vm((2, 3, 3) + tile, BF16), vm((2, 3, 3) + tile, BF16),
            vm((2, 2, S, S, 3) + tile, BF16),
            vm((3 * EMB, n_b), BF16), vm((3 * EMB, n_b), BF16),
            vm((3 * EMB, n_u), F32), vm((3 * EMB, CHUNK), F32),
            pltpu.SemaphoreType.DMA((NCHUNK,)), pltpu.SemaphoreType.DMA((NSEM,)), pltpu.SemaphoreType.DMA((NSEM,)),
        ]
        spec = pl.BlockSpec(memory_space=pltpu.VMEM)
        fu, fi, loss, gu, gi = pl.pallas_call(
            kernel,
            out_shape=outs,
            in_specs=[pl.BlockSpec(memory_space=pl.ANY), spec, spec, spec],
            out_specs=(spec,) * 5,
            scratch_shapes=scratch,
            compiler_params=pltpu.CompilerParams(collective_id=0, has_side_effects=True, vmem_limit_bytes=56 * 1024 * 1024),
        )(mask_blk, user_emb, item_emb, triples.T)
        return fu, fi, loss[0, 0], gu, gi

    user_spec = P(('row', 'col'), None)
    item_spec = P(('col', 'row'), None)
    return jax.shard_map(local_fn, mesh=mesh, in_specs=(P('row', 'col'), user_spec, item_spec, P()),
                         out_specs=(user_spec, item_spec, P(), user_spec, item_spec), check_vma=False)
```

```python
import jax
import jax.numpy as jnp
from jax import lax
from jax.experimental import pallas as pl
from jax.experimental.pallas import tpu as pltpu
from jax.sharding import PartitionSpec as P

SIDE = 4
STRIDE = (16, 4, 1)
EMB = 64
CHUNK = 256
NCHUNK = 16
LAYERS = 3
STAGES = 2 * LAYERS
F32 = jnp.float32
BF16 = jnp.bfloat16
NSEM = 480
PLANE_ORDER = (10, 6, 9, 11, 14, 5, 7, 13, 15, 2, 8, 1, 3, 4, 12)
NT = (((1,), (1,)), ((), ()))
MESH = pl.DeviceIdType.MESH


def block_rows(part, q):
    return slice(32 * part + 16 * (q // 2), 32 * part + 16 * (q // 2) + 16)


def block_lanes(q):
    return slice(128 * (q % 2), 128 * (q % 2) + 128)


def join_blocks(get):
    rows = []
    for part in range(2):
        for half in range(2):
            rows.append(jnp.concatenate([get(part, 2 * half), get(part, 2 * half + 1)], axis=1))
    return jnp.concatenate(rows, axis=0)


def kernel(mask_hbm, user_ref, item_ref, ids_ref,
           fu_ref, fi_ref, loss_ref, gu_ref, gi_ref,
           mask, adj, rowsum, rowsum_in, scale_u, colsum, colsum_in, scale_i,
           ut, up, up_in, u_acc, s_user,
           nat, it, part_sum, q1, r1, r2, i_acc, s_item,
           fin_b, fin_f, nat_f,
           sel, sel_in, w0, w1, w2, in1, in2, in3, rows_all, grad_u, grad_i, prod_u, prod_i,
           mask_sem, send_sem, recv_sem):
    row = lax.axis_index('row')
    col = lax.axis_index('col')
    pos = (lax.div(row, 16), lax.rem(lax.div(row, 4), 4), lax.rem(row, 4))
    step = [[p] + [lax.rem(p + k, SIDE) for k in range(1, SIDE)] for p in pos]
    offset = [[(step[a][k] - pos[a]) * STRIDE[a] if k else 0 for k in range(SIDE)] for a in range(3)]
    z, y, x = pos
    users = user_ref.shape[1]
    n_batch = ids_ref.shape[1]

    def peer(axis, k):
        return {'row': row + offset[axis][k]}

    partner = {'col': 1 - col}

    copies = []
    for j in range(NCHUNK):
        cp = pltpu.make_async_copy(mask_hbm.at[:, pl.ds(j * CHUNK, CHUNK)], mask.at[j], mask_sem.at[j])
        cp.start()
        copies.append(cp)

    def plane_peer(axes, k):
        return {'row': row + offset[axes[0]][k // SIDE] + offset[axes[1]][k % SIDE]}

    barrier = pltpu.get_barrier_semaphore()
    for axis in range(3):
        for k in range(1, SIDE):
            pl.semaphore_signal(barrier, inc=1, device_id=peer(axis, k), device_id_type=MESH)
    for axes in ((0, 1), (0, 2), (1, 2)):
        for k in range(SIDE * SIDE):
            if k // SIDE and k % SIDE:
                pl.semaphore_signal(barrier, inc=1, device_id=plane_peer(axes, k), device_id_type=MESH)
    pl.semaphore_signal(barrier, inc=1, device_id=partner, device_id_type=MESH)
    pl.semaphore_wait(barrier, 37)

    sent = []

    def send(src, dst, device):
        i = len(sent)
        cp = pltpu.make_async_remote_copy(src_ref=src, dst_ref=dst, send_sem=send_sem.at[i], recv_sem=recv_sem.at[i],
                                          device_id=device, device_id_type=MESH)
        cp.start()
        sent.append(cp)
        return cp

    def send_axis(axis, src, dst):
        return [send(src(step[axis][k]), dst(k - 1), peer(axis, k)) for k in (1, 3, 2)]

    def send_plane(axes, src, dst):
        return [send(src(step[axes[0]][k // SIDE], step[axes[1]][k % SIDE]), dst(k - 1), plane_peer(axes, k))
                for k in PLANE_ORDER]

    def arrive(cps):
        for cp in cps:
            cp.wait_recv()

    ut[0, col] = user_ref[...]
    u_first = [send(ut.at[0, col], ut.at[0, col], partner)]
    nat[x] = item_ref[...]
    i_first = send_axis(2, lambda t: nat.at[x], lambda k: nat.at[x])

    rowsum[...] = jnp.zeros_like(rowsum)
    for j in range(NCHUNK):
        copies[j].wait()
        m = mask[j]
        rowsum[...] += m[:, :128] + m[:, 128:]
        s = jnp.sum(m, axis=0, keepdims=True)
        colsum[0, 2 * j:2 * j + 1, :] = s[:, :128]
        colsum[0, 2 * j + 1:2 * j + 2, :] = s[:, 128:]
    rs_cp = [send(rowsum, rowsum_in, partner)]
    cs_cp = send_axis(0, lambda t: colsum.at[0], lambda k: colsum_in.at[0, k])

    arrive(i_first)
    chunk0 = jnp.concatenate([nat[k].astype(F32) for k in range(SIDE)], axis=0).T
    for part in range(2):
        for q in range(SIDE):
            it[0, part, z, y, q] = chunk0[block_rows(part, q), block_lanes(q)].astype(BF16)

    def gather_start(s, axis):
        if axis == 2:
            ref = it.at[s, :, z, y, x]
        elif axis == 0:
            ref = it.at[s, :, z, y]
        else:
            ref = it.at[s, :, :, y]
        return send_axis(axis, lambda t: ref, lambda k: ref)

    ag = gather_start(0, 0)
    arrive(rs_cp)
    deg_u = jnp.maximum(jnp.sum(rowsum[...] + rowsum_in[...], axis=1, keepdims=True), 1)
    scale_u[...] = jnp.broadcast_to(lax.rsqrt(deg_u.astype(F32)), scale_u.shape)
    arrive(cs_cp)
    colsum[1] = colsum[0] + colsum_in[0, 0] + colsum_in[0, 1] + colsum_in[0, 2]
    cs_cp = send_axis(1, lambda t: colsum.at[1], lambda k: colsum_in.at[1, k])
    arrive(ag)
    ag = gather_start(0, 1)
    arrive(cs_cp)
    colsum[2] = colsum[1] + colsum_in[1, 0] + colsum_in[1, 1] + colsum_in[1, 2]
    cs_cp = send_axis(2, lambda t: colsum.at[2], lambda k: colsum_in.at[2, k])
    arrive(cs_cp)
    deg_i = jnp.maximum(colsum[2] + colsum_in[2, 0] + colsum_in[2, 1] + colsum_in[2, 2], 1)
    scale_i[...] = lax.rsqrt(deg_i.astype(F32))
    for j in range(NCHUNK):
        su = scale_u[...]
        m = mask[j].astype(F32)
        adj[j, :, :128] = (su * m[:, :128] * scale_i[2 * j:2 * j + 1, :]).astype(BF16)
        adj[j, :, 128:] = (su * m[:, 128:] * scale_i[2 * j + 1:2 * j + 2, :]).astype(BF16)

    def at(ref, axis, t):
        return ref.at[(slice(None),) * axis + (t,)]

    def item_product(s, hold=False):
        lhs = jnp.concatenate([ut[s, 0], ut[s, 1]], axis=1)
        first = []
        for k in (2, 1, 3, 0):
            zz = step[0][k]
            for yy in range(SIDE):
                out = jnp.dot(lhs, adj[zz * SIDE + yy], preferred_element_type=F32)
                for part in range(2):
                    for q in range(SIDE):
                        part_sum[s, part, zz, yy, q] = out[block_rows(part, q), block_lanes(q)]
            if k and not hold:
                first.append(send(part_sum.at[s, 0, zz], r1.at[s, 0, k - 1], peer(0, k)))
        return first

    def scatter_start(s, first=None):
        if not first:
            first = send_axis(0, lambda t: part_sum.at[s, 0, t], lambda k: r1.at[s, 0, k])
        return [first, send_axis(2, lambda t: part_sum.at[s, 1, :, :, t], lambda k: r1.at[s, 1, k])]

    REST = ((1, 2), (0, 1))

    def scatter_mid(s, cps):
        out = []
        for p in range(2):
            arrive(cps[p])
            own = part_sum[s, 0, z] if p == 0 else part_sum[s, 1, :, :, x]
            q1[s, p] = own + r1[s, p, 0] + r1[s, p, 1] + r1[s, p, 2]
            out.append(send_plane(REST[p], lambda t0, t1, p=p: q1.at[s, p, t0, t1], lambda k, p=p: r2.at[s, p, k]))
        return out

    def scatter_end(s, cps):
        out = []
        for p in range(2):
            arrive(cps[p])
            out.append(q1[s, p, pos[REST[p][0]], pos[REST[p][1]]] + jnp.sum(r2[s, p], axis=0))
        return out

    def user_group(s, yy, first):
        acc = None
        for zz in range(SIDE):
            lhs = join_blocks(lambda part, q: it[s, part, zz, yy, q])
            d = lax.dot_general(lhs, adj[zz * SIDE + yy], NT, preferred_element_type=F32)
            acc = d if acc is None else acc + d
        for h in range(2):
            v = acc[:, h * users:(h + 1) * users]
            up[s, h] = v if first else up[s, h] + v

    def gather_plane(s):
        ref = it.at[s, :, z, y, x]
        return send_plane((0, 2), lambda t0, t1: ref, lambda k: ref)

    def user_own(s):
        user_group(s, y, True)

    def user_rest(s, ag):
        for cp, k in zip(ag, (1, 3, 2)):
            cp.wait_recv()
            user_group(s, step[1][SIDE - k], False)
        return [send(up.at[s], up_in.at[s], partner)]

    for p in range(2):
        i_acc[p] = it[0, p, z, y, x].astype(F32)
    arrive(u_first)
    for h in range(2):
        u_acc[h] = ut[0, h].astype(F32)

    def user_next(s):
        for h in range(2):
            nxt = (up[s, h] + up_in[s, h]).astype(BF16)
            u_acc[h] += nxt.astype(F32)
            if s + 1 < LAYERS:
                ut[s + 1, h] = nxt

    rs = scatter_start(0, item_product(0))
    arrive(ag)
    for k in range(SIDE):
        user_group(0, step[1][k], k == 0)
    ux = [send(up.at[0], up_in.at[0], partner)]
    arrive(ux)
    user_next(0)
    item_product(1, hold=True)
    rs = scatter_mid(0, rs)
    for s in range(LAYERS):
        if s == 0:
            rs_next = scatter_start(1)
        else:
            arrive(ag)
            ag = gather_start(s, 1)
            user_own(s)
            rs = scatter_mid(s, rs)
            ux = user_rest(s, ag)
        new = scatter_end(s, rs)
        for p in range(2):
            nxt = new[p].astype(BF16)
            i_acc[p] += nxt.astype(F32)
            if s + 1 < LAYERS:
                it[s + 1, p, z, y, x] = nxt
        if s + 1 < LAYERS:
            ag = gather_plane(s + 1)
        if s > 0:
            arrive(ux)
            user_next(s)
            if s + 1 < LAYERS:
                rs_next = scatter_start(s + 1, item_product(s + 1))
        rs = rs_next

    tiles = n_batch // CHUNK
    iota = lax.broadcasted_iota(jnp.int32, (users, CHUNK), 0)
    for p in range(2):
        fin_b[p, x] = (i_acc[p] * 0.25).astype(BF16)
    fb = send_axis(2, lambda t: fin_b.at[:, x], lambda k: fin_b.at[:, x])
    for h in range(2):
        ut[LAYERS, h] = (u_acc[h] * 0.25).astype(BF16)
    own_u = ut[LAYERS, col]
    fu_ref[...] = own_u

    def put_rows(rt, t, picked):
        for l in range(2):
            lt = 2 * t + l
            sel[lt // 8, (lt % 8) // 4, lt % 4, rt // 3, rt % 3] = picked[:, 128 * l:128 * l + 128].astype(BF16)

    base_u = (2 * row + col) * users
    for t in range(tiles):
        ids = ids_ref[0:1, t * CHUNK:(t + 1) * CHUNK]
        hot = jnp.where(iota == ids - base_u, 1.0, 0.0).astype(BF16)
        picked = jnp.dot(own_u, hot, preferred_element_type=F32)
        for r in range(4):
            put_rows(r, t, picked[16 * r:16 * r + 16])
    base_i = (col * NCHUNK + z * SIDE + y) * CHUNK
    iota_i = lax.broadcasted_iota(jnp.int32, (CHUNK, CHUNK), 0)
    iota_b = lax.broadcasted_iota(jnp.int32, (128, CHUNK), 0)
    x_half, x_side = lax.div(x, 2), lax.rem(x, 2)
    base_b = base_i + 128 * x_side
    own_i = jnp.concatenate([fin_b[0, x], fin_b[1, x]], axis=0)
    for g in range(1, 3):
        for t in range(tiles):
            hot = jnp.where(iota_b == ids_ref[g:g + 1, t * CHUNK:(t + 1) * CHUNK] - base_b, 1.0, 0.0).astype(BF16)
            picked = jnp.dot(own_i, hot, preferred_element_type=F32)
            for part in range(2):
                rows = picked[16 * part:16 * part + 16]
                for half in range(2):
                    put_rows(4 * g + 2 * part + half, t, jnp.where(x_half == half, rows, 0.0))

    sx = [send(sel.at[1 - col], sel_in, partner)]
    arrive(sx)
    w0[...] = sel[col] + sel_in[...]
    ax0, ax2 = (0, 2), (2, 0)
    cps = [send_axis(ax0[p], lambda t, p=p: w0.at[p, t], lambda k, p=p: in1.at[p, k]) for p in range(2)]
    nxt_cps = []
    arrive(fb)
    nat_f[...] = join_blocks(lambda part, q: fin_b[part, q]).astype(F32).T
    own = pl.ds(pl.multiple_of(x * EMB, EMB), EMB)
    fi_ref[...] = nat_f[own, :].astype(BF16)
    for p in range(2):
        arrive(cps[p])
        w1[p] = w0[p, pos[ax0[p]]] + in1[p, 0] + in1[p, 1] + in1[p, 2]
        nxt_cps.append(send_axis(1, lambda t, p=p: w1.at[p, t], lambda k, p=p: in2.at[p, k]))
    cps, nxt_cps = nxt_cps, []
    for p in range(2):
        arrive(cps[p])
        w2[p] = w1[p, y] + in2[p, 0] + in2[p, 1] + in2[p, 2]
        nxt_cps.append(send_axis(ax2[p], lambda t, p=p: w2.at[p], lambda k, p=p: in3.at[p, k]))
    cps, nxt_cps = nxt_cps, []
    for p in range(2):
        arrive(cps[p])
        a = pos[ax0[p]]
        rows_all[col, p, a, y] = w2[p] + in3[p, 0] + in3[p, 1] + in3[p, 2]
        ref = rows_all.at[col, p, a, y]
        nxt_cps.append(send_axis(1, lambda t, ref=ref: ref, lambda k, ref=ref: ref))
    cps, nxt_cps = nxt_cps, []
    for p in range(2):
        arrive(cps[p])
        ref = rows_all.at[col, p, pos[ax0[p]]]
        nxt_cps.append(send_axis(ax0[p], lambda t, ref=ref: ref, lambda k, ref=ref: ref))
    for p in range(2):
        arrive(nxt_cps[p])
    arrive([send(rows_all.at[col], rows_all.at[col], partner)])

    total = jnp.zeros((1, 128), F32)
    for lt in range(n_batch // 128):
        def rows_of(group):
            return jnp.concatenate([rows_all[lt // 8, (lt % 8) // 4, lt % 4, rt // 3, rt % 3].astype(F32)
                                    for rt in range(4 * group, 4 * group + 4)], axis=0)
        e_user, e_pos, e_neg = rows_of(0), rows_of(1), rows_of(2)
        margin = jnp.sum(e_user * e_pos, axis=0, keepdims=True) - jnp.sum(e_user * e_neg, axis=0, keepdims=True)
        soft = jnp.maximum(-margin, 0.0) + jnp.log1p(jnp.exp(-jnp.abs(margin)))
        total = total + soft
        coef = -jax.nn.sigmoid(-margin) / n_batch
        lanes = slice(lt * 128, lt * 128 + 128)
        for ref, g in ((grad_u, coef * (e_pos - e_neg)), (grad_i, coef * e_user)):
            hi = g.astype(BF16)
            left = g - hi.astype(F32)
            mid = left.astype(BF16)
            ref[0:EMB, lanes] = hi
            ref[EMB:2 * EMB, lanes] = mid
            ref[2 * EMB:3 * EMB, lanes] = (left - mid.astype(F32)).astype(BF16)
    loss_ref[...] = jnp.sum(total, axis=1, keepdims=True) / n_batch

    iota2 = lax.broadcasted_iota(jnp.int32, (2 * users, CHUNK), 0)
    prod_i[...] = jnp.zeros_like(prod_i)
    prod_u[...] = jnp.zeros_like(prod_u)
    for t in range(tiles):
        cut = slice(t * CHUNK, (t + 1) * CHUNK)
        plus = jnp.where(iota_i == ids_ref[1:2, cut] - base_i, 1.0, 0.0)
        minus = jnp.where(iota_i == ids_ref[2:3, cut] - base_i, 1.0, 0.0)
        prod_i[...] += lax.dot_general(grad_i[:, cut], (plus - minus).astype(BF16), NT, preferred_element_type=F32)
    seed = (prod_i[0:EMB, :] + prod_i[EMB:2 * EMB, :] + prod_i[2 * EMB:3 * EMB, :]) * 0.25
    s0 = LAYERS
    for part in range(2):
        for q in range(SIDE):
            block = seed[block_rows(part, q), block_lanes(q)]
            s_item[part, q] = block
            it[s0, part, z, y, q] = block.astype(BF16)
    ag = gather_start(s0, 0)
    for t in range(tiles):
        cut = slice(t * CHUNK, (t + 1) * CHUNK)
        hot = jnp.where(iota2 == ids_ref[0:1, cut] - row * (2 * users), 1.0, 0.0).astype(BF16)
        prod_u[...] += lax.dot_general(grad_u[:, cut], hot, NT, preferred_element_type=F32)
    seed = (prod_u[0:EMB, :] + prod_u[EMB:2 * EMB, :] + prod_u[2 * EMB:3 * EMB, :]) * 0.25
    for h in range(2):
        s_user[h] = seed[:, h * users:(h + 1) * users]
        ut[s0, h] = seed[:, h * users:(h + 1) * users].astype(BF16)

    rs = scatter_start(s0, item_product(s0))
    for s in range(s0, STAGES):
        arrive(ag)
        ag = gather_start(s, 1)
        user_own(s)
        rs = scatter_mid(s, rs)
        ux = user_rest(s, ag)
        new = scatter_end(s, rs)
        for p in range(2):
            nxt = s_item[p, x] + new[p]
            if s + 1 < STAGES:
                it[s + 1, p, z, y, x] = nxt.astype(BF16)
            else:
                fin_f[p, x] = nxt
        if s + 1 < STAGES:
            ag = gather_plane(s + 1)
        else:
            ff = send_axis(2, lambda t: fin_f.at[:, x], lambda k: fin_f.at[:, x])
        arrive(ux)
        if s + 1 < STAGES:
            for h in range(2):
                ut[s + 1, h] = (s_user[h] + (up[s, h] + up_in[s, h])).astype(BF16)
            rs = scatter_start(s + 1, item_product(s + 1))
        else:
            gu_ref[...] = s_user[col] + (up[s, col] + up_in[s, col])
    arrive(ff)
    nat_f[...] = join_blocks(lambda part, q: fin_f[part, q]).T
    gi_ref[...] = nat_f[own, :]
    for cp in sent:
        cp.wait_send()


def solution(mesh):
    def local_fn(mask_blk, user_emb, item_emb, triples):
        n_u, n_b = mask_blk.shape[0], triples.shape[0]
        half = n_u // 2
        vm = pltpu.VMEM
        outs = (jax.ShapeDtypeStruct((EMB, half), BF16), jax.ShapeDtypeStruct((EMB, EMB), BF16),
                jax.ShapeDtypeStruct((1, 1), F32), jax.ShapeDtypeStruct((EMB, half), F32),
                jax.ShapeDtypeStruct((EMB, EMB), F32))
        tile = (16, 128)
        S = SIDE
        scratch = [
            vm((NCHUNK, n_u, CHUNK), jnp.int32), vm((NCHUNK, n_u, CHUNK), BF16),
            vm((n_u, 128), jnp.int32), vm((n_u, 128), jnp.int32), vm((n_u, 128), F32),
            vm((3, 32, 128), jnp.int32), vm((3, 3, 32, 128), jnp.int32), vm((32, 128), F32),
            vm((STAGES, 2, EMB, half), BF16), vm((STAGES, 2, EMB, half), F32), vm((STAGES, 2, EMB, half), F32),
            vm((2, EMB, half), F32), vm((2, EMB, half), F32),
            vm((S, EMB, EMB), BF16), vm((STAGES, 2, S, S, S) + tile, BF16), vm((STAGES, 2, S, S, S) + tile, F32),
            vm((STAGES, 2, S, S) + tile, F32),
            vm((STAGES, 2, 3, S, S) + tile, F32), vm((STAGES, 2, S * S - 1) + tile, F32),
            vm((2,) + tile, F32), vm((2, S) + tile, F32),
            vm((2, S) + tile, BF16), vm((2, S) + tile, F32), vm((CHUNK, EMB), F32),
            vm((2, 2, S, S, 3) + tile, BF16), vm((2, S, S, 3) + tile, BF16), vm((2, S, S, 3) + tile, BF16),
            vm((2, S, 3) + tile, BF16), vm((2, 3) + tile, BF16),
            vm((2, 3, S, 3) + tile, BF16), vm((2, 3, 3) + tile, BF16), vm((2, 3, 3) + tile, BF16),
            vm((2, 2, S, S, 3) + tile, BF16),
            vm((3 * EMB, n_b), BF16), vm((3 * EMB, n_b), BF16),
            vm((3 * EMB, n_u), F32), vm((3 * EMB, CHUNK), F32),
            pltpu.SemaphoreType.DMA((NCHUNK,)), pltpu.SemaphoreType.DMA((NSEM,)), pltpu.SemaphoreType.DMA((NSEM,)),
        ]
        spec = pl.BlockSpec(memory_space=pltpu.VMEM)
        fu, fi, loss, gu, gi = pl.pallas_call(
            kernel,
            out_shape=outs,
            in_specs=[pl.BlockSpec(memory_space=pl.ANY), spec, spec, spec],
            out_specs=(spec,) * 5,
            scratch_shapes=scratch,
            compiler_params=pltpu.CompilerParams(collective_id=0, has_side_effects=True, vmem_limit_bytes=56 * 1024 * 1024),
        )(mask_blk, user_emb.T, item_emb, triples.T)
        return fu.T, fi, loss[0, 0], gu.T, gi

    user_spec = P(('row', 'col'), None)
    item_spec = P(('col', 'row'), None)
    return jax.shard_map(local_fn, mesh=mesh, in_specs=(P('row', 'col'), user_spec, item_spec, P()),
                         out_specs=(user_spec, item_spec, P(), user_spec, item_spec), check_vma=False)
```

```python
import jax
import jax.numpy as jnp
from jax import lax
from jax.experimental import pallas as pl
from jax.experimental.pallas import tpu as pltpu
from jax.sharding import PartitionSpec as P

SIDE = 4
STRIDE = (16, 4, 1)
EMB = 64
CHUNK = 256
NCHUNK = 16
LAYERS = 3
STAGES = 2 * LAYERS
F32 = jnp.float32
BF16 = jnp.bfloat16
NSEM = 160
PLANE_ORDER = (10, 6, 9, 11, 14, 5, 7, 13, 15, 2, 8, 1, 3, 4, 12)
NT = (((1,), (1,)), ((), ()))
MESH = pl.DeviceIdType.MESH


def block_rows(part, q):
    return slice(32 * part + 16 * (q // 2), 32 * part + 16 * (q // 2) + 16)


def block_lanes(q):
    return slice(128 * (q % 2), 128 * (q % 2) + 128)


def join_blocks(get):
    rows = []
    for part in range(2):
        for half in range(2):
            rows.append(jnp.concatenate([get(part, 2 * half), get(part, 2 * half + 1)], axis=1))
    return jnp.concatenate(rows, axis=0)


def kernel(mask_hbm, user_ref, item_ref, ids_ref,
           fu_ref, fi_ref, loss_ref, gu_ref, gi_ref,
           mask, adj, rowsum, rowsum_in, scale_u, colsum, colsum_in, scale_i,
           ut, up, up_in, u_acc, s_user,
           nat, it, part_sum, q1, r1, r2, i_acc, s_item,
           fin_b, fin_f, nat_f,
           sel, sel_in, w0, w1, in1, in2, rows_all, grad_u, grad_i, prod_u, prod_i,
           mask_sem, send_sem, recv_sem):
    row = lax.axis_index('row')
    col = lax.axis_index('col')
    pos = (lax.div(row, 16), lax.rem(lax.div(row, 4), 4), lax.rem(row, 4))
    step = [[p] + [lax.rem(p + k, SIDE) for k in range(1, SIDE)] for p in pos]
    offset = [[(step[a][k] - pos[a]) * STRIDE[a] if k else 0 for k in range(SIDE)] for a in range(3)]
    z, y, x = pos
    users = user_ref.shape[1]
    n_batch = ids_ref.shape[1]

    def peer(axis, k):
        return {'row': row + offset[axis][k]}

    partner = {'col': 1 - col}

    copies = []
    for j in range(NCHUNK):
        cp = pltpu.make_async_copy(mask_hbm.at[:, pl.ds(j * CHUNK, CHUNK)], mask.at[j], mask_sem.at[j])
        cp.start()
        copies.append(cp)

    def plane_peer(axes, k):
        return {'row': row + offset[axes[0]][k // SIDE] + offset[axes[1]][k % SIDE]}

    barrier = pltpu.get_barrier_semaphore()
    for axis in range(3):
        for k in range(1, SIDE):
            pl.semaphore_signal(barrier, inc=1, device_id=peer(axis, k), device_id_type=MESH)
    for axes in ((0, 1), (0, 2), (1, 2)):
        for k in range(SIDE * SIDE):
            if k // SIDE and k % SIDE:
                pl.semaphore_signal(barrier, inc=1, device_id=plane_peer(axes, k), device_id_type=MESH)
    pl.semaphore_signal(barrier, inc=1, device_id=partner, device_id_type=MESH)
    pl.semaphore_wait(barrier, 37)

    count = [0, 0]
    leaving = []

    def fresh(n=1):
        out = (count[0], count[1])
        count[0] += 1
        count[1] += n
        return out

    def send(src, dst, device, sems):
        pltpu.make_async_remote_copy(src_ref=src, dst_ref=dst, send_sem=send_sem.at[sems[0]], recv_sem=recv_sem.at[sems[1]],
                                     device_id=device, device_id_type=MESH).start()

    def left(ref, sems):
        leaving.append((ref, sems[0]))

    def arrive(ref, sems):
        pltpu.make_async_copy(ref, ref, recv_sem.at[sems[1]]).wait()

    def plus(sems, n):
        return (sems[0], sems[1] + n)

    def send_axis(axis, src, dst, sems):
        for k in (1, 3, 2):
            send(src(step[axis][k]), dst(k - 1), peer(axis, k), sems)

    def send_plane(axes, src, dst, sems):
        for k in PLANE_ORDER:
            send(src(step[axes[0]][k // SIDE], step[axes[1]][k % SIDE]), dst(k - 1), plane_peer(axes, k), sems)

    ut[0, col] = user_ref[...]
    u_sem = fresh()
    send(ut.at[0, col], ut.at[0, col], partner, u_sem)
    left(ut.at[0, 0], u_sem)
    nat[x] = item_ref[...]
    n_sem = fresh()
    send_axis(2, lambda t: nat.at[x], lambda k: nat.at[x], n_sem)
    left(nat.at[0:3], n_sem)

    rowsum[...] = jnp.zeros_like(rowsum)
    for j in range(NCHUNK):
        copies[j].wait()
        m = mask[j]
        rowsum[...] += m[:, :128] + m[:, 128:]
        s = jnp.sum(m, axis=0, keepdims=True)
        colsum[0, 2 * j:2 * j + 1, :] = s[:, :128]
        colsum[0, 2 * j + 1:2 * j + 2, :] = s[:, 128:]
    r_sem, c_sem = fresh(), fresh()
    send(rowsum, rowsum_in, partner, r_sem)
    left(rowsum, r_sem)
    send_axis(0, lambda t: colsum.at[0], lambda k: colsum_in.at[k], c_sem)
    left(colsum_in.at[0:3], c_sem)

    arrive(nat.at[0:3], n_sem)
    chunk0 = jnp.concatenate([nat[k].astype(F32) for k in range(SIDE)], axis=0).T
    for part in range(2):
        for q in range(SIDE):
            it[0, part, z, y, q] = chunk0[block_rows(part, q), block_lanes(q)].astype(BF16)

    stage_sem = [dict(user=fresh(), plane=fresh(SIDE), line=fresh(SIDE), axis=[fresh(SIDE), fresh(SIDE)],
                      last=[fresh(), fresh()]) for _ in range(STAGES)]

    def gather_plane(s):
        sems = stage_sem[s]['plane']
        ref = it.at[s, :, z, y, x]
        for k in PLANE_ORDER:
            send(ref, ref, plane_peer((0, 2), k), plus(sems, k // SIDE))
        left(r2.at[s, 0], sems)

    def gather_line(s):
        sems = stage_sem[s]['plane']
        ref = it.at[s, :, z, y]
        for k in (1, 3, 2):
            send(ref, ref, peer(0, k), plus(sems, k))
        left(it.at[s, :, 0:3, 0], sems)

    def gather_last(s, line=False):
        sems = stage_sem[s]
        for kz in (0, 1, 3, 2):
            ref = it.at[s, :, step[0][(SIDE - kz) % SIDE], y]
            if kz:
                arrive(ref, plus(sems['plane'], kz))
            elif not line:
                arrive(ref.at[:, 0:3], sems['plane'])
            for k in (1, 3, 2):
                send(ref, ref, peer(1, k), plus(sems['line'], k))
        left(r1.at[s, 0], sems['line'])

    gather_line(0)
    arrive(rowsum_in, r_sem)
    deg_u = jnp.maximum(jnp.sum(rowsum[...] + rowsum_in[...], axis=1, keepdims=True), 1)
    scale_u[...] = jnp.broadcast_to(lax.rsqrt(deg_u.astype(F32)), scale_u.shape)
    arrive(colsum_in.at[0:3], c_sem)
    colsum[1] = colsum[0] + colsum_in[0] + colsum_in[1] + colsum_in[2]
    d_sem = fresh()
    send_plane((1, 2), lambda t0, t1: colsum.at[1], lambda k: colsum_in.at[3 + k], d_sem)
    left(colsum_in.at[3:18], d_sem)
    gather_last(0, line=True)
    arrive(colsum_in.at[3:18], d_sem)
    deg_i = jnp.maximum(colsum[1] + jnp.sum(colsum_in[3:], axis=0), 1)
    scale_i[...] = lax.rsqrt(deg_i.astype(F32))
    for j in range(NCHUNK):
        su = scale_u[...]
        m = mask[j].astype(F32)
        adj[j, :, :128] = (su * m[:, :128] * scale_i[2 * j:2 * j + 1, :]).astype(BF16)
        adj[j, :, 128:] = (su * m[:, 128:] * scale_i[2 * j + 1:2 * j + 2, :]).astype(BF16)

    def at(ref, axis, t):
        return ref.at[(slice(None),) * axis + (t,)]

    def item_product(s, hold=False):
        lhs = jnp.concatenate([ut[s, 0], ut[s, 1]], axis=1)

        def body(i, _):
            ky = lax.rem(i + 1, SIDE)
            yy = lax.rem(y + ky, SIDE)
            for kz in (2, 1, 3, 0):
                zz = step[0][kz]
                out = jnp.dot(lhs, adj[zz * SIDE + yy], preferred_element_type=F32)
                for part in range(2):
                    for q in range(SIDE):
                        part_sum[s, part, zz, yy, q] = out[block_rows(part, q), block_lanes(q)]
            if not hold:
                scatter_send(s, ky, yy)
            return 0

        lax.fori_loop(0, SIDE, body, 0)
        for p in range(2):
            left(r1.at[s, p], stage_sem[s]['axis'][p])

    def scatter_send(s, ky, yy):
        sems = stage_sem[s]['axis']
        send_axis(0, lambda t: part_sum.at[s, 0, t, yy], lambda k: r1.at[s, 0, ky, k], plus(sems[0], ky))
        send_axis(2, lambda t: part_sum.at[s, 1, :, yy, t], lambda k: r1.at[s, 1, ky, k], plus(sems[1], ky))

    def scatter_mid(s):
        sems = stage_sem[s]

        def piece(ky, yy, off, ks):
            for p in range(2):
                axis = (2, 0)[p]
                arrive(r1.at[s, p, ky], plus(sems['axis'][p], ky))
                own = part_sum[s, 0, z, yy] if p == 0 else part_sum[s, 1, :, yy, x]
                q1[s, p, ky] = own + jnp.sum(r1[s, p, ky], axis=0)
                for k in ks:
                    send(q1.at[s, p, ky, step[axis][k]], r2.at[s, p, 4 * ky + k - 1], {'row': row + off + offset[axis][k]},
                         sems['last'][p])

        def body(ky, _):
            yy = lax.rem(y + ky, SIDE)
            piece(ky, yy, (yy - y) * STRIDE[1], (2, 1, 3, 0))
            return 0

        lax.fori_loop(1, SIDE, body, 0)
        piece(0, y, 0, (2, 1, 3))
        for p in range(2):
            left(r2.at[s, p], sems['last'][p])

    def scatter_end(s):
        out = []
        for p in range(2):
            arrive(r2.at[s, p], stage_sem[s]['last'][p])
            out.append(q1[s, p, 0, pos[(2, 0)[p]]] + jnp.sum(r2[s, p], axis=0))
        return out

    def user_group(s, yy, first):
        acc = None
        for zz in range(SIDE):
            lhs = join_blocks(lambda part, q: it[s, part, zz, yy, q])
            d = lax.dot_general(lhs, adj[zz * SIDE + yy], NT, preferred_element_type=F32)
            acc = d if acc is None else acc + d
        for h in range(2):
            v = acc[:, h * users:(h + 1) * users]
            up[s, h] = v if first else up[s, h] + v

    def user_own(s):
        user_group(s, y, True)

    def user_rest(s):
        def body(k, _):
            yy = lax.rem(y + SIDE - k, SIDE)
            arrive(it.at[s, :, :, yy], plus(stage_sem[s]['line'], k))
            user_group(s, yy, False)
            return 0

        lax.fori_loop(1, SIDE, body, 0)
        sems = stage_sem[s]['user']
        send(up.at[s], up_in.at[s], partner, sems)
        left(up.at[s], sems)

    def user_there(s):
        arrive(up_in.at[s], stage_sem[s]['user'])

    for p in range(2):
        i_acc[p] = it[0, p, z, y, x].astype(F32)
    arrive(ut.at[0, 1 - col], u_sem)
    for h in range(2):
        u_acc[h] = ut[0, h].astype(F32)

    def user_next(s):
        for h in range(2):
            nxt = (up[s, h] + up_in[s, h]).astype(BF16)
            u_acc[h] += nxt.astype(F32)
            if s + 1 < LAYERS:
                ut[s + 1, h] = nxt

    item_product(0)
    user_own(0)
    user_rest(0)
    user_there(0)
    user_next(0)
    item_product(1, hold=True)
    scatter_mid(0)
    for s in range(LAYERS):
        if s == 0:
            def late(i, _):
                ky = lax.rem(i + 1, SIDE)
                scatter_send(1, ky, lax.rem(y + ky, SIDE))
                return 0
            lax.fori_loop(0, SIDE, late, 0)
        else:
            gather_last(s)
            user_own(s)
            scatter_mid(s)
            user_rest(s)
        new = scatter_end(s)
        for p in range(2):
            nxt = new[p].astype(BF16)
            i_acc[p] += nxt.astype(F32)
            if s + 1 < LAYERS:
                it[s + 1, p, z, y, x] = nxt
        if s + 1 < LAYERS:
            gather_plane(s + 1)
        if s > 0:
            user_there(s)
            user_next(s)
            if s + 1 < LAYERS:
                item_product(s + 1)

    tiles = n_batch // CHUNK
    iota = lax.broadcasted_iota(jnp.int32, (users, CHUNK), 0)
    for p in range(2):
        fin_b[p, x] = (i_acc[p] * 0.25).astype(BF16)
    f_sem = fresh()
    send_axis(2, lambda t: fin_b.at[:, x], lambda k: fin_b.at[:, x], f_sem)
    left(fin_b.at[:, 0:3], f_sem)
    for h in range(2):
        ut[LAYERS, h] = (u_acc[h] * 0.25).astype(BF16)
    own_u = ut[LAYERS, col]
    fu_ref[...] = own_u

    def put_rows(rt, t, picked):
        for l in range(2):
            lt = 2 * t + l
            sel[lt // 8, (lt % 8) // 4, lt % 4, rt // 3, rt % 3] = picked[:, 128 * l:128 * l + 128].astype(BF16)

    base_u = (2 * row + col) * users
    for t in range(tiles):
        ids = ids_ref[0:1, t * CHUNK:(t + 1) * CHUNK]
        hot = jnp.where(iota == ids - base_u, 1.0, 0.0).astype(BF16)
        picked = jnp.dot(own_u, hot, preferred_element_type=F32)
        for r in range(4):
            put_rows(r, t, picked[16 * r:16 * r + 16])
    base_i = (col * NCHUNK + z * SIDE + y) * CHUNK
    iota_i = lax.broadcasted_iota(jnp.int32, (CHUNK, CHUNK), 0)
    iota_b = lax.broadcasted_iota(jnp.int32, (128, CHUNK), 0)
    x_half, x_side = lax.div(x, 2), lax.rem(x, 2)
    base_b = base_i + 128 * x_side
    own_i = jnp.concatenate([fin_b[0, x], fin_b[1, x]], axis=0)
    for g in range(1, 3):
        for t in range(tiles):
            hot = jnp.where(iota_b == ids_ref[g:g + 1, t * CHUNK:(t + 1) * CHUNK] - base_b, 1.0, 0.0).astype(BF16)
            picked = jnp.dot(own_i, hot, preferred_element_type=F32)
            for part in range(2):
                rows = picked[16 * part:16 * part + 16]
                for half in range(2):
                    put_rows(4 * g + 2 * part + half, t, jnp.where(x_half == half, rows, 0.0))

    x_sem = fresh()
    send(sel.at[1 - col], sel_in, partner, x_sem)
    left(sel_in, x_sem)
    arrive(sel_in, x_sem)
    w0[...] = sel[col] + sel_in[...]
    ax0, ax2 = (0, 2), (2, 0)
    sems = [fresh() for _ in range(2)]
    for p in range(2):
        send_plane((ax0[p], 1), lambda t0, t1: w0.at[p, t0, t1], lambda k: in1.at[p, k], sems[p])
        left(in1.at[p], sems[p])
    arrive(fin_b.at[:, 0:3], f_sem)
    nat_f[...] = join_blocks(lambda part, q: fin_b[part, q]).astype(F32).T
    own = pl.ds(pl.multiple_of(x * EMB, EMB), EMB)
    fi_ref[...] = nat_f[own, :].astype(BF16)
    sems2 = [fresh() for _ in range(2)]
    for p in range(2):
        arrive(in1.at[p], sems[p])
        w1[p] = (w0[p, pos[ax0[p]], y].astype(F32) + jnp.sum(in1[p].astype(F32), axis=0)).astype(BF16)
        send_axis(ax2[p], lambda t: w1.at[p], lambda k: in2.at[p, k], sems2[p])
        left(in2.at[p], sems2[p])
    sems3 = [fresh() for _ in range(2)]
    for p in range(2):
        arrive(in2.at[p], sems2[p])
        a = pos[ax0[p]]
        rows_all[col, p, a, y] = w1[p] + in2[p, 0] + in2[p, 1] + in2[p, 2]
        ref = rows_all.at[col, p, a, y]
        send_plane((ax0[p], 1), lambda t0, t1: ref, lambda k: ref, sems3[p])
        left(in1.at[p], sems3[p])
    for p in range(2):
        arrive(in1.at[p], sems3[p])
    o_sem = fresh()
    send(rows_all.at[col], rows_all.at[col], partner, o_sem)
    left(rows_all.at[0], o_sem)
    arrive(rows_all.at[1 - col], o_sem)

    total = jnp.zeros((1, 128), F32)
    for lt in range(n_batch // 128):
        def rows_of(group):
            return jnp.concatenate([rows_all[lt // 8, (lt % 8) // 4, lt % 4, rt // 3, rt % 3].astype(F32)
                                    for rt in range(4 * group, 4 * group + 4)], axis=0)
        e_user, e_pos, e_neg = rows_of(0), rows_of(1), rows_of(2)
        margin = jnp.sum(e_user * e_pos, axis=0, keepdims=True) - jnp.sum(e_user * e_neg, axis=0, keepdims=True)
        soft = jnp.maximum(-margin, 0.0) + jnp.log1p(jnp.exp(-jnp.abs(margin)))
        total = total + soft
        coef = -jax.nn.sigmoid(-margin) / n_batch
        lanes = slice(lt * 128, lt * 128 + 128)
        for ref, g in ((grad_u, coef * (e_pos - e_neg)), (grad_i, coef * e_user)):
            hi = g.astype(BF16)
            low = g - hi.astype(F32)
            mid = low.astype(BF16)
            ref[0:EMB, lanes] = hi
            ref[EMB:2 * EMB, lanes] = mid
            ref[2 * EMB:3 * EMB, lanes] = (low - mid.astype(F32)).astype(BF16)
    loss_ref[...] = jnp.sum(total, axis=1, keepdims=True) / n_batch

    iota2 = lax.broadcasted_iota(jnp.int32, (2 * users, CHUNK), 0)
    prod_i[...] = jnp.zeros_like(prod_i)
    prod_u[...] = jnp.zeros_like(prod_u)
    for t in range(tiles):
        cut = slice(t * CHUNK, (t + 1) * CHUNK)
        pos_hot = jnp.where(iota_i == ids_ref[1:2, cut] - base_i, 1.0, 0.0)
        neg_hot = jnp.where(iota_i == ids_ref[2:3, cut] - base_i, 1.0, 0.0)
        prod_i[...] += lax.dot_general(grad_i[:, cut], (pos_hot - neg_hot).astype(BF16), NT, preferred_element_type=F32)
    seed = (prod_i[0:EMB, :] + prod_i[EMB:2 * EMB, :] + prod_i[2 * EMB:3 * EMB, :]) * 0.25
    s0 = LAYERS
    for part in range(2):
        for q in range(SIDE):
            block = seed[block_rows(part, q), block_lanes(q)]
            s_item[part, q] = block
            it[s0, part, z, y, q] = block.astype(BF16)
    gather_line(s0)
    for t in range(tiles):
        cut = slice(t * CHUNK, (t + 1) * CHUNK)
        hot = jnp.where(iota2 == ids_ref[0:1, cut] - row * (2 * users), 1.0, 0.0).astype(BF16)
        prod_u[...] += lax.dot_general(grad_u[:, cut], hot, NT, preferred_element_type=F32)
    seed = (prod_u[0:EMB, :] + prod_u[EMB:2 * EMB, :] + prod_u[2 * EMB:3 * EMB, :]) * 0.25
    for h in range(2):
        s_user[h] = seed[:, h * users:(h + 1) * users]
        ut[s0, h] = seed[:, h * users:(h + 1) * users].astype(BF16)

    item_product(s0)
    for s in range(s0, STAGES):
        gather_last(s, line=s == s0)
        user_own(s)
        scatter_mid(s)
        user_rest(s)
        new = scatter_end(s)
        for p in range(2):
            nxt = s_item[p, x] + new[p]
            if s + 1 < STAGES:
                it[s + 1, p, z, y, x] = nxt.astype(BF16)
            else:
                fin_f[p, x] = nxt
        if s + 1 < STAGES:
            gather_plane(s + 1)
        else:
            e_sem = fresh()
            send_axis(2, lambda t: fin_f.at[:, x], lambda k: fin_f.at[:, x], e_sem)
            left(fin_f.at[:, 0:3], e_sem)
        user_there(s)
        if s + 1 < STAGES:
            for h in range(2):
                ut[s + 1, h] = (s_user[h] + (up[s, h] + up_in[s, h])).astype(BF16)
            item_product(s + 1)
        else:
            gu_ref[...] = s_user[col] + (up[s, col] + up_in[s, col])
    arrive(fin_f.at[:, 0:3], e_sem)
    nat_f[...] = join_blocks(lambda part, q: fin_f[part, q]).T
    gi_ref[...] = nat_f[own, :]
    for ref, i in leaving:
        pltpu.make_async_copy(ref, ref, send_sem.at[i]).wait()


def hand_over(*refs):
    for src, dst in zip(refs[:5], refs[5:]):
        dst[...] = src[...]


def solution(mesh):
    def local_fn(mask_blk, user_emb, item_emb, triples):
        n_u, n_b = mask_blk.shape[0], triples.shape[0]
        half = n_u // 2
        vm = pltpu.VMEM
        outs = (jax.ShapeDtypeStruct((EMB, half), BF16), jax.ShapeDtypeStruct((EMB, EMB), BF16),
                jax.ShapeDtypeStruct((1, 1), F32), jax.ShapeDtypeStruct((EMB, half), F32),
                jax.ShapeDtypeStruct((EMB, EMB), F32))
        tile = (16, 128)
        S = SIDE
        scratch = [
            vm((NCHUNK, n_u, CHUNK), jnp.int32), vm((NCHUNK, n_u, CHUNK), BF16),
            vm((n_u, 128), jnp.int32), vm((n_u, 128), jnp.int32), vm((n_u, 128), F32),
            vm((2, 32, 128), jnp.int32), vm((18, 32, 128), jnp.int32), vm((32, 128), F32),
            vm((STAGES, 2, EMB, half), BF16), vm((STAGES, 2, EMB, half), F32), vm((STAGES, 2, EMB, half), F32),
            vm((2, EMB, half), F32), vm((2, EMB, half), F32),
            vm((S, EMB, EMB), BF16), vm((STAGES, 2, S, S, S) + tile, BF16), vm((STAGES, 2, S, S, S) + tile, F32),
            vm((STAGES, 2, S, S) + tile, F32),
            vm((STAGES, 2, S, 3, S) + tile, F32), vm((STAGES, 2, S * S - 1) + tile, F32),
            vm((2,) + tile, F32), vm((2, S) + tile, F32),
            vm((2, S) + tile, BF16), vm((2, S) + tile, F32), vm((CHUNK, EMB), F32),
            vm((2, 2, S, S, 3) + tile, BF16), vm((2, S, S, 3) + tile, BF16), vm((2, S, S, 3) + tile, BF16),
            vm((2, 3) + tile, BF16), vm((2, S * S - 1, 3) + tile, BF16), vm((2, 3, 3) + tile, BF16),
            vm((2, 2, S, S, 3) + tile, BF16),
            vm((3 * EMB, n_b), BF16), vm((3 * EMB, n_b), BF16),
            vm((3 * EMB, n_u), F32), vm((3 * EMB, CHUNK), F32),
            pltpu.SemaphoreType.DMA((NCHUNK,)), pltpu.SemaphoreType.DMA((NSEM,)), pltpu.SemaphoreType.DMA((NSEM,)),
        ]
        spec = pl.BlockSpec(memory_space=pltpu.VMEM)
        fu, fi, loss, gu, gi = pl.pallas_call(
            kernel,
            out_shape=outs,
            in_specs=[pl.BlockSpec(memory_space=pl.ANY), spec, spec, spec],
            out_specs=(spec,) * 5,
            scratch_shapes=scratch,
            compiler_params=pltpu.CompilerParams(collective_id=0, has_side_effects=True, vmem_limit_bytes=56 * 1024 * 1024),
        )(mask_blk, user_emb.T, item_emb, triples.T)
        args = (fu, fi, loss, gu, gi)
        fu, fi, loss, gu, gi = pl.pallas_call(hand_over, out_shape=outs, in_specs=[spec] * 5, out_specs=(spec,) * 5)(*args)
        return fu.T, fi, loss[0, 0], gu.T, gi

    user_spec = P(('row', 'col'), None)
    item_spec = P(('col', 'row'), None)
    return jax.shard_map(local_fn, mesh=mesh, in_specs=(P('row', 'col'), user_spec, item_spec, P()),
                         out_specs=(user_spec, item_spec, P(), user_spec, item_spec), check_vma=False)
```

```python
import jax
import jax.numpy as jnp
from jax import lax
from jax.experimental import pallas as pl
from jax.experimental.pallas import tpu as pltpu
from jax.sharding import PartitionSpec as P

SIDE = 4
STRIDE = (16, 4, 1)
EMB = 64
CHUNK = 256
NCHUNK = 16
LAYERS = 3
STAGES = 2 * LAYERS
F32 = jnp.float32
BF16 = jnp.bfloat16
NSEM = 160
GATHER_ORDER = (1, 3, 2, 4, 5, 7, 6, 12, 13, 15, 14, 8, 9, 11, 10)
PLANE_ORDER = (10, 6, 9, 11, 14, 5, 7, 13, 15, 2, 8, 1, 3, 4, 12)
NT = (((1,), (1,)), ((), ()))
MESH = pl.DeviceIdType.MESH


def block_rows(part, q):
    return slice(32 * part + 16 * (q // 2), 32 * part + 16 * (q // 2) + 16)


def block_lanes(q):
    return slice(128 * (q % 2), 128 * (q % 2) + 128)


def join_blocks(get):
    rows = []
    for part in range(2):
        for half in range(2):
            rows.append(jnp.concatenate([get(part, 2 * half), get(part, 2 * half + 1)], axis=1))
    return jnp.concatenate(rows, axis=0)


def kernel(mask_hbm, user_ref, item_ref, ids_ref,
           fu_ref, fi_ref, loss_ref, gu_ref, gi_ref,
           mask, adj, rowsum, rowsum_in, scale_u, colsum, colsum_in, scale_i,
           ut, up, up_in, u_acc, s_user,
           nat, it, part_sum, q1, r1, r2, i_acc, s_item,
           fin_b, fin_f, nat_f,
           sel, sel_in, w0, w1, in1, in2, rows_all, grad_u, grad_i, prod_u, prod_i,
           mask_sem, send_sem, recv_sem):
    row = lax.axis_index('row')
    col = lax.axis_index('col')
    pos = (lax.div(row, 16), lax.rem(lax.div(row, 4), 4), lax.rem(row, 4))
    step = [[p] + [lax.rem(p + k, SIDE) for k in range(1, SIDE)] for p in pos]
    offset = [[(step[a][k] - pos[a]) * STRIDE[a] if k else 0 for k in range(SIDE)] for a in range(3)]
    z, y, x = pos
    users = user_ref.shape[1]
    n_batch = ids_ref.shape[1]

    def peer(axis, k):
        return {'row': row + offset[axis][k]}

    partner = {'col': 1 - col}

    copies = []
    for j in range(NCHUNK):
        cp = pltpu.make_async_copy(mask_hbm.at[:, pl.ds(j * CHUNK, CHUNK)], mask.at[j], mask_sem.at[j])
        cp.start()
        copies.append(cp)

    def plane_peer(axes, k):
        return {'row': row + offset[axes[0]][k // SIDE] + offset[axes[1]][k % SIDE]}

    barrier = pltpu.get_barrier_semaphore()
    for axis in range(3):
        for k in range(1, SIDE):
            pl.semaphore_signal(barrier, inc=1, device_id=peer(axis, k), device_id_type=MESH)
    for axes in ((0, 1), (0, 2), (1, 2)):
        for k in range(SIDE * SIDE):
            if k // SIDE and k % SIDE:
                pl.semaphore_signal(barrier, inc=1, device_id=plane_peer(axes, k), device_id_type=MESH)
    pl.semaphore_signal(barrier, inc=1, device_id=partner, device_id_type=MESH)
    pl.semaphore_wait(barrier, 37)

    count = [0, 0]
    leaving = []

    def fresh(n=1):
        out = (count[0], count[1])
        count[0] += 1
        count[1] += n
        return out

    def send(src, dst, device, sems):
        pltpu.make_async_remote_copy(src_ref=src, dst_ref=dst, send_sem=send_sem.at[sems[0]], recv_sem=recv_sem.at[sems[1]],
                                     device_id=device, device_id_type=MESH).start()

    def left(ref, sems):
        leaving.append((ref, sems[0]))

    def arrive(ref, sems):
        pltpu.make_async_copy(ref, ref, recv_sem.at[sems[1]]).wait()

    def plus(sems, n):
        return (sems[0], sems[1] + n)

    def send_axis(axis, src, dst, sems):
        for k in (1, 3, 2):
            send(src(step[axis][k]), dst(k - 1), peer(axis, k), sems)

    def send_plane(axes, src, dst, sems):
        for k in PLANE_ORDER:
            send(src(step[axes[0]][k // SIDE], step[axes[1]][k % SIDE]), dst(k - 1), plane_peer(axes, k), sems)

    ut[0, col] = user_ref[...]
    u_sem = fresh()
    send(ut.at[0, col], ut.at[0, col], partner, u_sem)
    left(ut.at[0, 0], u_sem)
    nat[x] = item_ref[...]
    n_sem = fresh()
    send_axis(2, lambda t: nat.at[x], lambda k: nat.at[x], n_sem)
    left(nat.at[0:3], n_sem)

    rowsum[...] = jnp.zeros_like(rowsum)
    for j in range(NCHUNK):
        copies[j].wait()
        m = mask[j]
        adj[j] = m.astype(F32).astype(BF16)
        rowsum[...] += m[:, :128] + m[:, 128:]
        s = jnp.sum(m, axis=0, keepdims=True)
        colsum[0, 2 * j:2 * j + 1, :] = s[:, :128]
        colsum[0, 2 * j + 1:2 * j + 2, :] = s[:, 128:]
    r_sem, c_sem = fresh(), fresh()
    send(rowsum, rowsum_in, partner, r_sem)
    left(rowsum, r_sem)
    send_axis(0, lambda t: colsum.at[0], lambda k: colsum_in.at[k], c_sem)
    left(colsum_in.at[0:3], c_sem)

    arrive(nat.at[0:3], n_sem)
    chunk0 = jnp.concatenate([nat[k].astype(F32) for k in range(SIDE)], axis=0).T
    for part in range(2):
        for q in range(SIDE):
            it[0, part, z, y, q] = chunk0[block_rows(part, q), block_lanes(q)].astype(BF16)

    stage_sem = [dict(user=fresh(), plane=fresh(SIDE), line=fresh(SIDE), axis=[fresh(SIDE), fresh(SIDE)],
                      last=[fresh(), fresh()]) for _ in range(STAGES)]

    def gather_plane(s):
        sems = stage_sem[s]['plane']
        ref = it.at[s, :, z, y, x]
        for k in GATHER_ORDER:
            send(ref, ref, plane_peer((0, 2), k), plus(sems, k // SIDE))
        left(r2.at[s, 0], sems)

    def gather_line(s):
        sems = stage_sem[s]['plane']
        ref = it.at[s, :, z, y]
        for k in (1, 3, 2):
            send(ref, ref, peer(0, k), plus(sems, k))
        left(it.at[s, :, 0:3, 0], sems)

    def gather_last(s, line=False):
        sems = stage_sem[s]
        for kz in (0, 1, 3, 2):
            ref = it.at[s, :, step[0][(SIDE - kz) % SIDE], y]
            if kz:
                arrive(ref, plus(sems['plane'], kz))
            elif not line:
                arrive(ref.at[:, 0:3], sems['plane'])
            for k in (1, 3, 2):
                send(ref, ref, peer(1, k), plus(sems['line'], k))
        left(r1.at[s, 0], sems['line'])

    gather_line(0)
    arrive(rowsum_in, r_sem)
    deg_u = jnp.maximum(jnp.sum(rowsum[...] + rowsum_in[...], axis=1, keepdims=True), 1)
    scale_u[...] = jnp.broadcast_to(lax.rsqrt(deg_u.astype(F32)), scale_u.shape)
    arrive(colsum_in.at[0:3], c_sem)
    colsum[1] = colsum[0] + colsum_in[0] + colsum_in[1] + colsum_in[2]
    d_sem = fresh()
    send_plane((1, 2), lambda t0, t1: colsum.at[1], lambda k: colsum_in.at[3 + k], d_sem)
    left(colsum_in.at[3:18], d_sem)
    gather_last(0, line=True)
    arrive(colsum_in.at[3:18], d_sem)
    deg_i = jnp.maximum(colsum[1] + jnp.sum(colsum_in[3:], axis=0), 1)
    scale_i[...] = lax.rsqrt(deg_i.astype(F32))
    for j in range(NCHUNK):
        su = scale_u[...]
        for l in range(2):
            lanes = slice(128 * l, 128 * l + 128)
            adj[j, :, lanes] = (su * scale_i[2 * j + l:2 * j + l + 1, :]).astype(BF16) * adj[j, :, lanes]

    def at(ref, axis, t):
        return ref.at[(slice(None),) * axis + (t,)]

    def item_product(s, hold=False):
        lhs = jnp.concatenate([ut[s, 0], ut[s, 1]], axis=1)

        def body(i, _):
            ky = lax.rem(i + 1, SIDE)
            yy = lax.rem(y + ky, SIDE)
            for kz in (2, 1, 3, 0):
                zz = step[0][kz]
                out = jnp.dot(lhs, adj[zz * SIDE + yy], preferred_element_type=F32)
                for part in range(2):
                    for q in range(SIDE):
                        part_sum[s, part, zz, yy, q] = out[block_rows(part, q), block_lanes(q)]
            if not hold:
                scatter_send(s, ky, yy)
            return 0

        lax.fori_loop(0, SIDE, body, 0)
        for p in range(2):
            left(r1.at[s, p], stage_sem[s]['axis'][p])

    def scatter_send(s, ky, yy):
        sems = stage_sem[s]['axis']
        send_axis(0, lambda t: part_sum.at[s, 0, t, yy], lambda k: r1.at[s, 0, ky, k], plus(sems[0], ky))
        send_axis(2, lambda t: part_sum.at[s, 1, :, yy, t], lambda k: r1.at[s, 1, ky, k], plus(sems[1], ky))

    def scatter_mid(s):
        sems = stage_sem[s]

        def piece(ky, yy, off, ks):
            for p in range(2):
                axis = (2, 0)[p]
                arrive(r1.at[s, p, ky], plus(sems['axis'][p], ky))
                own = part_sum[s, 0, z, yy] if p == 0 else part_sum[s, 1, :, yy, x]
                q1[s, p, ky] = own + jnp.sum(r1[s, p, ky], axis=0)
                for k in ks:
                    send(q1.at[s, p, ky, step[axis][k]], r2.at[s, p, 4 * ky + k - 1], {'row': row + off + offset[axis][k]},
                         sems['last'][p])

        def body(ky, _):
            yy = lax.rem(y + ky, SIDE)
            piece(ky, yy, (yy - y) * STRIDE[1], (2, 1, 3, 0))
            return 0

        lax.fori_loop(1, SIDE, body, 0)
        piece(0, y, 0, (2, 1, 3))
        for p in range(2):
            left(r2.at[s, p], sems['last'][p])

    def scatter_end(s):
        out = []
        for p in range(2):
            arrive(r2.at[s, p], stage_sem[s]['last'][p])
            out.append(q1[s, p, 0, pos[(2, 0)[p]]] + jnp.sum(r2[s, p], axis=0))
        return out

    def user_group(s, yy, first):
        acc = None
        for zz in range(SIDE):
            lhs = join_blocks(lambda part, q: it[s, part, zz, yy, q])
            d = lax.dot_general(lhs, adj[zz * SIDE + yy], NT, preferred_element_type=F32)
            acc = d if acc is None else acc + d
        for h in range(2):
            v = acc[:, h * users:(h + 1) * users]
            up[s, h] = v if first else up[s, h] + v

    def user_own(s):
        user_group(s, y, True)

    def user_rest(s):
        def body(k, _):
            yy = lax.rem(y + SIDE - k, SIDE)
            arrive(it.at[s, :, :, yy], plus(stage_sem[s]['line'], k))
            user_group(s, yy, False)
            return 0

        lax.fori_loop(1, SIDE, body, 0)
        sems = stage_sem[s]['user']
        send(up.at[s], up_in.at[s], partner, sems)
        left(up.at[s], sems)

    def user_there(s):
        arrive(up_in.at[s], stage_sem[s]['user'])

    for p in range(2):
        i_acc[p] = it[0, p, z, y, x].astype(F32)
    arrive(ut.at[0, 1 - col], u_sem)
    for h in range(2):
        u_acc[h] = ut[0, h].astype(F32)

    def user_next(s):
        for h in range(2):
            nxt = (up[s, h] + up_in[s, h]).astype(BF16)
            u_acc[h] += nxt.astype(F32)
            if s + 1 < LAYERS:
                ut[s + 1, h] = nxt

    item_product(0)
    user_own(0)
    user_rest(0)
    user_there(0)
    user_next(0)
    item_product(1, hold=True)
    scatter_mid(0)

    def late(i, _):
        ky = lax.rem(i + 1, SIDE)
        scatter_send(1, ky, lax.rem(y + ky, SIDE))
        return 0

    lax.fori_loop(0, SIDE, late, 0)

    def item_next(s):
        new = scatter_end(s)
        for p in range(2):
            nxt = new[p].astype(BF16)
            i_acc[p] += nxt.astype(F32)
            if s + 1 < LAYERS:
                it[s + 1, p, z, y, x] = nxt
        if s + 1 < LAYERS:
            gather_plane(s + 1)

    item_next(0)
    scatter_mid(1)
    gather_last(1)
    user_own(1)
    item_next(1)
    user_rest(1)
    user_there(1)
    user_next(1)
    item_product(2)
    gather_last(2)
    user_own(2)
    scatter_mid(2)
    user_rest(2)
    user_there(2)
    user_next(2)

    tiles = n_batch // CHUNK
    iota = lax.broadcasted_iota(jnp.int32, (users, CHUNK), 0)
    for h in range(2):
        ut[LAYERS, h] = (u_acc[h] * 0.25).astype(BF16)
    own_u = ut[LAYERS, col]
    fu_ref[...] = own_u

    def put_rows(rt, t, picked):
        for l in range(2):
            lt = 2 * t + l
            sel[lt // 8, (lt % 8) // 4, lt % 4, rt // 3, rt % 3] = picked[:, 128 * l:128 * l + 128].astype(BF16)

    base_u = (2 * row + col) * users
    for t in range(tiles):
        ids = ids_ref[0:1, t * CHUNK:(t + 1) * CHUNK]
        hot = jnp.where(iota == ids - base_u, 1.0, 0.0).astype(BF16)
        picked = jnp.dot(own_u, hot, preferred_element_type=F32)
        for r in range(4):
            put_rows(r, t, picked[16 * r:16 * r + 16])
    item_next(2)
    for p in range(2):
        fin_b[p, x] = (i_acc[p] * 0.25).astype(BF16)
    f_sem = fresh()
    send_axis(2, lambda t: fin_b.at[:, x], lambda k: fin_b.at[:, x], f_sem)
    left(fin_b.at[:, 0:3], f_sem)
    base_i = (col * NCHUNK + z * SIDE + y) * CHUNK
    iota_i = lax.broadcasted_iota(jnp.int32, (CHUNK, CHUNK), 0)
    iota_b = lax.broadcasted_iota(jnp.int32, (128, CHUNK), 0)
    x_half, x_side = lax.div(x, 2), lax.rem(x, 2)
    base_b = base_i + 128 * x_side
    own_i = jnp.concatenate([fin_b[0, x], fin_b[1, x]], axis=0)
    for g in range(1, 3):
        for t in range(tiles):
            hot = jnp.where(iota_b == ids_ref[g:g + 1, t * CHUNK:(t + 1) * CHUNK] - base_b, 1.0, 0.0).astype(BF16)
            picked = jnp.dot(own_i, hot, preferred_element_type=F32)
            for part in range(2):
                rows = picked[16 * part:16 * part + 16]
                for half in range(2):
                    put_rows(4 * g + 2 * part + half, t, jnp.where(x_half == half, rows, 0.0))

    x_sem = fresh()
    send(sel.at[1 - col], sel_in, partner, x_sem)
    left(sel_in, x_sem)
    arrive(sel_in, x_sem)
    w0[...] = sel[col] + sel_in[...]
    ax0, ax2 = (0, 2), (2, 0)
    sems = [fresh() for _ in range(2)]
    for p in range(2):
        send_plane((ax0[p], 1), lambda t0, t1: w0.at[p, t0, t1], lambda k: in1.at[p, k], sems[p])
        left(in1.at[p], sems[p])
    arrive(fin_b.at[:, 0:3], f_sem)
    nat_f[...] = join_blocks(lambda part, q: fin_b[part, q]).astype(F32).T
    own = pl.ds(pl.multiple_of(x * EMB, EMB), EMB)
    fi_ref[...] = nat_f[own, :].astype(BF16)
    sems2 = [fresh() for _ in range(2)]
    for p in range(2):
        arrive(in1.at[p], sems[p])
        w1[p] = (w0[p, pos[ax0[p]], y].astype(F32) + jnp.sum(in1[p].astype(F32), axis=0)).astype(BF16)
        send_axis(ax2[p], lambda t: w1.at[p], lambda k: in2.at[p, k], sems2[p])
        left(in2.at[p], sems2[p])
    sems3 = [fresh() for _ in range(2)]
    for p in range(2):
        arrive(in2.at[p], sems2[p])
        a = pos[ax0[p]]
        rows_all[col, p, a, y] = w1[p] + in2[p, 0] + in2[p, 1] + in2[p, 2]
        ref = rows_all.at[col, p, a, y]
        send_plane((ax0[p], 1), lambda t0, t1: ref, lambda k: ref, sems3[p])
        left(in1.at[p], sems3[p])
    for p in range(2):
        arrive(in1.at[p], sems3[p])
    o_sem = fresh()
    send(rows_all.at[col], rows_all.at[col], partner, o_sem)
    left(rows_all.at[0], o_sem)
    arrive(rows_all.at[1 - col], o_sem)

    total = jnp.zeros((1, 128), F32)
    for lt in range(n_batch // 128):
        def rows_of(group):
            return jnp.concatenate([rows_all[lt // 8, (lt % 8) // 4, lt % 4, rt // 3, rt % 3].astype(F32)
                                    for rt in range(4 * group, 4 * group + 4)], axis=0)
        e_user, e_pos, e_neg = rows_of(0), rows_of(1), rows_of(2)
        margin = jnp.sum(e_user * e_pos, axis=0, keepdims=True) - jnp.sum(e_user * e_neg, axis=0, keepdims=True)
        soft = jnp.maximum(-margin, 0.0) + jnp.log1p(jnp.exp(-jnp.abs(margin)))
        total = total + soft
        coef = -jax.nn.sigmoid(-margin) / n_batch
        lanes = slice(lt * 128, lt * 128 + 128)
        for ref, g in ((grad_u, coef * (e_pos - e_neg)), (grad_i, coef * e_user)):
            hi = g.astype(BF16)
            low = g - hi.astype(F32)
            mid = low.astype(BF16)
            ref[0:EMB, lanes] = hi
            ref[EMB:2 * EMB, lanes] = mid
            ref[2 * EMB:3 * EMB, lanes] = (low - mid.astype(F32)).astype(BF16)
    loss_ref[...] = jnp.sum(total, axis=1, keepdims=True) / n_batch

    iota2 = lax.broadcasted_iota(jnp.int32, (2 * users, CHUNK), 0)
    s0 = LAYERS
    prod_u[...] = jnp.zeros_like(prod_u)
    for t in range(tiles):
        cut = slice(t * CHUNK, (t + 1) * CHUNK)
        hot = jnp.where(iota2 == ids_ref[0:1, cut] - row * (2 * users), 1.0, 0.0).astype(BF16)
        prod_u[...] += lax.dot_general(grad_u[:, cut], hot, NT, preferred_element_type=F32)
    seed = (prod_u[0:EMB, :] + prod_u[EMB:2 * EMB, :] + prod_u[2 * EMB:3 * EMB, :]) * 0.25
    for h in range(2):
        s_user[h] = seed[:, h * users:(h + 1) * users]
        ut[s0, h] = seed[:, h * users:(h + 1) * users].astype(BF16)
    item_product(s0)

    def item_seeds(zz, _):
        base = (col * NCHUNK + zz * SIDE + y) * CHUNK
        prod_i[...] = jnp.zeros_like(prod_i)
        for t in range(tiles):
            cut = slice(t * CHUNK, (t + 1) * CHUNK)
            pos_hot = jnp.where(iota_i == ids_ref[1:2, cut] - base, 1.0, 0.0)
            neg_hot = jnp.where(iota_i == ids_ref[2:3, cut] - base, 1.0, 0.0)
            prod_i[...] += lax.dot_general(grad_i[:, cut], (pos_hot - neg_hot).astype(BF16), NT, preferred_element_type=F32)
        seed_i = (prod_i[0:EMB, :] + prod_i[EMB:2 * EMB, :] + prod_i[2 * EMB:3 * EMB, :]) * 0.25
        for part in range(2):
            for q in range(SIDE):
                block = seed_i[block_rows(part, q), block_lanes(q)]
                s_item[zz, part, q] = block
                it[s0, part, zz, y, q] = block.astype(BF16)
        ref = it.at[s0, :, zz, y]
        for k in (1, 3, 2):
            send(ref, ref, peer(1, k), plus(stage_sem[s0]['line'], k))
        return 0

    lax.fori_loop(0, SIDE, item_seeds, 0)
    left(r1.at[s0, 0], stage_sem[s0]['line'])

    for s in range(s0, STAGES):
        if s > s0:
            gather_last(s)
        user_own(s)
        scatter_mid(s)
        user_rest(s)
        new = scatter_end(s)
        for p in range(2):
            nxt = s_item[z, p, x] + new[p]
            if s + 1 < STAGES:
                it[s + 1, p, z, y, x] = nxt.astype(BF16)
            else:
                fin_f[p, x] = nxt
        if s + 1 < STAGES:
            gather_plane(s + 1)
        else:
            e_sem = fresh()
            send_axis(2, lambda t: fin_f.at[:, x], lambda k: fin_f.at[:, x], e_sem)
            left(fin_f.at[:, 0:3], e_sem)
        user_there(s)
        if s + 1 < STAGES:
            for h in range(2):
                ut[s + 1, h] = (s_user[h] + (up[s, h] + up_in[s, h])).astype(BF16)
            item_product(s + 1)
        else:
            gu_ref[...] = s_user[col] + (up[s, col] + up_in[s, col])
    arrive(fin_f.at[:, 0:3], e_sem)
    nat_f[...] = join_blocks(lambda part, q: fin_f[part, q]).T
    gi_ref[...] = nat_f[own, :]
    for ref, i in leaving:
        pltpu.make_async_copy(ref, ref, send_sem.at[i]).wait()


def hand_over(*refs):
    for src, dst in zip(refs[:5], refs[5:]):
        dst[...] = src[...]


def solution(mesh):
    def local_fn(mask_blk, user_emb, item_emb, triples):
        n_u, n_b = mask_blk.shape[0], triples.shape[0]
        half = n_u // 2
        vm = pltpu.VMEM
        outs = (jax.ShapeDtypeStruct((EMB, half), BF16), jax.ShapeDtypeStruct((EMB, EMB), BF16),
                jax.ShapeDtypeStruct((1, 1), F32), jax.ShapeDtypeStruct((EMB, half), F32),
                jax.ShapeDtypeStruct((EMB, EMB), F32))
        tile = (16, 128)
        S = SIDE
        scratch = [
            vm((NCHUNK, n_u, CHUNK), jnp.int32), vm((NCHUNK, n_u, CHUNK), BF16),
            vm((n_u, 128), jnp.int32), vm((n_u, 128), jnp.int32), vm((n_u, 128), F32),
            vm((2, 32, 128), jnp.int32), vm((18, 32, 128), jnp.int32), vm((32, 128), F32),
            vm((STAGES, 2, EMB, half), BF16), vm((STAGES, 2, EMB, half), F32), vm((STAGES, 2, EMB, half), F32),
            vm((2, EMB, half), F32), vm((2, EMB, half), F32),
            vm((S, EMB, EMB), BF16), vm((STAGES, 2, S, S, S) + tile, BF16), vm((STAGES, 2, S, S, S) + tile, F32),
            vm((STAGES, 2, S, S) + tile, F32),
            vm((STAGES, 2, S, 3, S) + tile, F32), vm((STAGES, 2, S * S - 1) + tile, F32),
            vm((2,) + tile, F32), vm((S, 2, S) + tile, F32),
            vm((2, S) + tile, BF16), vm((2, S) + tile, F32), vm((CHUNK, EMB), F32),
            vm((2, 2, S, S, 3) + tile, BF16), vm((2, S, S, 3) + tile, BF16), vm((2, S, S, 3) + tile, BF16),
            vm((2, 3) + tile, BF16), vm((2, S * S - 1, 3) + tile, BF16), vm((2, 3, 3) + tile, BF16),
            vm((2, 2, S, S, 3) + tile, BF16),
            vm((3 * EMB, n_b), BF16), vm((3 * EMB, n_b), BF16),
            vm((3 * EMB, n_u), F32), vm((3 * EMB, CHUNK), F32),
            pltpu.SemaphoreType.DMA((NCHUNK,)), pltpu.SemaphoreType.DMA((NSEM,)), pltpu.SemaphoreType.DMA((NSEM,)),
        ]
        spec = pl.BlockSpec(memory_space=pltpu.VMEM)
        fu, fi, loss, gu, gi = pl.pallas_call(
            kernel,
            out_shape=outs,
            in_specs=[pl.BlockSpec(memory_space=pl.ANY), spec, spec, spec],
            out_specs=(spec,) * 5,
            scratch_shapes=scratch,
            compiler_params=pltpu.CompilerParams(collective_id=0, has_side_effects=True, vmem_limit_bytes=56 * 1024 * 1024),
        )(mask_blk, user_emb.T, item_emb, triples.T)
        args = (fu, fi, loss, gu, gi)
        fu, fi, loss, gu, gi = pl.pallas_call(hand_over, out_shape=outs, in_specs=[spec] * 5, out_specs=(spec,) * 5)(*args)
        return fu.T, fi, loss[0, 0], gu.T, gi

    user_spec = P(('row', 'col'), None)
    item_spec = P(('col', 'row'), None)
    return jax.shard_map(local_fn, mesh=mesh, in_specs=(P('row', 'col'), user_spec, item_spec, P()),
                         out_specs=(user_spec, item_spec, P(), user_spec, item_spec), check_vma=False)
```

```python
import jax
import jax.numpy as jnp
from jax import lax
from jax.experimental import pallas as pl
from jax.experimental.pallas import tpu as pltpu
from jax.sharding import PartitionSpec as P

SIDE = 4
STRIDE = (16, 4, 1)
EMB = 64
CHUNK = 256
NCHUNK = 16
LAYERS = 3
STAGES = 2 * LAYERS
F32 = jnp.float32
BF16 = jnp.bfloat16
NSEM = 160
GATHER_ORDER = (1, 3, 2, 4, 5, 7, 6, 12, 13, 15, 14, 8, 9, 11, 10)
PLANE_ORDER = (10, 6, 9, 11, 14, 5, 7, 13, 15, 2, 8, 1, 3, 4, 12)
NT = (((1,), (1,)), ((), ()))
MESH = pl.DeviceIdType.MESH


def block_rows(part, q):
    return slice(32 * part + 16 * (q // 2), 32 * part + 16 * (q // 2) + 16)


def block_lanes(q):
    return slice(128 * (q % 2), 128 * (q % 2) + 128)


def join_blocks(get):
    rows = []
    for part in range(2):
        for half in range(2):
            rows.append(jnp.concatenate([get(part, 2 * half), get(part, 2 * half + 1)], axis=1))
    return jnp.concatenate(rows, axis=0)


def kernel(mask_hbm, user_ref, item_ref, ids_ref,
           fu_ref, fi_ref, loss_ref, gu_ref, gi_ref,
           mask, adj, rowsum, rowsum_in, scale_u, colsum, colsum_in, scale_i,
           ut, up, up_in, u_acc, s_user,
           nat, it, part_sum, q1, r1, r2, i_acc, s_item,
           fin_b, fin_f, nat_f,
           sel, sel_in, w0, w1, in1, in2, rows_all, grad_u, grad_i, prod_u, prod_i,
           mask_sem, send_sem, recv_sem):
    row = lax.axis_index('row')
    col = lax.axis_index('col')
    pos = (lax.div(row, 16), lax.rem(lax.div(row, 4), 4), lax.rem(row, 4))
    step = [[p] + [lax.rem(p + k, SIDE) for k in range(1, SIDE)] for p in pos]
    offset = [[(step[a][k] - pos[a]) * STRIDE[a] if k else 0 for k in range(SIDE)] for a in range(3)]
    z, y, x = pos
    users = user_ref.shape[1]
    n_batch = ids_ref.shape[1]

    def peer(axis, k):
        return {'row': row + offset[axis][k]}

    partner = {'col': 1 - col}

    copies = []
    for j in range(NCHUNK):
        cp = pltpu.make_async_copy(mask_hbm.at[:, pl.ds(j * CHUNK, CHUNK)], mask.at[j], mask_sem.at[j])
        cp.start()
        copies.append(cp)

    def plane_peer(axes, k):
        return {'row': row + offset[axes[0]][k // SIDE] + offset[axes[1]][k % SIDE]}

    barrier = pltpu.get_barrier_semaphore()
    for axis in range(3):
        for k in range(1, SIDE):
            pl.semaphore_signal(barrier, inc=1, device_id=peer(axis, k), device_id_type=MESH)
    for axes in ((0, 1), (0, 2), (1, 2)):
        for k in range(SIDE * SIDE):
            if k // SIDE and k % SIDE:
                pl.semaphore_signal(barrier, inc=1, device_id=plane_peer(axes, k), device_id_type=MESH)
    pl.semaphore_signal(barrier, inc=1, device_id=partner, device_id_type=MESH)
    pl.semaphore_wait(barrier, 37)

    count = [0, 0]
    leaving = []

    def fresh(n=1):
        out = (count[0], count[1])
        count[0] += 1
        count[1] += n
        return out

    def send(src, dst, device, sems):
        pltpu.make_async_remote_copy(src_ref=src, dst_ref=dst, send_sem=send_sem.at[sems[0]], recv_sem=recv_sem.at[sems[1]],
                                     device_id=device, device_id_type=MESH).start()

    def left(ref, sems):
        leaving.append((ref, sems[0]))

    def arrive(ref, sems):
        pltpu.make_async_copy(ref, ref, recv_sem.at[sems[1]]).wait()

    def plus(sems, n):
        return (sems[0], sems[1] + n)

    def send_axis(axis, src, dst, sems):
        for k in (1, 3, 2):
            send(src(step[axis][k]), dst(k - 1), peer(axis, k), sems)

    def send_plane(axes, src, dst, sems):
        for k in PLANE_ORDER:
            send(src(step[axes[0]][k // SIDE], step[axes[1]][k % SIDE]), dst(k - 1), plane_peer(axes, k), sems)

    ut[0, col] = user_ref[...]
    u_sem = fresh()
    send(ut.at[0, col], ut.at[0, col], partner, u_sem)
    left(ut.at[0, 0], u_sem)
    nat[x] = item_ref[...]
    n_sem = fresh()
    send_axis(2, lambda t: nat.at[x], lambda k: nat.at[x], n_sem)
    left(nat.at[0:3], n_sem)

    rowsum[...] = jnp.zeros_like(rowsum)
    for j in range(NCHUNK):
        copies[j].wait()
        m = mask[j]
        adj[j] = m.astype(F32).astype(BF16)
        rowsum[...] += m[:, :128] + m[:, 128:]
        s = jnp.sum(m, axis=0, keepdims=True)
        colsum[0, 2 * j:2 * j + 1, :] = s[:, :128]
        colsum[0, 2 * j + 1:2 * j + 2, :] = s[:, 128:]
    r_sem, c_sem = fresh(), fresh()
    send(rowsum, rowsum_in, partner, r_sem)
    left(rowsum, r_sem)
    send_axis(0, lambda t: colsum.at[0], lambda k: colsum_in.at[k], c_sem)
    left(colsum_in.at[0:3], c_sem)

    arrive(nat.at[0:3], n_sem)
    chunk0 = jnp.concatenate([nat[k].astype(F32) for k in range(SIDE)], axis=0).T
    for part in range(2):
        for q in range(SIDE):
            it[0, part, z, y, q] = chunk0[block_rows(part, q), block_lanes(q)].astype(BF16)

    stage_sem = [dict(user=fresh(), plane=fresh(SIDE), line=fresh(SIDE), axis=[fresh(SIDE), fresh(SIDE)],
                      last=[fresh(), fresh()]) for _ in range(STAGES)]

    def gather_plane(s):
        sems = stage_sem[s]['plane']
        ref = it.at[s, :, z, y, x]
        for k in GATHER_ORDER:
            send(ref, ref, plane_peer((0, 2), k), plus(sems, k // SIDE))
        left(r2.at[s, 0], sems)

    def gather_line(s):
        sems = stage_sem[s]['plane']
        ref = it.at[s, :, z, y]
        for k in (1, 3, 2):
            send(ref, ref, peer(0, k), plus(sems, k))
        left(it.at[s, :, 0:3, 0], sems)

    def gather_last(s, line=False):
        sems = stage_sem[s]
        for kz in (0, 1, 3, 2):
            ref = it.at[s, :, step[0][(SIDE - kz) % SIDE], y]
            if kz:
                arrive(ref, plus(sems['plane'], kz))
            elif not line:
                arrive(ref.at[:, 0:3], sems['plane'])
            for k in (1, 3, 2):
                send(ref, ref, peer(1, k), plus(sems['line'], k))
        left(r1.at[s, 0], sems['line'])

    gather_line(0)
    arrive(rowsum_in, r_sem)
    deg_u = jnp.maximum(jnp.sum(rowsum[...] + rowsum_in[...], axis=1, keepdims=True), 1)
    scale_u[...] = jnp.broadcast_to(lax.rsqrt(deg_u.astype(F32)), scale_u.shape)
    arrive(colsum_in.at[0:3], c_sem)
    colsum[1] = colsum[0] + colsum_in[0] + colsum_in[1] + colsum_in[2]
    d_sem = fresh()
    send_plane((1, 2), lambda t0, t1: colsum.at[1], lambda k: colsum_in.at[3 + k], d_sem)
    left(colsum_in.at[3:18], d_sem)
    gather_last(0, line=True)
    arrive(colsum_in.at[3:18], d_sem)
    deg_i = jnp.maximum(colsum[1] + jnp.sum(colsum_in[3:], axis=0), 1)
    scale_i[...] = lax.rsqrt(deg_i.astype(F32))
    for j in range(NCHUNK):
        su = scale_u[...]
        for l in range(2):
            lanes = slice(128 * l, 128 * l + 128)
            adj[j, :, lanes] = (su * scale_i[2 * j + l:2 * j + l + 1, :]).astype(BF16) * adj[j, :, lanes]

    def at(ref, axis, t):
        return ref.at[(slice(None),) * axis + (t,)]

    def item_product(s, hold=False):
        lhs = jnp.concatenate([ut[s, 0], ut[s, 1]], axis=1)

        def body(i, _):
            ky = lax.rem(i + 1, SIDE)
            yy = lax.rem(y + ky, SIDE)
            for kz in (2, 1, 3, 0):
                zz = step[0][kz]
                out = jnp.dot(lhs, adj[zz * SIDE + yy], preferred_element_type=F32)
                for part in range(2):
                    for q in range(SIDE):
                        part_sum[s, part, zz, yy, q] = out[block_rows(part, q), block_lanes(q)]
            if not hold:
                scatter_send(s, ky, yy)
            return 0

        lax.fori_loop(0, SIDE, body, 0)
        for p in range(2):
            left(r1.at[s, p], stage_sem[s]['axis'][p])

    def scatter_send(s, ky, yy):
        sems = stage_sem[s]['axis']
        send_axis(0, lambda t: part_sum.at[s, 0, t, yy], lambda k: r1.at[s, 0, ky, k], plus(sems[0], ky))
        send_axis(2, lambda t: part_sum.at[s, 1, :, yy, t], lambda k: r1.at[s, 1, ky, k], plus(sems[1], ky))

    def scatter_mid(s):
        sems = stage_sem[s]

        def piece(ky, yy, off, ks):
            for p in range(2):
                axis = (2, 0)[p]
                arrive(r1.at[s, p, ky], plus(sems['axis'][p], ky))
                own = part_sum[s, 0, z, yy] if p == 0 else part_sum[s, 1, :, yy, x]
                q1[s, p, ky] = own + jnp.sum(r1[s, p, ky], axis=0)
                for k in ks:
                    send(q1.at[s, p, ky, step[axis][k]], r2.at[s, p, 4 * ky + k - 1], {'row': row + off + offset[axis][k]},
                         sems['last'][p])

        def body(ky, _):
            yy = lax.rem(y + ky, SIDE)
            piece(ky, yy, (yy - y) * STRIDE[1], (2, 1, 3, 0))
            return 0

        lax.fori_loop(1, SIDE, body, 0)
        piece(0, y, 0, (2, 1, 3))
        for p in range(2):
            left(r2.at[s, p], sems['last'][p])

    def scatter_end(s):
        out = []
        for p in range(2):
            arrive(r2.at[s, p], stage_sem[s]['last'][p])
            out.append(q1[s, p, 0, pos[(2, 0)[p]]] + jnp.sum(r2[s, p], axis=0))
        return out

    def user_group(s, yy, first):
        acc = None
        for zz in range(SIDE):
            lhs = join_blocks(lambda part, q: it[s, part, zz, yy, q])
            d = lax.dot_general(lhs, adj[zz * SIDE + yy], NT, preferred_element_type=F32)
            acc = d if acc is None else acc + d
        for h in range(2):
            v = acc[:, h * users:(h + 1) * users]
            up[s, h] = v if first else up[s, h] + v

    def user_own(s):
        user_group(s, y, True)

    def user_rest(s):
        def body(i, _):
            k = 1 + lax.rem(2 * i, 3)
            yy = lax.rem(y + SIDE - k, SIDE)
            arrive(it.at[s, :, :, yy], plus(stage_sem[s]['line'], k))
            user_group(s, yy, False)
            return 0

        lax.fori_loop(0, SIDE - 1, body, 0)
        sems = stage_sem[s]['user']
        send(up.at[s], up_in.at[s], partner, sems)
        left(up.at[s], sems)

    def user_there(s):
        arrive(up_in.at[s], stage_sem[s]['user'])

    for p in range(2):
        i_acc[p] = it[0, p, z, y, x].astype(F32)
    arrive(ut.at[0, 1 - col], u_sem)
    for h in range(2):
        u_acc[h] = ut[0, h].astype(F32)

    def user_next(s):
        for h in range(2):
            nxt = (up[s, h] + up_in[s, h]).astype(BF16)
            u_acc[h] += nxt.astype(F32)
            if s + 1 < LAYERS:
                ut[s + 1, h] = nxt

    item_product(0)
    user_own(0)
    user_rest(0)
    user_there(0)
    user_next(0)
    item_product(1, hold=True)
    scatter_mid(0)

    def late(i, _):
        ky = lax.rem(i + 1, SIDE)
        scatter_send(1, ky, lax.rem(y + ky, SIDE))
        return 0

    lax.fori_loop(0, SIDE, late, 0)

    def item_next(s):
        new = scatter_end(s)
        for p in range(2):
            nxt = new[p].astype(BF16)
            i_acc[p] += nxt.astype(F32)
            if s + 1 < LAYERS:
                it[s + 1, p, z, y, x] = nxt
        if s + 1 < LAYERS:
            gather_plane(s + 1)

    item_next(0)
    gather_last(1)
    user_own(1)
    scatter_mid(1)
    item_next(1)
    user_rest(1)
    user_there(1)
    user_next(1)
    item_product(2)
    gather_last(2)
    user_own(2)
    scatter_mid(2)
    user_rest(2)
    user_there(2)
    user_next(2)

    tiles = n_batch // CHUNK
    iota = lax.broadcasted_iota(jnp.int32, (users, CHUNK), 0)
    for h in range(2):
        ut[LAYERS, h] = (u_acc[h] * 0.25).astype(BF16)
    own_u = ut[LAYERS, col]
    fu_ref[...] = own_u

    def put_rows(rt, t, picked):
        for l in range(2):
            lt = 2 * t + l
            sel[lt // 8, (lt % 8) // 4, lt % 4, rt // 3, rt % 3] = picked[:, 128 * l:128 * l + 128].astype(BF16)

    base_u = (2 * row + col) * users
    for t in range(tiles):
        ids = ids_ref[0:1, t * CHUNK:(t + 1) * CHUNK]
        hot = jnp.where(iota == ids - base_u, 1.0, 0.0).astype(BF16)
        picked = jnp.dot(own_u, hot, preferred_element_type=F32)
        for r in range(4):
            put_rows(r, t, picked[16 * r:16 * r + 16])
    item_next(2)
    for p in range(2):
        fin_b[p, x] = (i_acc[p] * 0.25).astype(BF16)
    f_sem = fresh()
    send_axis(2, lambda t: fin_b.at[:, x], lambda k: fin_b.at[:, x], f_sem)
    left(fin_b.at[:, 0:3], f_sem)
    base_i = (col * NCHUNK + z * SIDE + y) * CHUNK
    iota_i = lax.broadcasted_iota(jnp.int32, (CHUNK, CHUNK), 0)
    iota_b = lax.broadcasted_iota(jnp.int32, (128, CHUNK), 0)
    x_half, x_side = lax.div(x, 2), lax.rem(x, 2)
    base_b = base_i + 128 * x_side
    own_i = jnp.concatenate([fin_b[0, x], fin_b[1, x]], axis=0)
    for g in range(1, 3):
        for t in range(tiles):
            hot = jnp.where(iota_b == ids_ref[g:g + 1, t * CHUNK:(t + 1) * CHUNK] - base_b, 1.0, 0.0).astype(BF16)
            picked = jnp.dot(own_i, hot, preferred_element_type=F32)
            for part in range(2):
                rows = picked[16 * part:16 * part + 16]
                for half in range(2):
                    put_rows(4 * g + 2 * part + half, t, jnp.where(x_half == half, rows, 0.0))

    x_sem = fresh()
    send(sel.at[1 - col], sel_in, partner, x_sem)
    left(sel_in, x_sem)
    arrive(sel_in, x_sem)
    w0[...] = sel[col] + sel_in[...]
    ax0, ax2 = (0, 2), (2, 0)
    sems = [fresh() for _ in range(2)]
    for p in range(2):
        send_plane((ax0[p], 1), lambda t0, t1: w0.at[p, t0, t1], lambda k: in1.at[p, k], sems[p])
        left(in1.at[p], sems[p])
    arrive(fin_b.at[:, 0:3], f_sem)
    nat_f[...] = join_blocks(lambda part, q: fin_b[part, q]).astype(F32).T
    own = pl.ds(pl.multiple_of(x * EMB, EMB), EMB)
    fi_ref[...] = nat_f[own, :].astype(BF16)
    sems2 = [fresh() for _ in range(2)]
    for p in range(2):
        arrive(in1.at[p], sems[p])
        w1[p] = (w0[p, pos[ax0[p]], y].astype(F32) + jnp.sum(in1[p].astype(F32), axis=0)).astype(BF16)
        send_axis(ax2[p], lambda t: w1.at[p], lambda k: in2.at[p, k], sems2[p])
        left(in2.at[p], sems2[p])
    sems3 = [fresh() for _ in range(2)]
    for p in range(2):
        arrive(in2.at[p], sems2[p])
        a = pos[ax0[p]]
        rows_all[col, p, a, y] = w1[p] + in2[p, 0] + in2[p, 1] + in2[p, 2]
        ref = rows_all.at[col, p, a, y]
        send_plane((ax0[p], 1), lambda t0, t1: ref, lambda k: ref, sems3[p])
        left(in1.at[p], sems3[p])
    for p in range(2):
        arrive(in1.at[p], sems3[p])
    o_sem = fresh()
    send(rows_all.at[col], rows_all.at[col], partner, o_sem)
    left(rows_all.at[0], o_sem)
    arrive(rows_all.at[1 - col], o_sem)

    total = jnp.zeros((1, 128), F32)
    for lt in range(n_batch // 128):
        def rows_of(group):
            return jnp.concatenate([rows_all[lt // 8, (lt % 8) // 4, lt % 4, rt // 3, rt % 3].astype(F32)
                                    for rt in range(4 * group, 4 * group + 4)], axis=0)
        e_user, e_pos, e_neg = rows_of(0), rows_of(1), rows_of(2)
        margin = jnp.sum(e_user * e_pos, axis=0, keepdims=True) - jnp.sum(e_user * e_neg, axis=0, keepdims=True)
        soft = jnp.maximum(-margin, 0.0) + jnp.log1p(jnp.exp(-jnp.abs(margin)))
        total = total + soft
        coef = -jax.nn.sigmoid(-margin) / n_batch
        lanes = slice(lt * 128, lt * 128 + 128)
        for ref, g in ((grad_u, coef * (e_pos - e_neg)), (grad_i, coef * e_user)):
            hi = g.astype(BF16)
            low = g - hi.astype(F32)
            mid = low.astype(BF16)
            ref[0:EMB, lanes] = hi
            ref[EMB:2 * EMB, lanes] = mid
            ref[2 * EMB:3 * EMB, lanes] = (low - mid.astype(F32)).astype(BF16)
    loss_ref[...] = jnp.sum(total, axis=1, keepdims=True) / n_batch

    iota2 = lax.broadcasted_iota(jnp.int32, (2 * users, CHUNK), 0)
    s0 = LAYERS
    prod_u[...] = jnp.zeros_like(prod_u)
    for t in range(tiles):
        cut = slice(t * CHUNK, (t + 1) * CHUNK)
        hot = jnp.where(iota2 == ids_ref[0:1, cut] - row * (2 * users), 1.0, 0.0).astype(BF16)
        prod_u[...] += lax.dot_general(grad_u[:, cut], hot, NT, preferred_element_type=F32)
    seed = (prod_u[0:EMB, :] + prod_u[EMB:2 * EMB, :] + prod_u[2 * EMB:3 * EMB, :]) * 0.25
    for h in range(2):
        s_user[h] = seed[:, h * users:(h + 1) * users]
        ut[s0, h] = seed[:, h * users:(h + 1) * users].astype(BF16)
    item_product(s0)

    def item_seeds(zz, _):
        base = (col * NCHUNK + zz * SIDE + y) * CHUNK
        prod_i[...] = jnp.zeros_like(prod_i)
        for t in range(tiles):
            cut = slice(t * CHUNK, (t + 1) * CHUNK)
            pos_hot = jnp.where(iota_i == ids_ref[1:2, cut] - base, 1.0, 0.0)
            neg_hot = jnp.where(iota_i == ids_ref[2:3, cut] - base, 1.0, 0.0)
            prod_i[...] += lax.dot_general(grad_i[:, cut], (pos_hot - neg_hot).astype(BF16), NT, preferred_element_type=F32)
        seed_i = (prod_i[0:EMB, :] + prod_i[EMB:2 * EMB, :] + prod_i[2 * EMB:3 * EMB, :]) * 0.25
        for part in range(2):
            for q in range(SIDE):
                block = seed_i[block_rows(part, q), block_lanes(q)]
                s_item[zz, part, q] = block
                it[s0, part, zz, y, q] = block.astype(BF16)
        ref = it.at[s0, :, zz, y]
        for k in (1, 3, 2):
            send(ref, ref, peer(1, k), plus(stage_sem[s0]['line'], k))
        return 0

    lax.fori_loop(0, SIDE, item_seeds, 0)
    left(r1.at[s0, 0], stage_sem[s0]['line'])

    for s in range(s0, STAGES):
        if s > s0:
            gather_last(s)
        user_own(s)
        scatter_mid(s)
        user_rest(s)
        new = scatter_end(s)
        for p in range(2):
            nxt = s_item[z, p, x] + new[p]
            if s + 1 < STAGES:
                it[s + 1, p, z, y, x] = nxt.astype(BF16)
            else:
                fin_f[p, x] = nxt
        if s + 1 < STAGES:
            gather_plane(s + 1)
        else:
            e_sem = fresh()
            send_axis(2, lambda t: fin_f.at[:, x], lambda k: fin_f.at[:, x], e_sem)
            left(fin_f.at[:, 0:3], e_sem)
        user_there(s)
        if s + 1 < STAGES:
            for h in range(2):
                ut[s + 1, h] = (s_user[h] + (up[s, h] + up_in[s, h])).astype(BF16)
            item_product(s + 1)
        else:
            gu_ref[...] = s_user[col] + (up[s, col] + up_in[s, col])
    arrive(fin_f.at[:, 0:3], e_sem)
    nat_f[...] = join_blocks(lambda part, q: fin_f[part, q]).T
    gi_ref[...] = nat_f[own, :]
    for ref, i in leaving:
        pltpu.make_async_copy(ref, ref, send_sem.at[i]).wait()


def hand_over(*refs):
    for src, dst in zip(refs[:5], refs[5:]):
        dst[...] = src[...]


def solution(mesh):
    def local_fn(mask_blk, user_emb, item_emb, triples):
        n_u, n_b = mask_blk.shape[0], triples.shape[0]
        half = n_u // 2
        vm = pltpu.VMEM
        outs = (jax.ShapeDtypeStruct((EMB, half), BF16), jax.ShapeDtypeStruct((EMB, EMB), BF16),
                jax.ShapeDtypeStruct((1, 1), F32), jax.ShapeDtypeStruct((EMB, half), F32),
                jax.ShapeDtypeStruct((EMB, EMB), F32))
        tile = (16, 128)
        S = SIDE
        scratch = [
            vm((NCHUNK, n_u, CHUNK), jnp.int32), vm((NCHUNK, n_u, CHUNK), BF16),
            vm((n_u, 128), jnp.int32), vm((n_u, 128), jnp.int32), vm((n_u, 128), F32),
            vm((2, 32, 128), jnp.int32), vm((18, 32, 128), jnp.int32), vm((32, 128), F32),
            vm((STAGES, 2, EMB, half), BF16), vm((STAGES, 2, EMB, half), F32), vm((STAGES, 2, EMB, half), F32),
            vm((2, EMB, half), F32), vm((2, EMB, half), F32),
            vm((S, EMB, EMB), BF16), vm((STAGES, 2, S, S, S) + tile, BF16), vm((STAGES, 2, S, S, S) + tile, F32),
            vm((STAGES, 2, S, S) + tile, F32),
            vm((STAGES, 2, S, 3, S) + tile, F32), vm((STAGES, 2, S * S - 1) + tile, F32),
            vm((2,) + tile, F32), vm((S, 2, S) + tile, F32),
            vm((2, S) + tile, BF16), vm((2, S) + tile, F32), vm((CHUNK, EMB), F32),
            vm((2, 2, S, S, 3) + tile, BF16), vm((2, S, S, 3) + tile, BF16), vm((2, S, S, 3) + tile, BF16),
            vm((2, 3) + tile, BF16), vm((2, S * S - 1, 3) + tile, BF16), vm((2, 3, 3) + tile, BF16),
            vm((2, 2, S, S, 3) + tile, BF16),
            vm((3 * EMB, n_b), BF16), vm((3 * EMB, n_b), BF16),
            vm((3 * EMB, n_u), F32), vm((3 * EMB, CHUNK), F32),
            pltpu.SemaphoreType.DMA((NCHUNK,)), pltpu.SemaphoreType.DMA((NSEM,)), pltpu.SemaphoreType.DMA((NSEM,)),
        ]
        spec = pl.BlockSpec(memory_space=pltpu.VMEM)
        fu, fi, loss, gu, gi = pl.pallas_call(
            kernel,
            out_shape=outs,
            in_specs=[pl.BlockSpec(memory_space=pltpu.HBM), spec, spec, spec],
            out_specs=(spec,) * 5,
            scratch_shapes=scratch,
            compiler_params=pltpu.CompilerParams(collective_id=0, has_side_effects=True, vmem_limit_bytes=52 * 1024 * 1024),
        )(mask_blk, user_emb.T, item_emb, triples.T)
        args = (fu, fi, loss, gu, gi)
        fu, fi, loss, gu, gi = pl.pallas_call(hand_over, out_shape=outs, in_specs=[spec] * 5, out_specs=(spec,) * 5,
                                             compiler_params=pltpu.CompilerParams(vmem_limit_bytes=4 * 1024 * 1024))(*args)
        return fu.T, fi, loss[0, 0], gu.T, gi

    user_spec = P(('row', 'col'), None)
    item_spec = P(('col', 'row'), None)
    return jax.shard_map(local_fn, mesh=mesh, in_specs=(P('row', 'col'), user_spec, item_spec, P()),
                         out_specs=(user_spec, item_spec, P(), user_spec, item_spec), check_vma=False)
```

```python
import jax
import jax.numpy as jnp
from jax import lax
from jax.experimental import pallas as pl
from jax.experimental.pallas import tpu as pltpu
from jax.sharding import PartitionSpec as P

SIDE = 4
STRIDE = (16, 4, 1)
EMB = 64
CHUNK = 256
NCHUNK = 16
LAYERS = 3
STAGES = 2 * LAYERS
F32 = jnp.float32
BF16 = jnp.bfloat16
NSEM = 160
GATHER_ORDER = (1, 3, 2, 4, 5, 7, 6, 12, 13, 15, 14, 8, 9, 11, 10)
PLANE_ORDER = (10, 6, 9, 11, 14, 5, 7, 13, 15, 2, 8, 1, 3, 4, 12)
NT = (((1,), (1,)), ((), ()))
MESH = pl.DeviceIdType.MESH


def block_rows(part, q):
    return slice(32 * part + 16 * (q // 2), 32 * part + 16 * (q // 2) + 16)


def block_lanes(q):
    return slice(128 * (q % 2), 128 * (q % 2) + 128)


def join_blocks(get):
    rows = []
    for part in range(2):
        for half in range(2):
            rows.append(jnp.concatenate([get(part, 2 * half), get(part, 2 * half + 1)], axis=1))
    return jnp.concatenate(rows, axis=0)


def kernel(mask_hbm, user_hbm, item_hbm, ids_hbm,
           fu_ref, fi_ref, loss_ref, gu_ref, gi_ref,
           mask, adj, rowsum, rowsum_in, scale_u, colsum, colsum_in, scale_i,
           ut, up, up_in, u_acc, s_user,
           nat, it, part_sum, q1, r1, r2, i_acc, s_item,
           fin_b, fin_f, nat_f,
           sel, sel_in, w0, w1, in1, in2, rows_all, grad_u, grad_i, prod_u, prod_i,
           user_ref, item_ref, ids_ref, mask_sem, send_sem, recv_sem):
    row = lax.axis_index('row')
    col = lax.axis_index('col')
    pos = (lax.div(row, 16), lax.rem(lax.div(row, 4), 4), lax.rem(row, 4))
    step = [[p] + [lax.rem(p + k, SIDE) for k in range(1, SIDE)] for p in pos]
    offset = [[(step[a][k] - pos[a]) * STRIDE[a] if k else 0 for k in range(SIDE)] for a in range(3)]
    z, y, x = pos
    users = user_ref.shape[1]
    n_batch = ids_ref.shape[1]

    def peer(axis, k):
        return {'row': row + offset[axis][k]}

    partner = {'col': 1 - col}

    small = []
    for i, (src, dst) in enumerate(((user_hbm, user_ref), (item_hbm, item_ref), (ids_hbm, ids_ref))):
        cp = pltpu.make_async_copy(src, dst, mask_sem.at[NCHUNK + i])
        cp.start()
        small.append(cp)
    copies = []
    for j in range(NCHUNK):
        cp = pltpu.make_async_copy(mask_hbm.at[:, pl.ds(j * CHUNK, CHUNK)], mask.at[j], mask_sem.at[j])
        cp.start()
        copies.append(cp)

    def plane_peer(axes, k):
        return {'row': row + offset[axes[0]][k // SIDE] + offset[axes[1]][k % SIDE]}

    barrier = pltpu.get_barrier_semaphore()
    for axis in range(3):
        for k in range(1, SIDE):
            pl.semaphore_signal(barrier, inc=1, device_id=peer(axis, k), device_id_type=MESH)
    for axes in ((0, 1), (0, 2), (1, 2)):
        for k in range(SIDE * SIDE):
            if k // SIDE and k % SIDE:
                pl.semaphore_signal(barrier, inc=1, device_id=plane_peer(axes, k), device_id_type=MESH)
    pl.semaphore_signal(barrier, inc=1, device_id=partner, device_id_type=MESH)
    pl.semaphore_wait(barrier, 37)

    count = [0, 0]
    leaving = []

    def fresh(n=1):
        out = (count[0], count[1])
        count[0] += 1
        count[1] += n
        return out

    def send(src, dst, device, sems):
        pltpu.make_async_remote_copy(src_ref=src, dst_ref=dst, send_sem=send_sem.at[sems[0]], recv_sem=recv_sem.at[sems[1]],
                                     device_id=device, device_id_type=MESH).start()

    def left(ref, sems):
        leaving.append((ref, sems[0]))

    def arrive(ref, sems):
        pltpu.make_async_copy(ref, ref, recv_sem.at[sems[1]]).wait()

    def plus(sems, n):
        return (sems[0], sems[1] + n)

    def send_axis(axis, src, dst, sems):
        for k in (1, 3, 2):
            send(src(step[axis][k]), dst(k - 1), peer(axis, k), sems)

    def send_plane(axes, src, dst, sems):
        for k in PLANE_ORDER:
            send(src(step[axes[0]][k // SIDE], step[axes[1]][k % SIDE]), dst(k - 1), plane_peer(axes, k), sems)

    for cp in small:
        cp.wait()
    ut[0, col] = user_ref[...]
    u_sem = fresh()
    send(ut.at[0, col], ut.at[0, col], partner, u_sem)
    left(ut.at[0, 0], u_sem)
    nat[x] = item_ref[...]
    n_sem = fresh()
    send_axis(2, lambda t: nat.at[x], lambda k: nat.at[x], n_sem)
    left(nat.at[0:3], n_sem)

    rowsum[...] = jnp.zeros_like(rowsum)
    for j in range(NCHUNK):
        copies[j].wait()
        m = mask[j]
        adj[j] = m.astype(F32).astype(BF16)
        rowsum[...] += m[:, :128] + m[:, 128:]
        s = jnp.sum(m, axis=0, keepdims=True)
        colsum[0, 2 * j:2 * j + 1, :] = s[:, :128]
        colsum[0, 2 * j + 1:2 * j + 2, :] = s[:, 128:]
    r_sem, c_sem = fresh(), fresh()
    send(rowsum, rowsum_in, partner, r_sem)
    left(rowsum, r_sem)
    send_axis(0, lambda t: colsum.at[0], lambda k: colsum_in.at[k], c_sem)
    left(colsum_in.at[0:3], c_sem)

    arrive(nat.at[0:3], n_sem)
    chunk0 = jnp.concatenate([nat[k].astype(F32) for k in range(SIDE)], axis=0).T
    for part in range(2):
        for q in range(SIDE):
            it[0, part, z, y, q] = chunk0[block_rows(part, q), block_lanes(q)].astype(BF16)

    stage_sem = [dict(user=fresh(), plane=fresh(SIDE), line=fresh(SIDE), axis=[fresh(SIDE), fresh(SIDE)],
                      last=[fresh(), fresh()]) for _ in range(STAGES)]

    def gather_plane(s):
        sems = stage_sem[s]['plane']
        ref = it.at[s, :, z, y, x]
        for k in GATHER_ORDER:
            send(ref, ref, plane_peer((0, 2), k), plus(sems, k // SIDE))
        left(r2.at[s, 0], sems)

    def gather_line(s):
        sems = stage_sem[s]['plane']
        ref = it.at[s, :, z, y]
        for k in (1, 3, 2):
            send(ref, ref, peer(0, k), plus(sems, k))
        left(it.at[s, :, 0:3, 0], sems)

    def gather_last(s, line=False):
        sems = stage_sem[s]
        for kz in (0, 1, 3, 2):
            ref = it.at[s, :, step[0][(SIDE - kz) % SIDE], y]
            if kz:
                arrive(ref, plus(sems['plane'], kz))
            elif not line:
                arrive(ref.at[:, 0:3], sems['plane'])
            for k in (1, 3, 2):
                send(ref, ref, peer(1, k), plus(sems['line'], k))
        left(r1.at[s, 0], sems['line'])

    gather_line(0)
    arrive(rowsum_in, r_sem)
    deg_u = jnp.maximum(jnp.sum(rowsum[...] + rowsum_in[...], axis=1, keepdims=True), 1)
    scale_u[...] = jnp.broadcast_to(lax.rsqrt(deg_u.astype(F32)), scale_u.shape)
    arrive(colsum_in.at[0:3], c_sem)
    colsum[1] = colsum[0] + colsum_in[0] + colsum_in[1] + colsum_in[2]
    d_sem = fresh()
    send_plane((1, 2), lambda t0, t1: colsum.at[1], lambda k: colsum_in.at[3 + k], d_sem)
    left(colsum_in.at[3:18], d_sem)
    gather_last(0, line=True)
    arrive(colsum_in.at[3:18], d_sem)
    deg_i = jnp.maximum(colsum[1] + jnp.sum(colsum_in[3:], axis=0), 1)
    scale_i[...] = lax.rsqrt(deg_i.astype(F32))
    for j in range(NCHUNK):
        su = scale_u[...]
        for l in range(2):
            lanes = slice(128 * l, 128 * l + 128)
            adj[j, :, lanes] = (su * scale_i[2 * j + l:2 * j + l + 1, :]).astype(BF16) * adj[j, :, lanes]

    def at(ref, axis, t):
        return ref.at[(slice(None),) * axis + (t,)]

    def item_product(s, hold=False):
        lhs = jnp.concatenate([ut[s, 0], ut[s, 1]], axis=1)

        def body(i, _):
            ky = lax.rem(i + 1, SIDE)
            yy = lax.rem(y + ky, SIDE)
            for kz in (2, 1, 3, 0):
                zz = step[0][kz]
                out = jnp.dot(lhs, adj[zz * SIDE + yy], preferred_element_type=F32)
                for part in range(2):
                    for q in range(SIDE):
                        part_sum[s, part, zz, yy, q] = out[block_rows(part, q), block_lanes(q)]
            if not hold:
                scatter_send(s, ky, yy)
            return 0

        lax.fori_loop(0, SIDE, body, 0)
        for p in range(2):
            left(r1.at[s, p], stage_sem[s]['axis'][p])

    def scatter_send(s, ky, yy):
        sems = stage_sem[s]['axis']
        send_axis(0, lambda t: part_sum.at[s, 0, t, yy], lambda k: r1.at[s, 0, ky, k], plus(sems[0], ky))
        send_axis(2, lambda t: part_sum.at[s, 1, :, yy, t], lambda k: r1.at[s, 1, ky, k], plus(sems[1], ky))

    def scatter_mid(s, between=None):
        sems = stage_sem[s]

        def piece(ky, yy, off, ks):
            for p in range(2):
                axis = (2, 0)[p]
                arrive(r1.at[s, p, ky], plus(sems['axis'][p], ky))
                own = part_sum[s, 0, z, yy] if p == 0 else part_sum[s, 1, :, yy, x]
                q1[s, p, ky] = own + jnp.sum(r1[s, p, ky], axis=0)
                for k in ks:
                    send(q1.at[s, p, ky, step[axis][k]], r2.at[s, p, 4 * ky + k - 1], {'row': row + off + offset[axis][k]},
                         sems['last'][p])

        def body(ky, _):
            yy = lax.rem(y + ky, SIDE)
            piece(ky, yy, (yy - y) * STRIDE[1], (2, 1, 3, 0))
            return 0

        lax.fori_loop(1, SIDE, body, 0)
        if between:
            between()
        piece(0, y, 0, (2, 1, 3))
        for p in range(2):
            left(r2.at[s, p], sems['last'][p])

    def scatter_end(s):
        out = []
        for p in range(2):
            arrive(r2.at[s, p], stage_sem[s]['last'][p])
            out.append(q1[s, p, 0, pos[(2, 0)[p]]] + jnp.sum(r2[s, p], axis=0))
        return out

    def user_group(s, yy, first):
        acc = None
        for zz in range(SIDE):
            lhs = join_blocks(lambda part, q: it[s, part, zz, yy, q])
            d = lax.dot_general(lhs, adj[zz * SIDE + yy], NT, preferred_element_type=F32)
            acc = d if acc is None else acc + d
        for h in range(2):
            v = acc[:, h * users:(h + 1) * users]
            up[s, h] = v if first else up[s, h] + v

    def user_own(s):
        user_group(s, y, True)

    def user_rest(s):
        def body(i, _):
            k = 1 + lax.rem(2 * i, 3)
            yy = lax.rem(y + SIDE - k, SIDE)
            arrive(it.at[s, :, :, yy], plus(stage_sem[s]['line'], k))
            user_group(s, yy, False)
            return 0

        lax.fori_loop(0, SIDE - 1, body, 0)
        sems = stage_sem[s]['user']
        send(up.at[s], up_in.at[s], partner, sems)
        left(up.at[s], sems)

    def user_there(s):
        arrive(up_in.at[s], stage_sem[s]['user'])

    for p in range(2):
        i_acc[p] = it[0, p, z, y, x].astype(F32)
    arrive(ut.at[0, 1 - col], u_sem)
    for h in range(2):
        u_acc[h] = ut[0, h].astype(F32)

    def user_next(s):
        for h in range(2):
            nxt = (up[s, h] + up_in[s, h]).astype(BF16)
            u_acc[h] += nxt.astype(F32)
            if s + 1 < LAYERS:
                ut[s + 1, h] = nxt

    item_product(0)
    user_own(0)
    user_rest(0)
    user_there(0)
    user_next(0)
    item_product(1, hold=True)
    scatter_mid(0)

    def late(i, _):
        ky = lax.rem(i + 1, SIDE)
        scatter_send(1, ky, lax.rem(y + ky, SIDE))
        return 0

    lax.fori_loop(0, SIDE, late, 0)

    def item_next(s):
        new = scatter_end(s)
        for p in range(2):
            nxt = new[p].astype(BF16)
            i_acc[p] += nxt.astype(F32)
            if s + 1 < LAYERS:
                it[s + 1, p, z, y, x] = nxt
        if s + 1 < LAYERS:
            gather_plane(s + 1)

    item_next(0)
    scatter_mid(1, lambda: gather_last(1))
    user_own(1)
    item_next(1)
    user_rest(1)
    user_there(1)
    user_next(1)
    item_product(2)
    gather_last(2)
    user_own(2)
    scatter_mid(2)
    user_rest(2)
    user_there(2)
    user_next(2)

    tiles = n_batch // CHUNK
    iota = lax.broadcasted_iota(jnp.int32, (users, CHUNK), 0)
    for h in range(2):
        ut[LAYERS, h] = (u_acc[h] * 0.25).astype(BF16)
    own_u = ut[LAYERS, col]
    fu_ref[...] = own_u

    def put_rows(rt, t, picked):
        for l in range(2):
            lt = 2 * t + l
            sel[lt // 8, (lt % 8) // 4, lt % 4, rt // 3, rt % 3] = picked[:, 128 * l:128 * l + 128].astype(BF16)

    base_u = (2 * row + col) * users
    for t in range(tiles):
        ids = ids_ref[0:1, t * CHUNK:(t + 1) * CHUNK]
        hot = jnp.where(iota == ids - base_u, 1.0, 0.0).astype(BF16)
        picked = jnp.dot(own_u, hot, preferred_element_type=F32)
        for r in range(4):
            put_rows(r, t, picked[16 * r:16 * r + 16])
    item_next(2)
    for p in range(2):
        fin_b[p, x] = (i_acc[p] * 0.25).astype(BF16)
    f_sem = fresh()
    send_axis(2, lambda t: fin_b.at[:, x], lambda k: fin_b.at[:, x], f_sem)
    left(fin_b.at[:, 0:3], f_sem)
    base_i = (col * NCHUNK + z * SIDE + y) * CHUNK
    iota_i = lax.broadcasted_iota(jnp.int32, (CHUNK, CHUNK), 0)
    iota_b = lax.broadcasted_iota(jnp.int32, (128, CHUNK), 0)
    x_half, x_side = lax.div(x, 2), lax.rem(x, 2)
    base_b = base_i + 128 * x_side
    own_i = jnp.concatenate([fin_b[0, x], fin_b[1, x]], axis=0)
    for g in range(1, 3):
        for t in range(tiles):
            hot = jnp.where(iota_b == ids_ref[g:g + 1, t * CHUNK:(t + 1) * CHUNK] - base_b, 1.0, 0.0).astype(BF16)
            picked = jnp.dot(own_i, hot, preferred_element_type=F32)
            for part in range(2):
                rows = picked[16 * part:16 * part + 16]
                for half in range(2):
                    put_rows(4 * g + 2 * part + half, t, jnp.where(x_half == half, rows, 0.0))

    x_sem = fresh()
    send(sel.at[1 - col], sel_in, partner, x_sem)
    left(sel_in, x_sem)
    arrive(sel_in, x_sem)
    w0[...] = sel[col] + sel_in[...]
    ax0, ax2 = (0, 2), (2, 0)
    sems = [fresh() for _ in range(2)]
    for p in range(2):
        send_plane((ax0[p], 1), lambda t0, t1: w0.at[p, t0, t1], lambda k: in1.at[p, k], sems[p])
        left(in1.at[p], sems[p])
    arrive(fin_b.at[:, 0:3], f_sem)
    nat_f[...] = join_blocks(lambda part, q: fin_b[part, q]).astype(F32).T
    own = pl.ds(pl.multiple_of(x * EMB, EMB), EMB)
    fi_ref[...] = nat_f[own, :].astype(BF16)
    sems2 = [fresh() for _ in range(2)]
    for p in range(2):
        arrive(in1.at[p], sems[p])
        w1[p] = (w0[p, pos[ax0[p]], y].astype(F32) + jnp.sum(in1[p].astype(F32), axis=0)).astype(BF16)
        send_axis(ax2[p], lambda t: w1.at[p], lambda k: in2.at[p, k], sems2[p])
        left(in2.at[p], sems2[p])
    sems3 = [fresh() for _ in range(2)]
    for p in range(2):
        arrive(in2.at[p], sems2[p])
        a = pos[ax0[p]]
        rows_all[col, p, a, y] = w1[p] + in2[p, 0] + in2[p, 1] + in2[p, 2]
        ref = rows_all.at[col, p, a, y]
        send_plane((ax0[p], 1), lambda t0, t1: ref, lambda k: ref, sems3[p])
        left(in1.at[p], sems3[p])
    for p in range(2):
        arrive(in1.at[p], sems3[p])
    o_sem = fresh()
    send(rows_all.at[col], rows_all.at[col], partner, o_sem)
    left(rows_all.at[0], o_sem)
    arrive(rows_all.at[1 - col], o_sem)

    total = jnp.zeros((1, 128), F32)
    for lt in range(n_batch // 128):
        def rows_of(group):
            return jnp.concatenate([rows_all[lt // 8, (lt % 8) // 4, lt % 4, rt // 3, rt % 3].astype(F32)
                                    for rt in range(4 * group, 4 * group + 4)], axis=0)
        e_user, e_pos, e_neg = rows_of(0), rows_of(1), rows_of(2)
        margin = jnp.sum(e_user * e_pos, axis=0, keepdims=True) - jnp.sum(e_user * e_neg, axis=0, keepdims=True)
        soft = jnp.maximum(-margin, 0.0) + jnp.log1p(jnp.exp(-jnp.abs(margin)))
        total = total + soft
        coef = -jax.nn.sigmoid(-margin) / n_batch
        lanes = slice(lt * 128, lt * 128 + 128)
        for ref, g in ((grad_u, coef * (e_pos - e_neg)), (grad_i, coef * e_user)):
            hi = g.astype(BF16)
            low = g - hi.astype(F32)
            mid = low.astype(BF16)
            ref[0:EMB, lanes] = hi
            ref[EMB:2 * EMB, lanes] = mid
            ref[2 * EMB:3 * EMB, lanes] = (low - mid.astype(F32)).astype(BF16)
    loss_ref[...] = jnp.sum(total, axis=1, keepdims=True) / n_batch

    iota2 = lax.broadcasted_iota(jnp.int32, (2 * users, CHUNK), 0)
    s0 = LAYERS
    prod_u[...] = jnp.zeros_like(prod_u)
    for t in range(tiles):
        cut = slice(t * CHUNK, (t + 1) * CHUNK)
        hot = jnp.where(iota2 == ids_ref[0:1, cut] - row * (2 * users), 1.0, 0.0).astype(BF16)
        prod_u[...] += lax.dot_general(grad_u[:, cut], hot, NT, preferred_element_type=F32)
    seed = (prod_u[0:EMB, :] + prod_u[EMB:2 * EMB, :] + prod_u[2 * EMB:3 * EMB, :]) * 0.25
    for h in range(2):
        s_user[h] = seed[:, h * users:(h + 1) * users]
        ut[s0, h] = seed[:, h * users:(h + 1) * users].astype(BF16)
    item_product(s0)

    def item_seeds(zz, _):
        base = (col * NCHUNK + zz * SIDE + y) * CHUNK
        prod_i[...] = jnp.zeros_like(prod_i)
        for t in range(tiles):
            cut = slice(t * CHUNK, (t + 1) * CHUNK)
            pos_hot = jnp.where(iota_i == ids_ref[1:2, cut] - base, 1.0, 0.0)
            neg_hot = jnp.where(iota_i == ids_ref[2:3, cut] - base, 1.0, 0.0)
            prod_i[...] += lax.dot_general(grad_i[:, cut], (pos_hot - neg_hot).astype(BF16), NT, preferred_element_type=F32)
        seed_i = (prod_i[0:EMB, :] + prod_i[EMB:2 * EMB, :] + prod_i[2 * EMB:3 * EMB, :]) * 0.25
        for part in range(2):
            for q in range(SIDE):
                block = seed_i[block_rows(part, q), block_lanes(q)]
                s_item[zz, part, q] = block
                it[s0, part, zz, y, q] = block.astype(BF16)
        ref = it.at[s0, :, zz, y]
        for k in (1, 3, 2):
            send(ref, ref, peer(1, k), plus(stage_sem[s0]['line'], k))
        return 0

    lax.fori_loop(0, SIDE, item_seeds, 0)
    left(r1.at[s0, 0], stage_sem[s0]['line'])

    for s in range(s0, STAGES):
        if s > s0:
            gather_last(s)
        user_own(s)
        scatter_mid(s)
        user_rest(s)
        new = scatter_end(s)
        for p in range(2):
            nxt = s_item[z, p, x] + new[p]
            if s + 1 < STAGES:
                it[s + 1, p, z, y, x] = nxt.astype(BF16)
            else:
                fin_f[p, x] = nxt
        if s + 1 < STAGES:
            gather_plane(s + 1)
        else:
            e_sem = fresh()
            send_axis(2, lambda t: fin_f.at[:, x], lambda k: fin_f.at[:, x], e_sem)
            left(fin_f.at[:, 0:3], e_sem)
        user_there(s)
        if s + 1 < STAGES:
            for h in range(2):
                ut[s + 1, h] = (s_user[h] + (up[s, h] + up_in[s, h])).astype(BF16)
            item_product(s + 1)
        else:
            gu_ref[...] = s_user[col] + (up[s, col] + up_in[s, col])
    arrive(fin_f.at[:, 0:3], e_sem)
    nat_f[...] = join_blocks(lambda part, q: fin_f[part, q]).T
    gi_ref[...] = nat_f[own, :]
    for ref, i in leaving:
        pltpu.make_async_copy(ref, ref, send_sem.at[i]).wait()


def hand_over(*refs):
    for src, dst in zip(refs[:5], refs[5:]):
        dst[...] = src[...]


def solution(mesh):
    def local_fn(mask_blk, user_emb, item_emb, triples):
        n_u, n_b = mask_blk.shape[0], triples.shape[0]
        half = n_u // 2
        vm = pltpu.VMEM
        outs = (jax.ShapeDtypeStruct((EMB, half), BF16), jax.ShapeDtypeStruct((EMB, EMB), BF16),
                jax.ShapeDtypeStruct((1, 1), F32), jax.ShapeDtypeStruct((EMB, half), F32),
                jax.ShapeDtypeStruct((EMB, EMB), F32))
        tile = (16, 128)
        S = SIDE
        scratch = [
            vm((NCHUNK, n_u, CHUNK), jnp.int32), vm((NCHUNK, n_u, CHUNK), BF16),
            vm((n_u, 128), jnp.int32), vm((n_u, 128), jnp.int32), vm((n_u, 128), F32),
            vm((2, 32, 128), jnp.int32), vm((18, 32, 128), jnp.int32), vm((32, 128), F32),
            vm((STAGES, 2, EMB, half), BF16), vm((STAGES, 2, EMB, half), F32), vm((STAGES, 2, EMB, half), F32),
            vm((2, EMB, half), F32), vm((2, EMB, half), F32),
            vm((S, EMB, EMB), BF16), vm((STAGES, 2, S, S, S) + tile, BF16), vm((STAGES, 2, S, S, S) + tile, F32),
            vm((STAGES, 2, S, S) + tile, F32),
            vm((STAGES, 2, S, 3, S) + tile, F32), vm((STAGES, 2, S * S - 1) + tile, F32),
            vm((2,) + tile, F32), vm((S, 2, S) + tile, F32),
            vm((2, S) + tile, BF16), vm((2, S) + tile, F32), vm((CHUNK, EMB), F32),
            vm((2, 2, S, S, 3) + tile, BF16), vm((2, S, S, 3) + tile, BF16), vm((2, S, S, 3) + tile, BF16),
            vm((2, 3) + tile, BF16), vm((2, S * S - 1, 3) + tile, BF16), vm((2, 3, 3) + tile, BF16),
            vm((2, 2, S, S, 3) + tile, BF16),
            vm((3 * EMB, n_b), BF16), vm((3 * EMB, n_b), BF16),
            vm((3 * EMB, n_u), F32), vm((3 * EMB, CHUNK), F32),
            vm((EMB, half), BF16), vm((EMB, EMB), BF16), vm((3, n_b), jnp.int32),
            pltpu.SemaphoreType.DMA((NCHUNK + 3,)), pltpu.SemaphoreType.DMA((NSEM,)), pltpu.SemaphoreType.DMA((NSEM,)),
        ]
        spec = pl.BlockSpec(memory_space=pltpu.VMEM)
        fu, fi, loss, gu, gi = pl.pallas_call(
            kernel,
            out_shape=outs,
            in_specs=[pl.BlockSpec(memory_space=pl.ANY)] * 4,
            out_specs=(spec,) * 5,
            scratch_shapes=scratch,
            compiler_params=pltpu.CompilerParams(collective_id=0, has_side_effects=True, vmem_limit_bytes=56 * 1024 * 1024),
        )(mask_blk, user_emb.T, item_emb, triples.T)
        args = (fu, fi, loss, gu, gi)
        fu, fi, loss, gu, gi = pl.pallas_call(hand_over, out_shape=outs, in_specs=[spec] * 5, out_specs=(spec,) * 5)(*args)
        return fu.T, fi, loss[0, 0], gu.T, gi

    user_spec = P(('row', 'col'), None)
    item_spec = P(('col', 'row'), None)
    return jax.shard_map(local_fn, mesh=mesh, in_specs=(P('row', 'col'), user_spec, item_spec, P()),
                         out_specs=(user_spec, item_spec, P(), user_spec, item_spec), check_vma=False)
```

```python
import jax
import jax.numpy as jnp
from jax import lax
from jax.experimental import pallas as pl
from jax.experimental.pallas import tpu as pltpu
from jax.sharding import PartitionSpec as P

SIDE = 4
STRIDE = (16, 4, 1)
EMB = 64
CHUNK = 256
NCHUNK = 16
LAYERS = 3
STAGES = 2 * LAYERS
F32 = jnp.float32
BF16 = jnp.bfloat16
NSEM = 160
GATHER_ORDER = (1, 3, 2, 4, 5, 7, 6, 12, 13, 15, 14, 8, 9, 11, 10)
PLANE_ORDER = (10, 6, 9, 11, 14, 5, 7, 13, 15, 2, 8, 1, 3, 4, 12)
NT = (((1,), (1,)), ((), ()))
MESH = pl.DeviceIdType.MESH


def block_rows(part, q):
    return slice(32 * part + 16 * (q // 2), 32 * part + 16 * (q // 2) + 16)


def block_lanes(q):
    return slice(128 * (q % 2), 128 * (q % 2) + 128)


def join_blocks(get):
    rows = []
    for part in range(2):
        for half in range(2):
            rows.append(jnp.concatenate([get(part, 2 * half), get(part, 2 * half + 1)], axis=1))
    return jnp.concatenate(rows, axis=0)


def kernel(mask_hbm, user_hbm, item_hbm, ids_hbm,
           fu_ref, fi_ref, loss_ref, gu_ref, gi_ref,
           mask, adj, rowsum, rowsum_in, scale_u, colsum, colsum_in, scale_i,
           ut, up, up_in, u_acc, s_user,
           nat, it, part_sum, q1, r1, r2, i_acc, s_item,
           fin_b, fin_f, nat_f,
           sel, sel_in, w0, w1, in1, in2, rows_all, grad_u, grad_i, prod_u, su, su_in, si, si_in, loss_out, loss_in,
           user_ref, item_ref, ids_ref, mask_sem, send_sem, recv_sem):
    row = lax.axis_index('row')
    col = lax.axis_index('col')
    pos = (lax.div(row, 16), lax.rem(lax.div(row, 4), 4), lax.rem(row, 4))
    step = [[p] + [lax.rem(p + k, SIDE) for k in range(1, SIDE)] for p in pos]
    offset = [[(step[a][k] - pos[a]) * STRIDE[a] if k else 0 for k in range(SIDE)] for a in range(3)]
    z, y, x = pos
    users = user_ref.shape[1]
    n_batch = ids_ref.shape[1]

    def peer(axis, k):
        return {'row': row + offset[axis][k]}

    partner = {'col': 1 - col}

    small = []
    for i, (src, dst) in enumerate(((user_hbm, user_ref), (item_hbm, item_ref), (ids_hbm, ids_ref))):
        cp = pltpu.make_async_copy(src, dst, mask_sem.at[NCHUNK + i])
        cp.start()
        small.append(cp)
    copies = []
    for j in range(NCHUNK):
        cp = pltpu.make_async_copy(mask_hbm.at[:, pl.ds(j * CHUNK, CHUNK)], mask.at[j], mask_sem.at[j])
        cp.start()
        copies.append(cp)

    def plane_peer(axes, k):
        return {'row': row + offset[axes[0]][k // SIDE] + offset[axes[1]][k % SIDE]}

    barrier = pltpu.get_barrier_semaphore()
    for axis in range(3):
        for k in range(1, SIDE):
            pl.semaphore_signal(barrier, inc=1, device_id=peer(axis, k), device_id_type=MESH)
    for axes in ((0, 1), (0, 2), (1, 2)):
        for k in range(SIDE * SIDE):
            if k // SIDE and k % SIDE:
                pl.semaphore_signal(barrier, inc=1, device_id=plane_peer(axes, k), device_id_type=MESH)
    pl.semaphore_signal(barrier, inc=1, device_id=partner, device_id_type=MESH)
    pl.semaphore_wait(barrier, 37)

    count = [0, 0]
    leaving = []

    def fresh(n=1):
        out = (count[0], count[1])
        count[0] += 1
        count[1] += n
        return out

    def send(src, dst, device, sems):
        pltpu.make_async_remote_copy(src_ref=src, dst_ref=dst, send_sem=send_sem.at[sems[0]], recv_sem=recv_sem.at[sems[1]],
                                     device_id=device, device_id_type=MESH).start()

    def left(ref, sems):
        leaving.append((ref, sems[0]))

    def arrive(ref, sems):
        pltpu.make_async_copy(ref, ref, recv_sem.at[sems[1]]).wait()

    def plus(sems, n):
        return (sems[0], sems[1] + n)

    def send_axis(axis, src, dst, sems):
        for k in (1, 3, 2):
            send(src(step[axis][k]), dst(k - 1), peer(axis, k), sems)

    def send_plane(axes, src, dst, sems):
        for k in PLANE_ORDER:
            send(src(step[axes[0]][k // SIDE], step[axes[1]][k % SIDE]), dst(k - 1), plane_peer(axes, k), sems)

    for cp in small:
        cp.wait()
    ut[0, col] = user_ref[...]
    u_sem = fresh()
    send(ut.at[0, col], ut.at[0, col], partner, u_sem)
    left(ut.at[0, 0], u_sem)
    nat[x] = item_ref[...]
    n_sem = fresh()
    send_axis(2, lambda t: nat.at[x], lambda k: nat.at[x], n_sem)
    left(nat.at[0:3], n_sem)

    rowsum[...] = jnp.zeros_like(rowsum)
    for j in range(NCHUNK):
        copies[j].wait()
        m = mask[j]
        adj[j] = m.astype(F32).astype(BF16)
        rowsum[...] += m[:, :128] + m[:, 128:]
        s = jnp.sum(m, axis=0, keepdims=True)
        colsum[0, 2 * j:2 * j + 1, :] = s[:, :128]
        colsum[0, 2 * j + 1:2 * j + 2, :] = s[:, 128:]
    r_sem, c_sem = fresh(), fresh()
    send(rowsum, rowsum_in, partner, r_sem)
    left(rowsum, r_sem)
    send_axis(0, lambda t: colsum.at[0], lambda k: colsum_in.at[k], c_sem)
    left(colsum_in.at[0:3], c_sem)

    arrive(nat.at[0:3], n_sem)
    chunk0 = jnp.concatenate([nat[k].astype(F32) for k in range(SIDE)], axis=0).T
    for part in range(2):
        for q in range(SIDE):
            it[0, part, z, y, q] = chunk0[block_rows(part, q), block_lanes(q)].astype(BF16)

    stage_sem = [dict(user=fresh(), plane=fresh(SIDE), line=fresh(SIDE), axis=[fresh(SIDE), fresh(SIDE)],
                      last=[fresh(), fresh()]) for _ in range(STAGES)]

    def gather_plane(s):
        sems = stage_sem[s]['plane']
        ref = it.at[s, :, z, y, x]
        for k in GATHER_ORDER:
            send(ref, ref, plane_peer((0, 2), k), plus(sems, k // SIDE))
        left(r2.at[s, 0], sems)

    def gather_line(s):
        sems = stage_sem[s]['plane']
        ref = it.at[s, :, z, y]
        for k in (1, 3, 2):
            send(ref, ref, peer(0, k), plus(sems, k))
        left(it.at[s, :, 0:3, 0], sems)

    def gather_last(s, line=False):
        sems = stage_sem[s]
        for kz in (0, 1, 3, 2):
            ref = it.at[s, :, step[0][(SIDE - kz) % SIDE], y]
            if kz:
                arrive(ref, plus(sems['plane'], kz))
            elif not line:
                arrive(ref.at[:, 0:3], sems['plane'])
            for k in (1, 3, 2):
                send(ref, ref, peer(1, k), plus(sems['line'], k))
        left(r1.at[s, 0], sems['line'])

    gather_line(0)
    arrive(rowsum_in, r_sem)
    deg_u = jnp.maximum(jnp.sum(rowsum[...] + rowsum_in[...], axis=1, keepdims=True), 1)
    scale_u[...] = jnp.broadcast_to(lax.rsqrt(deg_u.astype(F32)), scale_u.shape)
    arrive(colsum_in.at[0:3], c_sem)
    colsum[1] = colsum[0] + colsum_in[0] + colsum_in[1] + colsum_in[2]
    d_sem = fresh()
    send_plane((1, 2), lambda t0, t1: colsum.at[1], lambda k: colsum_in.at[3 + k], d_sem)
    left(colsum_in.at[3:18], d_sem)
    gather_last(0, line=True)
    arrive(colsum_in.at[3:18], d_sem)
    deg_i = jnp.maximum(colsum[1] + jnp.sum(colsum_in[3:], axis=0), 1)
    scale_i[...] = lax.rsqrt(deg_i.astype(F32))
    for j in range(NCHUNK):
        rowscale = scale_u[...]
        for l in range(2):
            lanes = slice(128 * l, 128 * l + 128)
            adj[j, :, lanes] = (rowscale * scale_i[2 * j + l:2 * j + l + 1, :]).astype(BF16) * adj[j, :, lanes]

    def at(ref, axis, t):
        return ref.at[(slice(None),) * axis + (t,)]

    def item_product(s):
        lhs = jnp.concatenate([ut[s, 0], ut[s, 1]], axis=1)

        def body(i, _):
            ky = lax.rem(i + 1, SIDE)
            yy = lax.rem(y + ky, SIDE)
            for kz in (2, 1, 3, 0):
                zz = step[0][kz]
                out = jnp.dot(lhs, adj[zz * SIDE + yy], preferred_element_type=F32)
                for part in range(2):
                    for q in range(SIDE):
                        part_sum[s, part, zz, yy, q] = out[block_rows(part, q), block_lanes(q)]
            scatter_send(s, ky, yy)
            return 0

        lax.fori_loop(0, SIDE, body, 0)
        for p in range(2):
            left(r1.at[s, p], stage_sem[s]['axis'][p])

    def scatter_send(s, ky, yy):
        sems = stage_sem[s]['axis']
        send_axis(0, lambda t: part_sum.at[s, 0, t, yy], lambda k: r1.at[s, 0, ky, k], plus(sems[0], ky))
        send_axis(2, lambda t: part_sum.at[s, 1, :, yy, t], lambda k: r1.at[s, 1, ky, k], plus(sems[1], ky))

    def scatter_mid(s, between=None):
        sems = stage_sem[s]

        def piece(ky, yy, off, ks):
            for p in range(2):
                axis = (2, 0)[p]
                arrive(r1.at[s, p, ky], plus(sems['axis'][p], ky))
                own = part_sum[s, 0, z, yy] if p == 0 else part_sum[s, 1, :, yy, x]
                q1[s, p, ky] = own + jnp.sum(r1[s, p, ky], axis=0)
                for k in ks:
                    send(q1.at[s, p, ky, step[axis][k]], r2.at[s, p, 4 * ky + k - 1], {'row': row + off + offset[axis][k]},
                         sems['last'][p])

        def body(ky, _):
            yy = lax.rem(y + ky, SIDE)
            piece(ky, yy, (yy - y) * STRIDE[1], (2, 1, 3, 0))
            return 0

        lax.fori_loop(1, SIDE, body, 0)
        if between:
            between()
        piece(0, y, 0, (2, 1, 3))
        for p in range(2):
            left(r2.at[s, p], sems['last'][p])

    def scatter_end(s):
        out = []
        for p in range(2):
            arrive(r2.at[s, p], stage_sem[s]['last'][p])
            out.append(q1[s, p, 0, pos[(2, 0)[p]]] + jnp.sum(r2[s, p], axis=0))
        return out

    def user_group(s, yy, first):
        acc = None
        for zz in range(SIDE):
            lhs = join_blocks(lambda part, q: it[s, part, zz, yy, q])
            d = lax.dot_general(lhs, adj[zz * SIDE + yy], NT, preferred_element_type=F32)
            acc = d if acc is None else acc + d
        for h in range(2):
            v = acc[:, h * users:(h + 1) * users]
            up[s, h] = v if first else up[s, h] + v

    def user_own(s):
        user_group(s, y, True)

    def user_rest(s):
        def body(i, _):
            k = 1 + lax.rem(2 * i, 3)
            yy = lax.rem(y + SIDE - k, SIDE)
            arrive(it.at[s, :, :, yy], plus(stage_sem[s]['line'], k))
            user_group(s, yy, False)
            return 0

        lax.fori_loop(0, SIDE - 1, body, 0)
        sems = stage_sem[s]['user']
        send(up.at[s], up_in.at[s], partner, sems)
        left(up.at[s], sems)

    def user_there(s):
        arrive(up_in.at[s], stage_sem[s]['user'])

    for p in range(2):
        i_acc[p] = it[0, p, z, y, x].astype(F32)
    arrive(ut.at[0, 1 - col], u_sem)
    for h in range(2):
        u_acc[h] = ut[0, h].astype(F32)

    def user_next(s):
        for h in range(2):
            nxt = (up[s, h] + up_in[s, h]).astype(BF16)
            u_acc[h] += nxt.astype(F32)
            if s + 1 < LAYERS:
                ut[s + 1, h] = nxt

    item_product(0)
    user_own(0)
    user_rest(0)
    scatter_mid(0)
    user_there(0)
    user_next(0)
    item_product(1)

    def item_next(s):
        new = scatter_end(s)
        for p in range(2):
            nxt = new[p].astype(BF16)
            i_acc[p] += nxt.astype(F32)
            if s + 1 < LAYERS:
                it[s + 1, p, z, y, x] = nxt
        if s + 1 < LAYERS:
            gather_plane(s + 1)

    item_next(0)
    scatter_mid(1, lambda: gather_last(1))
    user_own(1)
    item_next(1)
    user_rest(1)
    user_there(1)
    user_next(1)
    item_product(2)
    gather_last(2)
    user_own(2)
    scatter_mid(2)
    user_rest(2)
    user_there(2)
    user_next(2)

    tiles = n_batch // CHUNK
    iota = lax.broadcasted_iota(jnp.int32, (users, CHUNK), 0)
    for h in range(2):
        ut[LAYERS, h] = (u_acc[h] * 0.25).astype(BF16)
    own_u = ut[LAYERS, col]
    fu_ref[...] = own_u

    def put_rows(rt, t, picked):
        for l in range(2):
            lt = 2 * t + l
            sel[lt // 8, (lt % 8) // 4, lt % 4, rt // 3, rt % 3] = picked[:, 128 * l:128 * l + 128].astype(BF16)

    base_u = (2 * row + col) * users
    for t in range(tiles):
        ids = ids_ref[0:1, t * CHUNK:(t + 1) * CHUNK]
        hot = jnp.where(iota == ids - base_u, 1.0, 0.0).astype(BF16)
        picked = jnp.dot(own_u, hot, preferred_element_type=F32)
        for r in range(4):
            put_rows(r, t, picked[16 * r:16 * r + 16])
    item_next(2)
    for p in range(2):
        fin_b[p, x] = (i_acc[p] * 0.25).astype(BF16)
    f_sem = fresh()
    send_axis(2, lambda t: fin_b.at[:, x], lambda k: fin_b.at[:, x], f_sem)
    left(fin_b.at[:, 0:3], f_sem)
    base_i = (col * NCHUNK + z * SIDE + y) * CHUNK
    iota_i = lax.broadcasted_iota(jnp.int32, (CHUNK, CHUNK), 0)
    iota_b = lax.broadcasted_iota(jnp.int32, (128, CHUNK), 0)
    x_half, x_side = lax.div(x, 2), lax.rem(x, 2)
    base_b = base_i + 128 * x_side
    own_i = jnp.concatenate([fin_b[0, x], fin_b[1, x]], axis=0)
    for g in range(1, 3):
        for t in range(tiles):
            hot = jnp.where(iota_b == ids_ref[g:g + 1, t * CHUNK:(t + 1) * CHUNK] - base_b, 1.0, 0.0).astype(BF16)
            picked = jnp.dot(own_i, hot, preferred_element_type=F32)
            for part in range(2):
                rows = picked[16 * part:16 * part + 16]
                for half in range(2):
                    put_rows(4 * g + 2 * part + half, t, jnp.where(x_half == half, rows, 0.0))

    x_sem = fresh()
    send(sel.at[1 - col], sel_in, partner, x_sem)
    left(sel_in, x_sem)
    arrive(sel_in, x_sem)
    w0[...] = sel[col] + sel_in[...]
    ax0, ax2 = (0, 2), (2, 0)
    sems = [fresh() for _ in range(2)]
    for p in range(2):
        send_plane((ax0[p], 1), lambda t0, t1: w0.at[p, t0, t1], lambda k: in1.at[p, k], sems[p])
        left(in1.at[p], sems[p])
    arrive(fin_b.at[:, 0:3], f_sem)
    nat_f[...] = join_blocks(lambda part, q: fin_b[part, q]).astype(F32).T
    own = pl.ds(pl.multiple_of(x * EMB, EMB), EMB)
    fi_ref[...] = nat_f[own, :].astype(BF16)
    sems2 = [fresh() for _ in range(2)]
    for p in range(2):
        arrive(in1.at[p], sems[p])
        w1[p] = (w0[p, pos[ax0[p]], y].astype(F32) + jnp.sum(in1[p].astype(F32), axis=0)).astype(BF16)
        send_axis(ax2[p], lambda t: w1.at[p], lambda k: in2.at[p, k], sems2[p])
        left(in2.at[p], sems2[p])
    sems3 = [fresh() for _ in range(2)]
    for p in range(2):
        arrive(in2.at[p], sems2[p])
        a = pos[ax0[p]]
        rows_all[col, p, a, y] = w1[p] + in2[p, 0] + in2[p, 1] + in2[p, 2]
        ref = rows_all.at[col, p, a, y]
        send_plane((ax0[p], 1), lambda t0, t1: ref, lambda k: ref, sems3[p])
        left(in1.at[p], sems3[p])
    for p in range(2):
        arrive(in1.at[p], sems3[p])
    total = jnp.zeros((1, 128), F32)
    for lt in range(n_batch // 256):
        def rows_of(group):
            return jnp.concatenate([rows_all[col, lt // 4, lt % 4, rt // 3, rt % 3].astype(F32)
                                    for rt in range(4 * group, 4 * group + 4)], axis=0)
        e_user, e_pos, e_neg = rows_of(0), rows_of(1), rows_of(2)
        margin = jnp.sum(e_user * e_pos, axis=0, keepdims=True) - jnp.sum(e_user * e_neg, axis=0, keepdims=True)
        soft = jnp.maximum(-margin, 0.0) + jnp.log1p(jnp.exp(-jnp.abs(margin)))
        total = total + soft
        coef = -jax.nn.sigmoid(-margin) / n_batch
        lanes = slice(lt * 128, lt * 128 + 128)
        for ref, g in ((grad_u, coef * (e_pos - e_neg)), (grad_i, coef * e_user)):
            hi = g.astype(BF16)
            low = g - hi.astype(F32)
            mid = low.astype(BF16)
            ref[0:EMB, lanes] = hi
            ref[EMB:2 * EMB, lanes] = mid
            ref[2 * EMB:3 * EMB, lanes] = (low - mid.astype(F32)).astype(BF16)
    loss_out[...] = jnp.broadcast_to(total, loss_out.shape)
    l_sem = fresh()
    send(loss_out, loss_in, partner, l_sem)
    left(loss_out, l_sem)

    iota2 = lax.broadcasted_iota(jnp.int32, (2 * users, CHUNK), 0)
    s0 = LAYERS
    own_half = pl.multiple_of(col * (n_batch // 2), 128)

    def three(v):
        return v[0:EMB] + v[EMB:2 * EMB] + v[2 * EMB:3 * EMB]

    prod_u[...] = jnp.zeros_like(prod_u)
    for t in range(tiles // 2):
        cut = slice(t * CHUNK, (t + 1) * CHUNK)
        ids = ids_ref[0:1, pl.ds(own_half + t * CHUNK, CHUNK)]
        hot = jnp.where(iota2 == ids - row * (2 * users), 1.0, 0.0).astype(BF16)
        prod_u[...] += lax.dot_general(grad_u[:, cut], hot, NT, preferred_element_type=F32)
    seed = three(prod_u[...])
    for h in range(2):
        su[h] = seed[:, h * users:(h + 1) * users]
    su_sem = fresh()
    send(su, su_in, partner, su_sem)
    left(su, su_sem)

    def item_part(side, zz):
        base = (side * NCHUNK + zz * SIDE + y) * CHUNK
        acc = None
        for t in range(tiles // 2):
            cut = slice(t * CHUNK, (t + 1) * CHUNK)
            at_t = pl.ds(own_half + t * CHUNK, CHUNK)
            pos_hot = jnp.where(iota_i == ids_ref[1:2, at_t] - base, 1.0, 0.0)
            neg_hot = jnp.where(iota_i == ids_ref[2:3, at_t] - base, 1.0, 0.0)
            d = lax.dot_general(grad_i[:, cut], (pos_hot - neg_hot).astype(BF16), NT, preferred_element_type=F32)
            acc = d if acc is None else acc + d
        return three(acc)

    si_sem = fresh(SIDE)

    def other_seeds(zz, _):
        si[zz] = item_part(1 - col, zz)
        send(si.at[zz], si_in.at[zz], partner, plus(si_sem, zz))
        return 0

    lax.fori_loop(0, SIDE, other_seeds, 0)
    left(si, si_sem)
    arrive(su_in, su_sem)
    for h in range(2):
        v = (su[h] + su_in[h]) * 0.25
        s_user[h] = v
        ut[s0, h] = v.astype(BF16)
    item_product(s0)

    def item_seeds(zz, _):
        seed_i = item_part(col, zz)
        arrive(si_in.at[zz], plus(si_sem, zz))
        seed_i = (seed_i + si_in[zz]) * 0.25
        for part in range(2):
            for q in range(SIDE):
                block = seed_i[block_rows(part, q), block_lanes(q)]
                s_item[zz, part, q] = block
                it[s0, part, zz, y, q] = block.astype(BF16)
        ref = it.at[s0, :, zz, y]
        for k in (1, 3, 2):
            send(ref, ref, peer(1, k), plus(stage_sem[s0]['line'], k))
        return 0

    lax.fori_loop(0, SIDE, item_seeds, 0)
    left(r1.at[s0, 0], stage_sem[s0]['line'])
    arrive(loss_in, l_sem)
    loss_ref[...] = jnp.sum(total + loss_in[0:1], axis=1, keepdims=True) / n_batch

    for s in range(s0, STAGES):
        if s > s0:
            gather_last(s)
        user_own(s)
        scatter_mid(s)
        user_rest(s)
        new = scatter_end(s)
        for p in range(2):
            nxt = s_item[z, p, x] + new[p]
            if s + 1 < STAGES:
                it[s + 1, p, z, y, x] = nxt.astype(BF16)
            else:
                fin_f[p, x] = nxt
        if s + 1 < STAGES:
            gather_plane(s + 1)
        else:
            e_sem = fresh()
            send_axis(2, lambda t: fin_f.at[:, x], lambda k: fin_f.at[:, x], e_sem)
            left(fin_f.at[:, 0:3], e_sem)
        user_there(s)
        if s + 1 < STAGES:
            for h in range(2):
                ut[s + 1, h] = (s_user[h] + (up[s, h] + up_in[s, h])).astype(BF16)
            item_product(s + 1)
        else:
            gu_ref[...] = s_user[col] + (up[s, col] + up_in[s, col])
    arrive(fin_f.at[:, 0:3], e_sem)
    nat_f[...] = join_blocks(lambda part, q: fin_f[part, q]).T
    gi_ref[...] = nat_f[own, :]
    for ref, i in leaving:
        pltpu.make_async_copy(ref, ref, send_sem.at[i]).wait()


def hand_over(*refs):
    for src, dst in zip(refs[:5], refs[5:]):
        dst[...] = src[...]


def solution(mesh):
    def local_fn(mask_blk, user_emb, item_emb, triples):
        n_u, n_b = mask_blk.shape[0], triples.shape[0]
        half = n_u // 2
        vm = pltpu.VMEM
        outs = (jax.ShapeDtypeStruct((EMB, half), BF16), jax.ShapeDtypeStruct((EMB, EMB), BF16),
                jax.ShapeDtypeStruct((1, 1), F32), jax.ShapeDtypeStruct((EMB, half), F32),
                jax.ShapeDtypeStruct((EMB, EMB), F32))
        tile = (16, 128)
        S = SIDE
        scratch = [
            vm((NCHUNK, n_u, CHUNK), jnp.int32), vm((NCHUNK, n_u, CHUNK), BF16),
            vm((n_u, 128), jnp.int32), vm((n_u, 128), jnp.int32), vm((n_u, 128), F32),
            vm((2, 32, 128), jnp.int32), vm((18, 32, 128), jnp.int32), vm((32, 128), F32),
            vm((STAGES, 2, EMB, half), BF16), vm((STAGES, 2, EMB, half), F32), vm((STAGES, 2, EMB, half), F32),
            vm((2, EMB, half), F32), vm((2, EMB, half), F32),
            vm((S, EMB, EMB), BF16), vm((STAGES, 2, S, S, S) + tile, BF16), vm((STAGES, 2, S, S, S) + tile, F32),
            vm((STAGES, 2, S, S) + tile, F32),
            vm((STAGES, 2, S, 3, S) + tile, F32), vm((STAGES, 2, S * S - 1) + tile, F32),
            vm((2,) + tile, F32), vm((S, 2, S) + tile, F32),
            vm((2, S) + tile, BF16), vm((2, S) + tile, F32), vm((CHUNK, EMB), F32),
            vm((2, 2, S, S, 3) + tile, BF16), vm((2, S, S, 3) + tile, BF16), vm((2, S, S, 3) + tile, BF16),
            vm((2, 3) + tile, BF16), vm((2, S * S - 1, 3) + tile, BF16), vm((2, 3, 3) + tile, BF16),
            vm((2, 2, S, S, 3) + tile, BF16),
            vm((3 * EMB, n_b // 2), BF16), vm((3 * EMB, n_b // 2), BF16),
            vm((3 * EMB, n_u), F32), vm((2, EMB, half), F32), vm((2, EMB, half), F32),
            vm((S, EMB, CHUNK), F32), vm((S, EMB, CHUNK), F32), vm((8, 128), F32), vm((8, 128), F32),
            vm((EMB, half), BF16), vm((EMB, EMB), BF16), vm((3, n_b), jnp.int32),
            pltpu.SemaphoreType.DMA((NCHUNK + 3,)), pltpu.SemaphoreType.DMA((NSEM,)), pltpu.SemaphoreType.DMA((NSEM,)),
        ]
        spec = pl.BlockSpec(memory_space=pltpu.VMEM)
        fu, fi, loss, gu, gi = pl.pallas_call(
            kernel,
            out_shape=outs,
            in_specs=[pl.BlockSpec(memory_space=pl.ANY)] * 4,
            out_specs=(spec,) * 5,
            scratch_shapes=scratch,
            compiler_params=pltpu.CompilerParams(collective_id=0, has_side_effects=True, vmem_limit_bytes=56 * 1024 * 1024),
        )(mask_blk, user_emb.T, item_emb, triples.T)
        args = (fu, fi, loss, gu, gi)
        fu, fi, loss, gu, gi = pl.pallas_call(hand_over, out_shape=outs, in_specs=[spec] * 5, out_specs=(spec,) * 5)(*args)
        return fu.T, fi, loss[0, 0], gu.T, gi

    user_spec = P(('row', 'col'), None)
    item_spec = P(('col', 'row'), None)
    return jax.shard_map(local_fn, mesh=mesh, in_specs=(P('row', 'col'), user_spec, item_spec, P()),
                         out_specs=(user_spec, item_spec, P(), user_spec, item_spec), check_vma=False)
```

```python
import jax
import jax.numpy as jnp
from jax import lax
from jax.experimental import pallas as pl
from jax.experimental.pallas import tpu as pltpu
from jax.sharding import PartitionSpec as P

SIDE = 4
STRIDE = (16, 4, 1)
EMB = 64
CHUNK = 256
NCHUNK = 16
LAYERS = 3
STAGES = 2 * LAYERS
F32 = jnp.float32
BF16 = jnp.bfloat16
NSEM = 160
GATHER_ORDER = (1, 3, 2, 4, 5, 7, 6, 12, 13, 15, 14, 8, 9, 11, 10)
PLANE_ORDER = (10, 6, 9, 11, 14, 5, 7, 13, 15, 2, 8, 1, 3, 4, 12)
NT = (((1,), (1,)), ((), ()))
MESH = pl.DeviceIdType.MESH


def block_rows(part, q):
    return slice(32 * part + 16 * (q // 2), 32 * part + 16 * (q // 2) + 16)


def block_lanes(q):
    return slice(128 * (q % 2), 128 * (q % 2) + 128)


def join_blocks(get):
    rows = []
    for part in range(2):
        for half in range(2):
            rows.append(jnp.concatenate([get(part, 2 * half), get(part, 2 * half + 1)], axis=1))
    return jnp.concatenate(rows, axis=0)


def kernel(mask_hbm, user_hbm, item_hbm, ids_hbm,
           fu_ref, fi_ref, loss_ref, gu_ref, gi_ref,
           mask, adj, rowsum, rowsum_in, scale_u, colsum, colsum_in, scale_i,
           ut, up, up_in, u_acc, s_user,
           nat, it, part_sum, q1, r1, r2, i_acc, s_item,
           fin_b, fin_f, nat_f,
           sel, sel_in, w0, w1, in1, in2, rows_all, grad_u, grad_i, prod_u, su, su_in, si, si_in, loss_out, loss_in,
           user_ref, item_ref, ids_ref, mask_sem, send_sem, recv_sem):
    row = lax.axis_index('row')
    col = lax.axis_index('col')
    pos = (lax.div(row, 16), lax.rem(lax.div(row, 4), 4), lax.rem(row, 4))
    step = [[p] + [lax.rem(p + k, SIDE) for k in range(1, SIDE)] for p in pos]
    offset = [[(step[a][k] - pos[a]) * STRIDE[a] if k else 0 for k in range(SIDE)] for a in range(3)]
    z, y, x = pos
    users = user_ref.shape[1]
    n_batch = ids_ref.shape[1]

    def peer(axis, k):
        return {'row': row + offset[axis][k]}

    partner = {'col': 1 - col}

    small = []
    for i, (src, dst) in enumerate(((user_hbm, user_ref), (item_hbm, item_ref), (ids_hbm, ids_ref))):
        cp = pltpu.make_async_copy(src, dst, mask_sem.at[NCHUNK + i])
        cp.start()
        small.append(cp)
    copies = []
    for j in range(NCHUNK):
        cp = pltpu.make_async_copy(mask_hbm.at[:, pl.ds(j * CHUNK, CHUNK)], mask.at[j], mask_sem.at[j])
        cp.start()
        copies.append(cp)

    def plane_peer(axes, k):
        return {'row': row + offset[axes[0]][k // SIDE] + offset[axes[1]][k % SIDE]}

    barrier = pltpu.get_barrier_semaphore()
    for axis in range(3):
        for k in range(1, SIDE):
            pl.semaphore_signal(barrier, inc=1, device_id=peer(axis, k), device_id_type=MESH)
    for axes in ((0, 1), (0, 2), (1, 2)):
        for k in range(SIDE * SIDE):
            if k // SIDE and k % SIDE:
                pl.semaphore_signal(barrier, inc=1, device_id=plane_peer(axes, k), device_id_type=MESH)
    pl.semaphore_signal(barrier, inc=1, device_id=partner, device_id_type=MESH)
    pl.semaphore_wait(barrier, 37)

    count = [0, 0]
    leaving = []

    def fresh(n=1):
        out = (count[0], count[1])
        count[0] += 1
        count[1] += n
        return out

    def send(src, dst, device, sems):
        pltpu.make_async_remote_copy(src_ref=src, dst_ref=dst, send_sem=send_sem.at[sems[0]], recv_sem=recv_sem.at[sems[1]],
                                     device_id=device, device_id_type=MESH).start()

    def left(ref, sems):
        leaving.append((ref, sems[0]))

    def arrive(ref, sems):
        pltpu.make_async_copy(ref, ref, recv_sem.at[sems[1]]).wait()

    def plus(sems, n):
        return (sems[0], sems[1] + n)

    def send_axis(axis, src, dst, sems):
        for k in (1, 3, 2):
            send(src(step[axis][k]), dst(k - 1), peer(axis, k), sems)

    def send_plane(axes, src, dst, sems):
        for k in PLANE_ORDER:
            send(src(step[axes[0]][k // SIDE], step[axes[1]][k % SIDE]), dst(k - 1), plane_peer(axes, k), sems)

    for cp in small:
        cp.wait()
    ut[0, col] = user_ref[...]
    u_sem = fresh()
    send(ut.at[0, col], ut.at[0, col], partner, u_sem)
    left(ut.at[0, 0], u_sem)
    nat[x] = item_ref[...]
    n_sem = fresh()
    send_axis(2, lambda t: nat.at[x], lambda k: nat.at[x], n_sem)
    left(nat.at[0:3], n_sem)

    rowsum[...] = jnp.zeros_like(rowsum)
    for j in range(NCHUNK):
        copies[j].wait()
        m = mask[j]
        adj[j] = m.astype(F32).astype(BF16)
        rowsum[...] += m[:, :128] + m[:, 128:]
        s = jnp.sum(m, axis=0, keepdims=True)
        colsum[0, 2 * j:2 * j + 1, :] = s[:, :128]
        colsum[0, 2 * j + 1:2 * j + 2, :] = s[:, 128:]
    r_sem, c_sem = fresh(), fresh()
    send(rowsum, rowsum_in, partner, r_sem)
    left(rowsum, r_sem)
    send_axis(0, lambda t: colsum.at[0], lambda k: colsum_in.at[k], c_sem)
    left(colsum_in.at[0:3], c_sem)

    arrive(nat.at[0:3], n_sem)
    chunk0 = jnp.concatenate([nat[k].astype(F32) for k in range(SIDE)], axis=0).T
    for part in range(2):
        for q in range(SIDE):
            it[0, part, z, y, q] = chunk0[block_rows(part, q), block_lanes(q)].astype(BF16)

    stage_sem = [dict(user=fresh(), plane=fresh(SIDE), line=fresh(SIDE), axis=[fresh(SIDE), fresh(SIDE)],
                      last=[fresh(), fresh()]) for _ in range(STAGES)]

    def gather_plane(s):
        sems = stage_sem[s]['plane']
        ref = it.at[s, :, z, y, x]
        for k in GATHER_ORDER:
            send(ref, ref, plane_peer((0, 2), k), plus(sems, k // SIDE))
        left(r2.at[s, 0], sems)

    def gather_line(s):
        sems = stage_sem[s]['plane']
        ref = it.at[s, :, z, y]
        for k in (1, 3, 2):
            send(ref, ref, peer(0, k), plus(sems, k))
        left(it.at[s, :, 0:3, 0], sems)

    def gather_last(s, line=False):
        sems = stage_sem[s]
        for kz in (0, 1, 3, 2):
            ref = it.at[s, :, step[0][(SIDE - kz) % SIDE], y]
            if kz:
                arrive(ref, plus(sems['plane'], kz))
            elif not line:
                arrive(ref.at[:, 0:3], sems['plane'])
            for k in (1, 3, 2):
                send(ref, ref, peer(1, k), plus(sems['line'], k))
        left(r1.at[s, 0], sems['line'])

    gather_line(0)
    arrive(rowsum_in, r_sem)
    deg_u = jnp.maximum(jnp.sum(rowsum[...] + rowsum_in[...], axis=1, keepdims=True), 1)
    scale_u[...] = jnp.broadcast_to(lax.rsqrt(deg_u.astype(F32)), scale_u.shape)
    arrive(colsum_in.at[0:3], c_sem)
    colsum[1] = colsum[0] + colsum_in[0] + colsum_in[1] + colsum_in[2]
    d_sem = fresh()
    send_plane((1, 2), lambda t0, t1: colsum.at[1], lambda k: colsum_in.at[3 + k], d_sem)
    left(colsum_in.at[3:18], d_sem)
    gather_last(0, line=True)
    arrive(colsum_in.at[3:18], d_sem)
    deg_i = jnp.maximum(colsum[1] + jnp.sum(colsum_in[3:], axis=0), 1)
    scale_i[...] = lax.rsqrt(deg_i.astype(F32))

    def form(j):
        rowscale = scale_u[...]
        for l in range(2):
            lanes = slice(128 * l, 128 * l + 128)
            adj[j, :, lanes] = (rowscale * scale_i[pl.ds(2 * j + l, 1), :]).astype(BF16) * adj[j, :, lanes]

    def at(ref, axis, t):
        return ref.at[(slice(None),) * axis + (t,)]

    def item_product(s, before=None):
        lhs = jnp.concatenate([ut[s, 0], ut[s, 1]], axis=1)

        def body(i, _):
            ky = lax.rem(i + 1, SIDE)
            yy = lax.rem(y + ky, SIDE)
            for kz in (2, 1, 3, 0):
                zz = step[0][kz]
                if before:
                    before(zz * SIDE + yy)
                out = jnp.dot(lhs, adj[zz * SIDE + yy], preferred_element_type=F32)
                for part in range(2):
                    for q in range(SIDE):
                        part_sum[s, part, zz, yy, q] = out[block_rows(part, q), block_lanes(q)]
            scatter_send(s, ky, yy)
            return 0

        lax.fori_loop(0, SIDE, body, 0)
        for p in range(2):
            left(r1.at[s, p], stage_sem[s]['axis'][p])

    def scatter_send(s, ky, yy):
        sems = stage_sem[s]['axis']
        send_axis(0, lambda t: part_sum.at[s, 0, t, yy], lambda k: r1.at[s, 0, ky, k], plus(sems[0], ky))
        send_axis(2, lambda t: part_sum.at[s, 1, :, yy, t], lambda k: r1.at[s, 1, ky, k], plus(sems[1], ky))

    def scatter_mid(s, between=None):
        sems = stage_sem[s]

        def piece(ky, yy, off, ks):
            for p in range(2):
                axis = (2, 0)[p]
                arrive(r1.at[s, p, ky], plus(sems['axis'][p], ky))
                own = part_sum[s, 0, z, yy] if p == 0 else part_sum[s, 1, :, yy, x]
                q1[s, p, ky] = own + jnp.sum(r1[s, p, ky], axis=0)
                for k in ks:
                    send(q1.at[s, p, ky, step[axis][k]], r2.at[s, p, 4 * ky + k - 1], {'row': row + off + offset[axis][k]},
                         sems['last'][p])

        def body(ky, _):
            yy = lax.rem(y + ky, SIDE)
            piece(ky, yy, (yy - y) * STRIDE[1], (2, 1, 3, 0))
            return 0

        lax.fori_loop(1, SIDE, body, 0)
        if between:
            between()
        piece(0, y, 0, (2, 1, 3))
        for p in range(2):
            left(r2.at[s, p], sems['last'][p])

    def scatter_end(s):
        out = []
        for p in range(2):
            arrive(r2.at[s, p], stage_sem[s]['last'][p])
            out.append(q1[s, p, 0, pos[(2, 0)[p]]] + jnp.sum(r2[s, p], axis=0))
        return out

    def user_group(s, yy, first):
        acc = None
        for zz in range(SIDE):
            lhs = join_blocks(lambda part, q: it[s, part, zz, yy, q])
            d = lax.dot_general(lhs, adj[zz * SIDE + yy], NT, preferred_element_type=F32)
            acc = d if acc is None else acc + d
        for h in range(2):
            v = acc[:, h * users:(h + 1) * users]
            up[s, h] = v if first else up[s, h] + v

    def user_own(s):
        user_group(s, y, True)

    def user_rest(s):
        def body(i, _):
            k = 1 + lax.rem(2 * i, 3)
            yy = lax.rem(y + SIDE - k, SIDE)
            arrive(it.at[s, :, :, yy], plus(stage_sem[s]['line'], k))
            user_group(s, yy, False)
            return 0

        lax.fori_loop(0, SIDE - 1, body, 0)
        sems = stage_sem[s]['user']
        send(up.at[s], up_in.at[s], partner, sems)
        left(up.at[s], sems)

    def user_there(s):
        arrive(up_in.at[s], stage_sem[s]['user'])

    for p in range(2):
        i_acc[p] = it[0, p, z, y, x].astype(F32)
    arrive(ut.at[0, 1 - col], u_sem)
    for h in range(2):
        u_acc[h] = ut[0, h].astype(F32)

    def user_next(s):
        for h in range(2):
            nxt = (up[s, h] + up_in[s, h]).astype(BF16)
            u_acc[h] += nxt.astype(F32)
            if s + 1 < LAYERS:
                ut[s + 1, h] = nxt

    item_product(0, form)
    user_own(0)
    user_rest(0)
    scatter_mid(0)
    user_there(0)
    user_next(0)
    item_product(1)

    def item_next(s):
        new = scatter_end(s)
        for p in range(2):
            nxt = new[p].astype(BF16)
            i_acc[p] += nxt.astype(F32)
            if s + 1 < LAYERS:
                it[s + 1, p, z, y, x] = nxt
        if s + 1 < LAYERS:
            gather_plane(s + 1)

    item_next(0)
    scatter_mid(1, lambda: gather_last(1))
    user_own(1)
    item_next(1)
    user_rest(1)
    user_there(1)
    user_next(1)
    item_product(2)
    gather_last(2)
    user_own(2)
    scatter_mid(2)
    user_rest(2)
    user_there(2)
    user_next(2)

    tiles = n_batch // CHUNK
    iota = lax.broadcasted_iota(jnp.int32, (users, CHUNK), 0)
    for h in range(2):
        ut[LAYERS, h] = (u_acc[h] * 0.25).astype(BF16)
    own_u = ut[LAYERS, col]
    fu_ref[...] = own_u

    def put_rows(rt, t, picked):
        for l in range(2):
            lt = 2 * t + l
            sel[lt // 8, (lt % 8) // 4, lt % 4, rt // 3, rt % 3] = picked[:, 128 * l:128 * l + 128].astype(BF16)

    base_u = (2 * row + col) * users
    for t in range(tiles):
        ids = ids_ref[0:1, t * CHUNK:(t + 1) * CHUNK]
        hot = jnp.where(iota == ids - base_u, 1.0, 0.0).astype(BF16)
        picked = jnp.dot(own_u, hot, preferred_element_type=F32)
        for r in range(4):
            put_rows(r, t, picked[16 * r:16 * r + 16])
    item_next(2)
    for p in range(2):
        fin_b[p, x] = (i_acc[p] * 0.25).astype(BF16)
    f_sem = fresh()
    send_axis(2, lambda t: fin_b.at[:, x], lambda k: fin_b.at[:, x], f_sem)
    left(fin_b.at[:, 0:3], f_sem)
    base_i = (col * NCHUNK + z * SIDE + y) * CHUNK
    iota_i = lax.broadcasted_iota(jnp.int32, (CHUNK, CHUNK), 0)
    iota_b = lax.broadcasted_iota(jnp.int32, (128, CHUNK), 0)
    x_half, x_side = lax.div(x, 2), lax.rem(x, 2)
    base_b = base_i + 128 * x_side
    own_i = jnp.concatenate([fin_b[0, x], fin_b[1, x]], axis=0)
    for g in range(1, 3):
        for t in range(tiles):
            hot = jnp.where(iota_b == ids_ref[g:g + 1, t * CHUNK:(t + 1) * CHUNK] - base_b, 1.0, 0.0).astype(BF16)
            picked = jnp.dot(own_i, hot, preferred_element_type=F32)
            for part in range(2):
                rows = picked[16 * part:16 * part + 16]
                for half in range(2):
                    put_rows(4 * g + 2 * part + half, t, jnp.where(x_half == half, rows, 0.0))

    x_sem = fresh()
    send(sel.at[1 - col], sel_in, partner, x_sem)
    left(sel_in, x_sem)
    arrive(sel_in, x_sem)
    w0[...] = sel[col] + sel_in[...]
    ax0, ax2 = (0, 2), (2, 0)
    sems = [fresh() for _ in range(2)]
    for p in range(2):
        send_plane((ax0[p], 1), lambda t0, t1: w0.at[p, t0, t1], lambda k: in1.at[p, k], sems[p])
        left(in1.at[p], sems[p])
    arrive(fin_b.at[:, 0:3], f_sem)
    nat_f[...] = join_blocks(lambda part, q: fin_b[part, q]).astype(F32).T
    own = pl.ds(pl.multiple_of(x * EMB, EMB), EMB)
    fi_ref[...] = nat_f[own, :].astype(BF16)
    sems2 = [fresh() for _ in range(2)]
    for p in range(2):
        arrive(in1.at[p], sems[p])
        w1[p] = (w0[p, pos[ax0[p]], y].astype(F32) + jnp.sum(in1[p].astype(F32), axis=0)).astype(BF16)
        send_axis(ax2[p], lambda t: w1.at[p], lambda k: in2.at[p, k], sems2[p])
        left(in2.at[p], sems2[p])
    sems3 = [fresh() for _ in range(2)]
    for p in range(2):
        arrive(in2.at[p], sems2[p])
        a = pos[ax0[p]]
        rows_all[col, p, a, y] = w1[p] + in2[p, 0] + in2[p, 1] + in2[p, 2]
        ref = rows_all.at[col, p, a, y]
        send_plane((ax0[p], 1), lambda t0, t1: ref, lambda k: ref, sems3[p])
        left(in1.at[p], sems3[p])
    for p in range(2):
        arrive(in1.at[p], sems3[p])
    total = jnp.zeros((1, 128), F32)
    for lt in range(n_batch // 256):
        def rows_of(group):
            return jnp.concatenate([rows_all[col, lt // 4, lt % 4, rt // 3, rt % 3].astype(F32)
                                    for rt in range(4 * group, 4 * group + 4)], axis=0)
        e_user, e_pos, e_neg = rows_of(0), rows_of(1), rows_of(2)
        margin = jnp.sum(e_user * e_pos, axis=0, keepdims=True) - jnp.sum(e_user * e_neg, axis=0, keepdims=True)
        soft = jnp.maximum(-margin, 0.0) + jnp.log1p(jnp.exp(-jnp.abs(margin)))
        total = total + soft
        coef = -jax.nn.sigmoid(-margin) / n_batch
        lanes = slice(lt * 128, lt * 128 + 128)
        for ref, g in ((grad_u, coef * (e_pos - e_neg)), (grad_i, coef * e_user)):
            hi = g.astype(BF16)
            low = g - hi.astype(F32)
            mid = low.astype(BF16)
            ref[0:EMB, lanes] = hi
            ref[EMB:2 * EMB, lanes] = mid
            ref[2 * EMB:3 * EMB, lanes] = (low - mid.astype(F32)).astype(BF16)
    loss_out[...] = jnp.broadcast_to(total, loss_out.shape)
    l_sem = fresh()
    send(loss_out, loss_in, partner, l_sem)
    left(loss_out, l_sem)

    iota2 = lax.broadcasted_iota(jnp.int32, (2 * users, CHUNK), 0)
    s0 = LAYERS
    own_half = pl.multiple_of(col * (n_batch // 2), 128)

    def three(v):
        return v[0:EMB] + v[EMB:2 * EMB] + v[2 * EMB:3 * EMB]

    prod_u[...] = jnp.zeros_like(prod_u)
    for t in range(tiles // 2):
        cut = slice(t * CHUNK, (t + 1) * CHUNK)
        ids = ids_ref[0:1, pl.ds(own_half + t * CHUNK, CHUNK)]
        hot = jnp.where(iota2 == ids - row * (2 * users), 1.0, 0.0).astype(BF16)
        prod_u[...] += lax.dot_general(grad_u[:, cut], hot, NT, preferred_element_type=F32)
    seed = three(prod_u[...])
    for h in range(2):
        su[h] = seed[:, h * users:(h + 1) * users]
    su_sem = fresh()
    send(su, su_in, partner, su_sem)
    left(su, su_sem)

    def item_part(side, zz):
        base = (side * NCHUNK + zz * SIDE + y) * CHUNK
        acc = None
        for t in range(tiles // 2):
            cut = slice(t * CHUNK, (t + 1) * CHUNK)
            at_t = pl.ds(own_half + t * CHUNK, CHUNK)
            pos_hot = jnp.where(iota_i == ids_ref[1:2, at_t] - base, 1.0, 0.0)
            neg_hot = jnp.where(iota_i == ids_ref[2:3, at_t] - base, 1.0, 0.0)
            d = lax.dot_general(grad_i[:, cut], (pos_hot - neg_hot).astype(BF16), NT, preferred_element_type=F32)
            acc = d if acc is None else acc + d
        return three(acc)

    si_sem = fresh(SIDE)

    def other_seeds(zz, _):
        si[zz] = item_part(1 - col, zz)
        send(si.at[zz], si_in.at[zz], partner, plus(si_sem, zz))
        return 0

    lax.fori_loop(0, SIDE, other_seeds, 0)
    left(si, si_sem)
    arrive(su_in, su_sem)
    for h in range(2):
        v = (su[h] + su_in[h]) * 0.25
        s_user[h] = v
        ut[s0, h] = v.astype(BF16)
    item_product(s0)

    def item_seeds(zz, _):
        seed_i = item_part(col, zz)
        arrive(si_in.at[zz], plus(si_sem, zz))
        seed_i = (seed_i + si_in[zz]) * 0.25
        for part in range(2):
            for q in range(SIDE):
                block = seed_i[block_rows(part, q), block_lanes(q)]
                s_item[zz, part, q] = block
                it[s0, part, zz, y, q] = block.astype(BF16)
        ref = it.at[s0, :, zz, y]
        for k in (1, 3, 2):
            send(ref, ref, peer(1, k), plus(stage_sem[s0]['line'], k))
        return 0

    lax.fori_loop(0, SIDE, item_seeds, 0)
    left(r1.at[s0, 0], stage_sem[s0]['line'])
    arrive(loss_in, l_sem)
    loss_ref[...] = jnp.sum(total + loss_in[0:1], axis=1, keepdims=True) / n_batch

    for s in range(s0, STAGES):
        if s > s0:
            gather_last(s)
        user_own(s)
        scatter_mid(s)
        user_rest(s)
        new = scatter_end(s)
        for p in range(2):
            nxt = s_item[z, p, x] + new[p]
            if s + 1 < STAGES:
                it[s + 1, p, z, y, x] = nxt.astype(BF16)
            else:
                fin_f[p, x] = nxt
        if s + 1 < STAGES:
            gather_plane(s + 1)
        else:
            e_sem = fresh()
            send_axis(2, lambda t: fin_f.at[:, x], lambda k: fin_f.at[:, x], e_sem)
            left(fin_f.at[:, 0:3], e_sem)
        user_there(s)
        if s + 1 < STAGES:
            for h in range(2):
                ut[s + 1, h] = (s_user[h] + (up[s, h] + up_in[s, h])).astype(BF16)
            item_product(s + 1)
        else:
            gu_ref[...] = s_user[col] + (up[s, col] + up_in[s, col])
    arrive(fin_f.at[:, 0:3], e_sem)
    nat_f[...] = join_blocks(lambda part, q: fin_f[part, q]).T
    gi_ref[...] = nat_f[own, :]
    for ref, i in leaving:
        pltpu.make_async_copy(ref, ref, send_sem.at[i]).wait()


def hand_over(*refs):
    for src, dst in zip(refs[:5], refs[5:]):
        dst[...] = src[...]


def solution(mesh):
    def local_fn(mask_blk, user_emb, item_emb, triples):
        n_u, n_b = mask_blk.shape[0], triples.shape[0]
        half = n_u // 2
        vm = pltpu.VMEM
        outs = (jax.ShapeDtypeStruct((EMB, half), BF16), jax.ShapeDtypeStruct((EMB, EMB), BF16),
                jax.ShapeDtypeStruct((1, 1), F32), jax.ShapeDtypeStruct((EMB, half), F32),
                jax.ShapeDtypeStruct((EMB, EMB), F32))
        tile = (16, 128)
        S = SIDE
        scratch = [
            vm((NCHUNK, n_u, CHUNK), jnp.int32), vm((NCHUNK, n_u, CHUNK), BF16),
            vm((n_u, 128), jnp.int32), vm((n_u, 128), jnp.int32), vm((n_u, 128), F32),
            vm((2, 32, 128), jnp.int32), vm((18, 32, 128), jnp.int32), vm((32, 128), F32),
            vm((STAGES, 2, EMB, half), BF16), vm((STAGES, 2, EMB, half), F32), vm((STAGES, 2, EMB, half), F32),
            vm((2, EMB, half), F32), vm((2, EMB, half), F32),
            vm((S, EMB, EMB), BF16), vm((STAGES, 2, S, S, S) + tile, BF16), vm((STAGES, 2, S, S, S) + tile, F32),
            vm((STAGES, 2, S, S) + tile, F32),
            vm((STAGES, 2, S, 3, S) + tile, F32), vm((STAGES, 2, S * S - 1) + tile, F32),
            vm((2,) + tile, F32), vm((S, 2, S) + tile, F32),
            vm((2, S) + tile, BF16), vm((2, S) + tile, F32), vm((CHUNK, EMB), F32),
            vm((2, 2, S, S, 3) + tile, BF16), vm((2, S, S, 3) + tile, BF16), vm((2, S, S, 3) + tile, BF16),
            vm((2, 3) + tile, BF16), vm((2, S * S - 1, 3) + tile, BF16), vm((2, 3, 3) + tile, BF16),
            vm((2, 2, S, S, 3) + tile, BF16),
            vm((3 * EMB, n_b // 2), BF16), vm((3 * EMB, n_b // 2), BF16),
            vm((3 * EMB, n_u), F32), vm((2, EMB, half), F32), vm((2, EMB, half), F32),
            vm((S, EMB, CHUNK), F32), vm((S, EMB, CHUNK), F32), vm((8, 128), F32), vm((8, 128), F32),
            vm((EMB, half), BF16), vm((EMB, EMB), BF16), vm((3, n_b), jnp.int32),
            pltpu.SemaphoreType.DMA((NCHUNK + 3,)), pltpu.SemaphoreType.DMA((NSEM,)), pltpu.SemaphoreType.DMA((NSEM,)),
        ]
        spec = pl.BlockSpec(memory_space=pltpu.VMEM)
        fu, fi, loss, gu, gi = pl.pallas_call(
            kernel,
            out_shape=outs,
            in_specs=[pl.BlockSpec(memory_space=pl.ANY)] * 4,
            out_specs=(spec,) * 5,
            scratch_shapes=scratch,
            compiler_params=pltpu.CompilerParams(collective_id=0, has_side_effects=True, vmem_limit_bytes=56 * 1024 * 1024),
        )(mask_blk, user_emb.T, item_emb, triples.T)
        args = (fu, fi, loss, gu, gi)
        fu, fi, loss, gu, gi = pl.pallas_call(hand_over, out_shape=outs, in_specs=[spec] * 5, out_specs=(spec,) * 5)(*args)
        return fu.T, fi, loss[0, 0], gu.T, gi

    user_spec = P(('row', 'col'), None)
    item_spec = P(('col', 'row'), None)
    return jax.shard_map(local_fn, mesh=mesh, in_specs=(P('row', 'col'), user_spec, item_spec, P()),
                         out_specs=(user_spec, item_spec, P(), user_spec, item_spec), check_vma=False)
```

```python
import jax
import jax.numpy as jnp
from jax import lax
from jax.experimental import pallas as pl
from jax.experimental.pallas import tpu as pltpu
from jax.sharding import PartitionSpec as P

SIDE = 4
STRIDE = (16, 4, 1)
EMB = 64
CHUNK = 256
NCHUNK = 16
LAYERS = 3
STAGES = 2 * LAYERS
F32 = jnp.float32
BF16 = jnp.bfloat16
NSEM = 160
GATHER_ORDER = (1, 3, 2, 4, 5, 7, 6, 12, 13, 15, 14, 8, 9, 11, 10)
PLANE_ORDER = (10, 6, 9, 11, 14, 5, 7, 13, 15, 2, 8, 1, 3, 4, 12)
NT = (((1,), (1,)), ((), ()))
MESH = pl.DeviceIdType.MESH


def block_rows(part, q):
    return slice(32 * part + 16 * (q // 2), 32 * part + 16 * (q // 2) + 16)


def block_lanes(q):
    return slice(128 * (q % 2), 128 * (q % 2) + 128)


def join_blocks(get):
    rows = []
    for part in range(2):
        for half in range(2):
            rows.append(jnp.concatenate([get(part, 2 * half), get(part, 2 * half + 1)], axis=1))
    return jnp.concatenate(rows, axis=0)


def kernel(mask_hbm, user_hbm, item_hbm, ids_hbm,
           fu_ref, fi_ref, loss_ref, gu_ref, gi_ref,
           mask, adj, rowsum, rowsum_in, scale_u, colsum, colsum_in, scale_i,
           ut, up, up_in, u_acc, s_user,
           nat, it, part_sum, q1, r1, r2, i_acc, s_item,
           fin_b, fin_f, nat_f,
           sel, sel_in, w0, w1, in1, in2, rows_all, grad_u, grad_i, prod_u, su, su_in, si, si_in, loss_out, loss_in,
           user_ref, item_ref, ids_ref, mask_sem, send_sem, recv_sem):
    row = lax.axis_index('row')
    col = lax.axis_index('col')
    pos = (lax.div(row, 16), lax.rem(lax.div(row, 4), 4), lax.rem(row, 4))
    step = [[p] + [lax.rem(p + k, SIDE) for k in range(1, SIDE)] for p in pos]
    offset = [[(step[a][k] - pos[a]) * STRIDE[a] if k else 0 for k in range(SIDE)] for a in range(3)]
    z, y, x = pos
    users = user_ref.shape[1]
    n_batch = ids_ref.shape[1]

    def peer(axis, k):
        return {'row': row + offset[axis][k]}

    partner = {'col': 1 - col}

    small = []
    for i, (src, dst) in enumerate(((user_hbm, user_ref), (item_hbm, item_ref), (ids_hbm, ids_ref))):
        cp = pltpu.make_async_copy(src, dst, mask_sem.at[NCHUNK + i])
        cp.start()
        small.append(cp)
    copies = []
    for j in range(NCHUNK):
        cp = pltpu.make_async_copy(mask_hbm.at[:, pl.ds(j * CHUNK, CHUNK)], mask.at[j], mask_sem.at[j])
        cp.start()
        copies.append(cp)

    def plane_peer(axes, k):
        return {'row': row + offset[axes[0]][k // SIDE] + offset[axes[1]][k % SIDE]}

    barrier = pltpu.get_barrier_semaphore()
    for axis in range(3):
        for k in range(1, SIDE):
            pl.semaphore_signal(barrier, inc=1, device_id=peer(axis, k), device_id_type=MESH)
    for axes in ((0, 1), (0, 2), (1, 2)):
        for k in range(SIDE * SIDE):
            if k // SIDE and k % SIDE:
                pl.semaphore_signal(barrier, inc=1, device_id=plane_peer(axes, k), device_id_type=MESH)
    pl.semaphore_signal(barrier, inc=1, device_id=partner, device_id_type=MESH)
    pl.semaphore_wait(barrier, 37)

    count = [0, 0]
    leaving = []

    def fresh(n=1):
        out = (count[0], count[1])
        count[0] += 1
        count[1] += n
        return out

    def send(src, dst, device, sems):
        pltpu.make_async_remote_copy(src_ref=src, dst_ref=dst, send_sem=send_sem.at[sems[0]], recv_sem=recv_sem.at[sems[1]],
                                     device_id=device, device_id_type=MESH).start()

    def left(ref, sems):
        leaving.append((ref, sems[0]))

    def arrive(ref, sems):
        pltpu.make_async_copy(ref, ref, recv_sem.at[sems[1]]).wait()

    def plus(sems, n):
        return (sems[0], sems[1] + n)

    def send_axis(axis, src, dst, sems):
        for k in (1, 3, 2):
            send(src(step[axis][k]), dst(k - 1), peer(axis, k), sems)

    def send_plane(axes, src, dst, sems):
        for k in PLANE_ORDER:
            send(src(step[axes[0]][k // SIDE], step[axes[1]][k % SIDE]), dst(k - 1), plane_peer(axes, k), sems)

    for cp in small:
        cp.wait()
    ut[0, col] = user_ref[...]
    u_sem = fresh()
    send(ut.at[0, col], ut.at[0, col], partner, u_sem)
    left(ut.at[0, 0], u_sem)
    nat[x] = item_ref[...]
    n_sem = fresh()
    send_axis(2, lambda t: nat.at[x], lambda k: nat.at[x], n_sem)
    left(nat.at[0:3], n_sem)

    rowsum[...] = jnp.zeros_like(rowsum)
    for j in range(NCHUNK):
        copies[j].wait()
        m = mask[j]
        adj[j] = m.astype(F32).astype(BF16)
        rowsum[...] += m[:, :128] + m[:, 128:]
        s = jnp.sum(m, axis=0, keepdims=True)
        colsum[0, 2 * j:2 * j + 1, :] = s[:, :128]
        colsum[0, 2 * j + 1:2 * j + 2, :] = s[:, 128:]
    r_sem, c_sem = fresh(), fresh()
    send(rowsum, rowsum_in, partner, r_sem)
    left(rowsum, r_sem)
    send_axis(0, lambda t: colsum.at[0], lambda k: colsum_in.at[k], c_sem)
    left(colsum_in.at[0:3], c_sem)

    arrive(nat.at[0:3], n_sem)
    chunk0 = jnp.concatenate([nat[k].astype(F32) for k in range(SIDE)], axis=0).T
    for part in range(2):
        for q in range(SIDE):
            it[0, part, z, y, q] = chunk0[block_rows(part, q), block_lanes(q)].astype(BF16)

    stage_sem = [dict(user=fresh(), plane=fresh(SIDE), line=fresh(SIDE), axis=[fresh(SIDE), fresh(SIDE)],
                      last=[fresh(), fresh()]) for _ in range(STAGES)]

    def gather_plane(s):
        sems = stage_sem[s]['plane']
        ref = it.at[s, :, z, y, x]
        for k in GATHER_ORDER:
            send(ref, ref, plane_peer((0, 2), k), plus(sems, k // SIDE))
        left(r2.at[s, 0], sems)

    def gather_line(s):
        sems = stage_sem[s]['plane']
        ref = it.at[s, :, z, y]
        for k in (1, 3, 2):
            send(ref, ref, peer(0, k), plus(sems, k))
        left(it.at[s, :, 0:3, 0], sems)

    def gather_last(s, line=False):
        sems = stage_sem[s]
        for kz in (0, 1, 3, 2):
            ref = it.at[s, :, step[0][(SIDE - kz) % SIDE], y]
            if kz:
                arrive(ref, plus(sems['plane'], kz))
            elif not line:
                arrive(ref.at[:, 0:3], sems['plane'])
            for k in (1, 3, 2):
                send(ref, ref, peer(1, k), plus(sems['line'], k))
        left(r1.at[s, 0], sems['line'])

    gather_line(0)
    arrive(rowsum_in, r_sem)
    deg_u = jnp.maximum(jnp.sum(rowsum[...] + rowsum_in[...], axis=1, keepdims=True), 1)
    scale_u[...] = jnp.broadcast_to(lax.rsqrt(deg_u.astype(F32)), scale_u.shape)
    arrive(colsum_in.at[0:3], c_sem)
    colsum[1] = colsum[0] + colsum_in[0] + colsum_in[1] + colsum_in[2]
    d_sem = fresh()
    send_plane((1, 2), lambda t0, t1: colsum.at[1], lambda k: colsum_in.at[3 + k], d_sem)
    left(colsum_in.at[3:18], d_sem)
    gather_last(0, line=True)
    arrive(colsum_in.at[3:18], d_sem)
    deg_i = jnp.maximum(colsum[1] + jnp.sum(colsum_in[3:], axis=0), 1)
    scale_i[...] = lax.rsqrt(deg_i.astype(F32))
    for j in range(NCHUNK):
        rowscale = scale_u[...]
        for l in range(2):
            lanes = slice(128 * l, 128 * l + 128)
            adj[j, :, lanes] = (rowscale * scale_i[2 * j + l:2 * j + l + 1, :]).astype(BF16) * adj[j, :, lanes]

    def at(ref, axis, t):
        return ref.at[(slice(None),) * axis + (t,)]

    def item_product(s):
        lhs = jnp.concatenate([ut[s, 0], ut[s, 1]], axis=1)

        def body(i, _):
            ky = lax.rem(i + 1, SIDE)
            yy = lax.rem(y + ky, SIDE)
            for kz in (2, 1, 3, 0):
                zz = step[0][kz]
                out = jnp.dot(lhs, adj[zz * SIDE + yy], preferred_element_type=F32)
                for part in range(2):
                    for q in range(SIDE):
                        part_sum[s, part, zz, yy, q] = out[block_rows(part, q), block_lanes(q)]
            scatter_send(s, ky, yy)
            return 0

        lax.fori_loop(0, SIDE, body, 0)
        for p in range(2):
            left(r1.at[s, p], stage_sem[s]['axis'][p])

    def scatter_send(s, ky, yy):
        sems = stage_sem[s]['axis']
        send_axis(0, lambda t: part_sum.at[s, 0, t, yy], lambda k: r1.at[s, 0, ky, k], plus(sems[0], ky))
        send_axis(2, lambda t: part_sum.at[s, 1, :, yy, t], lambda k: r1.at[s, 1, ky, k], plus(sems[1], ky))

    def scatter_mid(s, between=None):
        sems = stage_sem[s]

        def piece(ky, yy, off, ks):
            for p in range(2):
                axis = (2, 0)[p]
                arrive(r1.at[s, p, ky], plus(sems['axis'][p], ky))
                own = part_sum[s, 0, z, yy] if p == 0 else part_sum[s, 1, :, yy, x]
                q1[s, p, ky] = own + jnp.sum(r1[s, p, ky], axis=0)
                for k in ks:
                    send(q1.at[s, p, ky, step[axis][k]], r2.at[s, p, 4 * ky + k - 1], {'row': row + off + offset[axis][k]},
                         sems['last'][p])

        def body(ky, _):
            yy = lax.rem(y + ky, SIDE)
            piece(ky, yy, (yy - y) * STRIDE[1], (2, 1, 3, 0))
            return 0

        lax.fori_loop(1, SIDE, body, 0)
        if between:
            between()
        piece(0, y, 0, (2, 1, 3))
        for p in range(2):
            left(r2.at[s, p], sems['last'][p])

    def scatter_end(s):
        out = []
        for p in range(2):
            arrive(r2.at[s, p], stage_sem[s]['last'][p])
            out.append(q1[s, p, 0, pos[(2, 0)[p]]] + jnp.sum(r2[s, p], axis=0))
        return out

    def user_group(s, yy, first):
        acc = None
        for zz in range(SIDE):
            lhs = join_blocks(lambda part, q: it[s, part, zz, yy, q])
            d = lax.dot_general(lhs, adj[zz * SIDE + yy], NT, preferred_element_type=F32)
            acc = d if acc is None else acc + d
        for h in range(2):
            v = acc[:, h * users:(h + 1) * users]
            up[s, h] = v if first else up[s, h] + v

    def user_own(s):
        user_group(s, y, True)

    def user_rest(s):
        def body(i, _):
            k = 1 + lax.rem(2 * i, 3)
            yy = lax.rem(y + SIDE - k, SIDE)
            arrive(it.at[s, :, :, yy], plus(stage_sem[s]['line'], k))
            user_group(s, yy, False)
            return 0

        lax.fori_loop(0, SIDE - 1, body, 0)
        sems = stage_sem[s]['user']
        send(up.at[s], up_in.at[s], partner, sems)
        left(up.at[s], sems)

    def user_there(s):
        arrive(up_in.at[s], stage_sem[s]['user'])

    for p in range(2):
        i_acc[p] = it[0, p, z, y, x].astype(F32)
    arrive(ut.at[0, 1 - col], u_sem)
    for h in range(2):
        u_acc[h] = ut[0, h].astype(F32)

    def user_next(s):
        for h in range(2):
            nxt = (up[s, h] + up_in[s, h]).astype(BF16)
            u_acc[h] += nxt.astype(F32)
            if s + 1 < LAYERS:
                ut[s + 1, h] = nxt

    item_product(0)
    user_own(0)
    user_rest(0)
    scatter_mid(0)
    user_there(0)
    user_next(0)
    item_product(1)

    def item_next(s):
        new = scatter_end(s)
        for p in range(2):
            nxt = new[p].astype(BF16)
            i_acc[p] += nxt.astype(F32)
            if s + 1 < LAYERS:
                it[s + 1, p, z, y, x] = nxt
        if s + 1 < LAYERS:
            gather_plane(s + 1)

    item_next(0)
    scatter_mid(1, lambda: gather_last(1))
    user_own(1)
    item_next(1)
    user_rest(1)
    user_there(1)
    user_next(1)
    item_product(2)
    gather_last(2)
    user_own(2)
    scatter_mid(2)
    user_rest(2)
    user_there(2)
    user_next(2)

    tiles = n_batch // CHUNK
    iota = lax.broadcasted_iota(jnp.int32, (users, CHUNK), 0)
    for h in range(2):
        ut[LAYERS, h] = (u_acc[h] * 0.25).astype(BF16)
    own_u = ut[LAYERS, col]
    fu_ref[...] = own_u

    def put_rows(rt, t, picked):
        for l in range(2):
            lt = 2 * t + l
            sel[lt // 8, rt % 3, lt % 4, rt // 3, (lt % 8) // 4] = picked[:, 128 * l:128 * l + 128].astype(BF16)

    base_u = (2 * row + col) * users
    for t in range(tiles):
        ids = ids_ref[0:1, t * CHUNK:(t + 1) * CHUNK]
        hot = jnp.where(iota == ids - base_u, 1.0, 0.0).astype(BF16)
        picked = jnp.dot(own_u, hot, preferred_element_type=F32)
        for r in range(4):
            put_rows(r, t, picked[16 * r:16 * r + 16])
    item_next(2)
    for p in range(2):
        fin_b[p, x] = (i_acc[p] * 0.25).astype(BF16)
    f_sem = fresh()
    send_axis(2, lambda t: fin_b.at[:, x], lambda k: fin_b.at[:, x], f_sem)
    left(fin_b.at[:, 0:3], f_sem)
    base_i = (col * NCHUNK + z * SIDE + y) * CHUNK
    iota_i = lax.broadcasted_iota(jnp.int32, (CHUNK, CHUNK), 0)
    iota_b = lax.broadcasted_iota(jnp.int32, (128, CHUNK), 0)
    x_half, x_side = lax.div(x, 2), lax.rem(x, 2)
    base_b = base_i + 128 * x_side
    own_i = jnp.concatenate([fin_b[0, x], fin_b[1, x]], axis=0)
    for g in range(1, 3):
        for t in range(tiles):
            hot = jnp.where(iota_b == ids_ref[g:g + 1, t * CHUNK:(t + 1) * CHUNK] - base_b, 1.0, 0.0).astype(BF16)
            picked = jnp.dot(own_i, hot, preferred_element_type=F32)
            for part in range(2):
                rows = picked[16 * part:16 * part + 16]
                for half in range(2):
                    put_rows(4 * g + 2 * part + half, t, jnp.where(x_half == half, rows, 0.0))

    x_sem = fresh()
    send(sel.at[1 - col], sel_in, partner, x_sem)
    left(sel_in, x_sem)
    arrive(sel_in, x_sem)
    w0[...] = sel[col] + sel_in[...]
    planes, third = ((0, 1), (2, 1), (0, 2)), (2, 0, 1)
    sems = [fresh() for _ in range(3)]
    for p in range(3):
        send_plane(planes[p], lambda t0, t1: w0.at[p, t0, t1], lambda k: in1.at[p, k], sems[p])
        left(in1.at[p], sems[p])
    arrive(fin_b.at[:, 0:3], f_sem)
    nat_f[...] = join_blocks(lambda part, q: fin_b[part, q]).astype(F32).T
    own = pl.ds(pl.multiple_of(x * EMB, EMB), EMB)
    fi_ref[...] = nat_f[own, :].astype(BF16)
    sems2 = [fresh() for _ in range(3)]
    for p in range(3):
        arrive(in1.at[p], sems[p])
        mine = w0[p, pos[planes[p][0]], pos[planes[p][1]]].astype(F32)
        w1[p] = (mine + jnp.sum(in1[p].astype(F32), axis=0)).astype(BF16)
        send_axis(third[p], lambda t: w1.at[p], lambda k: in2.at[p, k], sems2[p])
        left(in2.at[p], sems2[p])
    sems3 = [fresh() for _ in range(3)]
    for p in range(3):
        arrive(in2.at[p], sems2[p])
        ref = rows_all.at[col, p, pos[planes[p][0]], pos[planes[p][1]]]
        ref[...] = w1[p] + in2[p, 0] + in2[p, 1] + in2[p, 2]
        send_plane(planes[p], lambda t0, t1: ref, lambda k: ref, sems3[p])
        left(in1.at[p], sems3[p])
    for p in range(3):
        arrive(in1.at[p], sems3[p])
    total = jnp.zeros((1, 128), F32)
    for lt in range(n_batch // 256):
        def rows_of(group):
            return jnp.concatenate([rows_all[col, rt % 3, lt % 4, rt // 3, lt // 4].astype(F32)
                                    for rt in range(4 * group, 4 * group + 4)], axis=0)
        e_user, e_pos, e_neg = rows_of(0), rows_of(1), rows_of(2)
        margin = jnp.sum(e_user * e_pos, axis=0, keepdims=True) - jnp.sum(e_user * e_neg, axis=0, keepdims=True)
        soft = jnp.maximum(-margin, 0.0) + jnp.log1p(jnp.exp(-jnp.abs(margin)))
        total = total + soft
        coef = -jax.nn.sigmoid(-margin) / n_batch
        lanes = slice(lt * 128, lt * 128 + 128)
        for ref, g in ((grad_u, coef * (e_pos - e_neg)), (grad_i, coef * e_user)):
            hi = g.astype(BF16)
            low = g - hi.astype(F32)
            mid = low.astype(BF16)
            ref[0:EMB, lanes] = hi
            ref[EMB:2 * EMB, lanes] = mid
            ref[2 * EMB:3 * EMB, lanes] = (low - mid.astype(F32)).astype(BF16)
    loss_out[...] = jnp.broadcast_to(total, loss_out.shape)
    l_sem = fresh()
    send(loss_out, loss_in, partner, l_sem)
    left(loss_out, l_sem)

    iota2 = lax.broadcasted_iota(jnp.int32, (2 * users, CHUNK), 0)
    s0 = LAYERS
    own_half = pl.multiple_of(col * (n_batch // 2), 128)

    def three(v):
        return v[0:EMB] + v[EMB:2 * EMB] + v[2 * EMB:3 * EMB]

    prod_u[...] = jnp.zeros_like(prod_u)
    for t in range(tiles // 2):
        cut = slice(t * CHUNK, (t + 1) * CHUNK)
        ids = ids_ref[0:1, pl.ds(own_half + t * CHUNK, CHUNK)]
        hot = jnp.where(iota2 == ids - row * (2 * users), 1.0, 0.0).astype(BF16)
        prod_u[...] += lax.dot_general(grad_u[:, cut], hot, NT, preferred_element_type=F32)
    seed = three(prod_u[...])
    for h in range(2):
        su[h] = seed[:, h * users:(h + 1) * users]
    su_sem = fresh()
    send(su, su_in, partner, su_sem)
    left(su, su_sem)

    def item_part(side, zz):
        base = (side * NCHUNK + zz * SIDE + y) * CHUNK
        acc = None
        for t in range(tiles // 2):
            cut = slice(t * CHUNK, (t + 1) * CHUNK)
            at_t = pl.ds(own_half + t * CHUNK, CHUNK)
            pos_hot = jnp.where(iota_i == ids_ref[1:2, at_t] - base, 1.0, 0.0)
            neg_hot = jnp.where(iota_i == ids_ref[2:3, at_t] - base, 1.0, 0.0)
            d = lax.dot_general(grad_i[:, cut], (pos_hot - neg_hot).astype(BF16), NT, preferred_element_type=F32)
            acc = d if acc is None else acc + d
        return three(acc)

    si_sem = fresh(SIDE)

    def other_seeds(zz, _):
        si[zz] = item_part(1 - col, zz)
        send(si.at[zz], si_in.at[zz], partner, plus(si_sem, zz))
        return 0

    lax.fori_loop(0, SIDE, other_seeds, 0)
    left(si, si_sem)
    arrive(su_in, su_sem)
    for h in range(2):
        v = (su[h] + su_in[h]) * 0.25
        s_user[h] = v
        ut[s0, h] = v.astype(BF16)
    item_product(s0)

    def item_seeds(zz, _):
        seed_i = item_part(col, zz)
        arrive(si_in.at[zz], plus(si_sem, zz))
        seed_i = (seed_i + si_in[zz]) * 0.25
        for part in range(2):
            for q in range(SIDE):
                block = seed_i[block_rows(part, q), block_lanes(q)]
                s_item[zz, part, q] = block
                it[s0, part, zz, y, q] = block.astype(BF16)
        ref = it.at[s0, :, zz, y]
        for k in (1, 3, 2):
            send(ref, ref, peer(1, k), plus(stage_sem[s0]['line'], k))
        return 0

    lax.fori_loop(0, SIDE, item_seeds, 0)
    left(r1.at[s0, 0], stage_sem[s0]['line'])
    arrive(loss_in, l_sem)
    loss_ref[...] = jnp.sum(total + loss_in[0:1], axis=1, keepdims=True) / n_batch

    for s in range(s0, STAGES):
        if s > s0:
            gather_last(s)
        user_own(s)
        scatter_mid(s)
        user_rest(s)
        new = scatter_end(s)
        for p in range(2):
            nxt = s_item[z, p, x] + new[p]
            if s + 1 < STAGES:
                it[s + 1, p, z, y, x] = nxt.astype(BF16)
            else:
                fin_f[p, x] = nxt
        if s + 1 < STAGES:
            gather_plane(s + 1)
        else:
            e_sem = fresh()
            send_axis(2, lambda t: fin_f.at[:, x], lambda k: fin_f.at[:, x], e_sem)
            left(fin_f.at[:, 0:3], e_sem)
        user_there(s)
        if s + 1 < STAGES:
            for h in range(2):
                ut[s + 1, h] = (s_user[h] + (up[s, h] + up_in[s, h])).astype(BF16)
            item_product(s + 1)
        else:
            gu_ref[...] = s_user[col] + (up[s, col] + up_in[s, col])
    arrive(fin_f.at[:, 0:3], e_sem)
    nat_f[...] = join_blocks(lambda part, q: fin_f[part, q]).T
    gi_ref[...] = nat_f[own, :]
    for ref, i in leaving:
        pltpu.make_async_copy(ref, ref, send_sem.at[i]).wait()


def hand_over(*refs):
    for src, dst in zip(refs[:5], refs[5:]):
        dst[...] = src[...]


def solution(mesh):
    def local_fn(mask_blk, user_emb, item_emb, triples):
        n_u, n_b = mask_blk.shape[0], triples.shape[0]
        half = n_u // 2
        vm = pltpu.VMEM
        outs = (jax.ShapeDtypeStruct((EMB, half), BF16), jax.ShapeDtypeStruct((EMB, EMB), BF16),
                jax.ShapeDtypeStruct((1, 1), F32), jax.ShapeDtypeStruct((EMB, half), F32),
                jax.ShapeDtypeStruct((EMB, EMB), F32))
        tile = (16, 128)
        S = SIDE
        scratch = [
            vm((NCHUNK, n_u, CHUNK), jnp.int32), vm((NCHUNK, n_u, CHUNK), BF16),
            vm((n_u, 128), jnp.int32), vm((n_u, 128), jnp.int32), vm((n_u, 128), F32),
            vm((2, 32, 128), jnp.int32), vm((18, 32, 128), jnp.int32), vm((32, 128), F32),
            vm((STAGES, 2, EMB, half), BF16), vm((STAGES, 2, EMB, half), F32), vm((STAGES, 2, EMB, half), F32),
            vm((2, EMB, half), F32), vm((2, EMB, half), F32),
            vm((S, EMB, EMB), BF16), vm((STAGES, 2, S, S, S) + tile, BF16), vm((STAGES, 2, S, S, S) + tile, F32),
            vm((STAGES, 2, S, S) + tile, F32),
            vm((STAGES, 2, S, 3, S) + tile, F32), vm((STAGES, 2, S * S - 1) + tile, F32),
            vm((2,) + tile, F32), vm((S, 2, S) + tile, F32),
            vm((2, S) + tile, BF16), vm((2, S) + tile, F32), vm((CHUNK, EMB), F32),
            vm((2, 3, S, S, 2) + tile, BF16), vm((3, S, S, 2) + tile, BF16), vm((3, S, S, 2) + tile, BF16),
            vm((3, 2) + tile, BF16), vm((3, S * S - 1, 2) + tile, BF16), vm((3, 3, 2) + tile, BF16),
            vm((2, 3, S, S, 2) + tile, BF16),
            vm((3 * EMB, n_b // 2), BF16), vm((3 * EMB, n_b // 2), BF16),
            vm((3 * EMB, n_u), F32), vm((2, EMB, half), F32), vm((2, EMB, half), F32),
            vm((S, EMB, CHUNK), F32), vm((S, EMB, CHUNK), F32), vm((8, 128), F32), vm((8, 128), F32),
            vm((EMB, half), BF16), vm((EMB, EMB), BF16), vm((3, n_b), jnp.int32),
            pltpu.SemaphoreType.DMA((NCHUNK + 3,)), pltpu.SemaphoreType.DMA((NSEM,)), pltpu.SemaphoreType.DMA((NSEM,)),
        ]
        spec = pl.BlockSpec(memory_space=pltpu.VMEM)
        fu, fi, loss, gu, gi = pl.pallas_call(
            kernel,
            out_shape=outs,
            in_specs=[pl.BlockSpec(memory_space=pl.ANY)] * 4,
            out_specs=(spec,) * 5,
            scratch_shapes=scratch,
            compiler_params=pltpu.CompilerParams(collective_id=0, has_side_effects=True, vmem_limit_bytes=56 * 1024 * 1024),
        )(mask_blk, user_emb.T, item_emb, triples.T)
        args = (fu, fi, loss, gu, gi)
        fu, fi, loss, gu, gi = pl.pallas_call(hand_over, out_shape=outs, in_specs=[spec] * 5, out_specs=(spec,) * 5)(*args)
        return fu.T, fi, loss[0, 0], gu.T, gi

    user_spec = P(('row', 'col'), None)
    item_spec = P(('col', 'row'), None)
    return jax.shard_map(local_fn, mesh=mesh, in_specs=(P('row', 'col'), user_spec, item_spec, P()),
                         out_specs=(user_spec, item_spec, P(), user_spec, item_spec), check_vma=False)
```

```python
import jax
import jax.numpy as jnp
from jax import lax
from jax.experimental import pallas as pl
from jax.experimental.pallas import tpu as pltpu
from jax.sharding import PartitionSpec as P

SIDE = 4
STRIDE = (16, 4, 1)
EMB = 64
CHUNK = 256
NCHUNK = 16
LAYERS = 3
STAGES = 2 * LAYERS
F32 = jnp.float32
BF16 = jnp.bfloat16
NSEM = 160
GATHER_ORDER = (1, 3, 2, 4, 5, 7, 6, 12, 13, 15, 14, 8, 9, 11, 10)
PLANE_ORDER = (10, 6, 9, 11, 14, 5, 7, 13, 15, 2, 8, 1, 3, 4, 12)
NT = (((1,), (1,)), ((), ()))
MESH = pl.DeviceIdType.MESH


def block_rows(part, q):
    return slice(32 * part + 16 * (q // 2), 32 * part + 16 * (q // 2) + 16)


def block_lanes(q):
    return slice(128 * (q % 2), 128 * (q % 2) + 128)


def join_blocks(get):
    rows = []
    for part in range(2):
        for half in range(2):
            rows.append(jnp.concatenate([get(part, 2 * half), get(part, 2 * half + 1)], axis=1))
    return jnp.concatenate(rows, axis=0)


def kernel(mask_hbm, user_hbm, item_hbm, ids_hbm,
           fu_ref, fi_ref, loss_ref, gu_ref, gi_ref,
           mask, adj, rowsum, rowsum_in, scale_u, colsum, colsum_in, scale_i,
           ut, up, up_in, u_acc, s_user,
           nat, it, part_sum, q1, r1, r2, i_acc, s_item,
           fin_b, fin_f, nat_f,
           sel, sel_in, w0, w1, in1, in2, rows_all, grad_u, grad_i, prod_u, su, su_in, si, si_in, loss_out, loss_in,
           user_ref, item_ref, ids_ref, mask_sem, send_sem, recv_sem):
    row = lax.axis_index('row')
    col = lax.axis_index('col')
    pos = (lax.div(row, 16), lax.rem(lax.div(row, 4), 4), lax.rem(row, 4))
    step = [[p] + [lax.rem(p + k, SIDE) for k in range(1, SIDE)] for p in pos]
    offset = [[(step[a][k] - pos[a]) * STRIDE[a] if k else 0 for k in range(SIDE)] for a in range(3)]
    z, y, x = pos
    users = user_ref.shape[1]
    n_batch = ids_ref.shape[1]

    def peer(axis, k):
        return {'row': row + offset[axis][k]}

    partner = {'col': 1 - col}

    small = []
    for i, (src, dst) in enumerate(((user_hbm, user_ref), (item_hbm, item_ref), (ids_hbm, ids_ref))):
        cp = pltpu.make_async_copy(src, dst, mask_sem.at[NCHUNK + i])
        cp.start()
        small.append(cp)
    copies = []
    for j in range(NCHUNK):
        cp = pltpu.make_async_copy(mask_hbm.at[:, pl.ds(j * CHUNK, CHUNK)], mask.at[j], mask_sem.at[j])
        cp.start()
        copies.append(cp)

    def plane_peer(axes, k):
        return {'row': row + offset[axes[0]][k // SIDE] + offset[axes[1]][k % SIDE]}

    barrier = pltpu.get_barrier_semaphore()
    for axis in range(3):
        for k in range(1, SIDE):
            pl.semaphore_signal(barrier, inc=1, device_id=peer(axis, k), device_id_type=MESH)
    for axes in ((0, 1), (0, 2), (1, 2)):
        for k in range(SIDE * SIDE):
            if k // SIDE and k % SIDE:
                pl.semaphore_signal(barrier, inc=1, device_id=plane_peer(axes, k), device_id_type=MESH)
    pl.semaphore_signal(barrier, inc=1, device_id=partner, device_id_type=MESH)
    pl.semaphore_wait(barrier, 37)

    count = [0, 0]
    leaving = []

    def fresh(n=1):
        out = (count[0], count[1])
        count[0] += 1
        count[1] += n
        return out

    def send(src, dst, device, sems):
        pltpu.make_async_remote_copy(src_ref=src, dst_ref=dst, send_sem=send_sem.at[sems[0]], recv_sem=recv_sem.at[sems[1]],
                                     device_id=device, device_id_type=MESH).start()

    def left(ref, sems):
        leaving.append((ref, sems[0]))

    def arrive(ref, sems):
        pltpu.make_async_copy(ref, ref, recv_sem.at[sems[1]]).wait()

    def plus(sems, n):
        return (sems[0], sems[1] + n)

    def send_axis(axis, src, dst, sems):
        for k in (1, 3, 2):
            send(src(step[axis][k]), dst(k - 1), peer(axis, k), sems)

    def send_plane(axes, src, dst, sems):
        for k in PLANE_ORDER:
            send(src(step[axes[0]][k // SIDE], step[axes[1]][k % SIDE]), dst(k - 1), plane_peer(axes, k), sems)

    for cp in small:
        cp.wait()
    ut[0, col] = user_ref[...]
    u_sem = fresh()
    send(ut.at[0, col], ut.at[0, col], partner, u_sem)
    left(ut.at[0, 0], u_sem)
    nat[x] = item_ref[...]
    n_sem = fresh()
    send_axis(2, lambda t: nat.at[x], lambda k: nat.at[x], n_sem)
    left(nat.at[0:3], n_sem)

    rowsum[...] = jnp.zeros_like(rowsum)
    for j in range(NCHUNK):
        copies[j].wait()
        m = mask[j]
        adj[j] = m.astype(F32).astype(BF16)
        rowsum[...] += m[:, :128] + m[:, 128:]
        s = jnp.sum(m, axis=0, keepdims=True)
        colsum[0, 2 * j:2 * j + 1, :] = s[:, :128]
        colsum[0, 2 * j + 1:2 * j + 2, :] = s[:, 128:]
    r_sem = fresh()
    parts = ((slice(0, 16), 0, (1, 2)), (slice(16, 24), 2, (1, 0)), (slice(24, 32), 1, (0, 2)))
    c_sem = [fresh() for _ in parts]
    send(rowsum, rowsum_in, partner, r_sem)
    left(rowsum, r_sem)
    for (rows, axis, _), sems in zip(parts, c_sem):
        send_axis(axis, lambda t: colsum.at[0, rows], lambda k: colsum_in.at[k, rows], sems)
        left(colsum_in.at[0:3, rows], sems)

    arrive(nat.at[0:3], n_sem)
    chunk0 = jnp.concatenate([nat[k].astype(F32) for k in range(SIDE)], axis=0).T
    for part in range(2):
        for q in range(SIDE):
            it[0, part, z, y, q] = chunk0[block_rows(part, q), block_lanes(q)].astype(BF16)

    stage_sem = [dict(user=fresh(), plane=fresh(SIDE), line=fresh(SIDE), axis=[fresh(SIDE), fresh(SIDE)],
                      last=[fresh(), fresh()]) for _ in range(STAGES)]

    def gather_plane(s):
        sems = stage_sem[s]['plane']
        ref = it.at[s, :, z, y, x]
        for k in GATHER_ORDER:
            send(ref, ref, plane_peer((0, 2), k), plus(sems, k // SIDE))
        left(r2.at[s, 0], sems)

    def gather_line(s):
        sems = stage_sem[s]['plane']
        ref = it.at[s, :, z, y]
        for k in (1, 3, 2):
            send(ref, ref, peer(0, k), plus(sems, k))
        left(it.at[s, :, 0:3, 0], sems)

    def gather_last(s, line=False):
        sems = stage_sem[s]
        for kz in (0, 1, 3, 2):
            ref = it.at[s, :, step[0][(SIDE - kz) % SIDE], y]
            if kz:
                arrive(ref, plus(sems['plane'], kz))
            elif not line:
                arrive(ref.at[:, 0:3], sems['plane'])
            for k in (1, 3, 2):
                send(ref, ref, peer(1, k), plus(sems['line'], k))
        left(r1.at[s, 0], sems['line'])

    gather_line(0)
    arrive(rowsum_in, r_sem)
    deg_u = jnp.maximum(jnp.sum(rowsum[...] + rowsum_in[...], axis=1, keepdims=True), 1)
    scale_u[...] = jnp.broadcast_to(lax.rsqrt(deg_u.astype(F32)), scale_u.shape)
    d_sem = [fresh() for _ in parts]
    for (rows, _, axes), sems, sems2 in zip(parts, c_sem, d_sem):
        arrive(colsum_in.at[0:3, rows], sems)
        colsum[1, rows] = colsum[0, rows] + colsum_in[0, rows] + colsum_in[1, rows] + colsum_in[2, rows]
        send_plane(axes, lambda t0, t1: colsum.at[1, rows], lambda k: colsum_in.at[3 + k, rows], sems2)
        left(colsum_in.at[3:18, rows], sems2)
    gather_last(0, line=True)
    for (rows, _, _), sems in zip(parts, d_sem):
        arrive(colsum_in.at[3:18, rows], sems)
    deg_i = jnp.maximum(colsum[1] + jnp.sum(colsum_in[3:], axis=0), 1)
    scale_i[...] = lax.rsqrt(deg_i.astype(F32))
    for j in range(NCHUNK):
        rowscale = scale_u[...]
        for l in range(2):
            lanes = slice(128 * l, 128 * l + 128)
            adj[j, :, lanes] = (rowscale * scale_i[2 * j + l:2 * j + l + 1, :]).astype(BF16) * adj[j, :, lanes]

    def at(ref, axis, t):
        return ref.at[(slice(None),) * axis + (t,)]

    def item_product(s):
        lhs = jnp.concatenate([ut[s, 0], ut[s, 1]], axis=1)

        def body(i, _):
            ky = lax.rem(i + 1, SIDE)
            yy = lax.rem(y + ky, SIDE)
            for kz in (2, 1, 3, 0):
                zz = step[0][kz]
                out = jnp.dot(lhs, adj[zz * SIDE + yy], preferred_element_type=F32)
                for part in range(2):
                    for q in range(SIDE):
                        part_sum[s, part, zz, yy, q] = out[block_rows(part, q), block_lanes(q)]
            scatter_send(s, ky, yy)
            return 0

        lax.fori_loop(0, SIDE, body, 0)
        for p in range(2):
            left(r1.at[s, p], stage_sem[s]['axis'][p])

    def scatter_send(s, ky, yy):
        sems = stage_sem[s]['axis']
        send_axis(0, lambda t: part_sum.at[s, 0, t, yy], lambda k: r1.at[s, 0, ky, k], plus(sems[0], ky))
        send_axis(2, lambda t: part_sum.at[s, 1, :, yy, t], lambda k: r1.at[s, 1, ky, k], plus(sems[1], ky))

    def scatter_mid(s, between=None):
        sems = stage_sem[s]

        def piece(ky, yy, off, ks):
            for p in range(2):
                axis = (2, 0)[p]
                arrive(r1.at[s, p, ky], plus(sems['axis'][p], ky))
                own = part_sum[s, 0, z, yy] if p == 0 else part_sum[s, 1, :, yy, x]
                q1[s, p, ky] = own + jnp.sum(r1[s, p, ky], axis=0)
                for k in ks:
                    send(q1.at[s, p, ky, step[axis][k]], r2.at[s, p, 4 * ky + k - 1], {'row': row + off + offset[axis][k]},
                         sems['last'][p])

        def body(ky, _):
            yy = lax.rem(y + ky, SIDE)
            piece(ky, yy, (yy - y) * STRIDE[1], (2, 1, 3, 0))
            return 0

        lax.fori_loop(1, SIDE, body, 0)
        if between:
            between()
        piece(0, y, 0, (2, 1, 3))
        for p in range(2):
            left(r2.at[s, p], sems['last'][p])

    def scatter_end(s):
        out = []
        for p in range(2):
            arrive(r2.at[s, p], stage_sem[s]['last'][p])
            out.append(q1[s, p, 0, pos[(2, 0)[p]]] + jnp.sum(r2[s, p], axis=0))
        return out

    def user_group(s, yy, first):
        acc = None
        for zz in range(SIDE):
            lhs = join_blocks(lambda part, q: it[s, part, zz, yy, q])
            d = lax.dot_general(lhs, adj[zz * SIDE + yy], NT, preferred_element_type=F32)
            acc = d if acc is None else acc + d
        for h in range(2):
            v = acc[:, h * users:(h + 1) * users]
            up[s, h] = v if first else up[s, h] + v

    def user_own(s):
        user_group(s, y, True)

    def user_rest(s):
        def body(i, _):
            k = 1 + lax.rem(2 * i, 3)
            yy = lax.rem(y + SIDE - k, SIDE)
            arrive(it.at[s, :, :, yy], plus(stage_sem[s]['line'], k))
            user_group(s, yy, False)
            return 0

        lax.fori_loop(0, SIDE - 1, body, 0)
        sems = stage_sem[s]['user']
        send(up.at[s], up_in.at[s], partner, sems)
        left(up.at[s], sems)

    def user_there(s):
        arrive(up_in.at[s], stage_sem[s]['user'])

    for p in range(2):
        i_acc[p] = it[0, p, z, y, x].astype(F32)
    arrive(ut.at[0, 1 - col], u_sem)
    for h in range(2):
        u_acc[h] = ut[0, h].astype(F32)

    def user_next(s):
        for h in range(2):
            nxt = (up[s, h] + up_in[s, h]).astype(BF16)
            u_acc[h] += nxt.astype(F32)
            if s + 1 < LAYERS:
                ut[s + 1, h] = nxt

    item_product(0)
    user_own(0)
    user_rest(0)
    scatter_mid(0)
    user_there(0)
    user_next(0)
    item_product(1)

    def item_next(s):
        new = scatter_end(s)
        for p in range(2):
            nxt = new[p].astype(BF16)
            i_acc[p] += nxt.astype(F32)
            if s + 1 < LAYERS:
                it[s + 1, p, z, y, x] = nxt
        if s + 1 < LAYERS:
            gather_plane(s + 1)

    item_next(0)
    scatter_mid(1, lambda: gather_last(1))
    user_own(1)
    item_next(1)
    user_rest(1)
    user_there(1)
    user_next(1)
    item_product(2)
    gather_last(2)
    user_own(2)
    scatter_mid(2)
    user_rest(2)
    user_there(2)
    user_next(2)

    tiles = n_batch // CHUNK
    iota = lax.broadcasted_iota(jnp.int32, (users, CHUNK), 0)
    for h in range(2):
        ut[LAYERS, h] = (u_acc[h] * 0.25).astype(BF16)
    own_u = ut[LAYERS, col]
    fu_ref[...] = own_u

    def put_rows(rt, t, picked):
        for l in range(2):
            lt = 2 * t + l
            sel[lt // 8, rt % 3, lt % 4, rt // 3, (lt % 8) // 4] = picked[:, 128 * l:128 * l + 128].astype(BF16)

    base_u = (2 * row + col) * users
    for t in range(tiles):
        ids = ids_ref[0:1, t * CHUNK:(t + 1) * CHUNK]
        hot = jnp.where(iota == ids - base_u, 1.0, 0.0).astype(BF16)
        picked = jnp.dot(own_u, hot, preferred_element_type=F32)
        for r in range(4):
            put_rows(r, t, picked[16 * r:16 * r + 16])
    item_next(2)
    for p in range(2):
        fin_b[p, x] = (i_acc[p] * 0.25).astype(BF16)
    f_sem = fresh()
    send_axis(2, lambda t: fin_b.at[:, x], lambda k: fin_b.at[:, x], f_sem)
    left(fin_b.at[:, 0:3], f_sem)
    base_i = (col * NCHUNK + z * SIDE + y) * CHUNK
    iota_i = lax.broadcasted_iota(jnp.int32, (CHUNK, CHUNK), 0)
    iota_b = lax.broadcasted_iota(jnp.int32, (128, CHUNK), 0)
    x_half, x_side = lax.div(x, 2), lax.rem(x, 2)
    base_b = base_i + 128 * x_side
    own_i = jnp.concatenate([fin_b[0, x], fin_b[1, x]], axis=0)
    for g in range(1, 3):
        for t in range(tiles):
            hot = jnp.where(iota_b == ids_ref[g:g + 1, t * CHUNK:(t + 1) * CHUNK] - base_b, 1.0, 0.0).astype(BF16)
            picked = jnp.dot(own_i, hot, preferred_element_type=F32)
            for part in range(2):
                rows = picked[16 * part:16 * part + 16]
                for half in range(2):
                    put_rows(4 * g + 2 * part + half, t, jnp.where(x_half == half, rows, 0.0))

    x_sem = fresh()
    send(sel.at[1 - col], sel_in, partner, x_sem)
    left(sel_in, x_sem)
    arrive(sel_in, x_sem)
    w0[...] = sel[col] + sel_in[...]
    planes, third = ((0, 1), (2, 1), (0, 2)), (2, 0, 1)
    sems = [fresh() for _ in range(3)]
    for p in range(3):
        send_plane(planes[p], lambda t0, t1: w0.at[p, t0, t1], lambda k: in1.at[p, k], sems[p])
        left(in1.at[p], sems[p])
    arrive(fin_b.at[:, 0:3], f_sem)
    nat_f[...] = join_blocks(lambda part, q: fin_b[part, q]).astype(F32).T
    own = pl.ds(pl.multiple_of(x * EMB, EMB), EMB)
    fi_ref[...] = nat_f[own, :].astype(BF16)
    sems2 = [fresh() for _ in range(3)]
    for p in range(3):
        arrive(in1.at[p], sems[p])
        mine = w0[p, pos[planes[p][0]], pos[planes[p][1]]].astype(F32)
        w1[p] = (mine + jnp.sum(in1[p].astype(F32), axis=0)).astype(BF16)
        send_axis(third[p], lambda t: w1.at[p], lambda k: in2.at[p, k], sems2[p])
        left(in2.at[p], sems2[p])
    sems3 = [fresh() for _ in range(3)]
    for p in range(3):
        arrive(in2.at[p], sems2[p])
        ref = rows_all.at[col, p, pos[planes[p][0]], pos[planes[p][1]]]
        ref[...] = w1[p] + in2[p, 0] + in2[p, 1] + in2[p, 2]
        send_plane(planes[p], lambda t0, t1: ref, lambda k: ref, sems3[p])
        left(in1.at[p], sems3[p])
    for p in range(3):
        arrive(in1.at[p], sems3[p])
    total = jnp.zeros((1, 128), F32)
    for lt in range(n_batch // 256):
        def rows_of(group):
            return jnp.concatenate([rows_all[col, rt % 3, lt % 4, rt // 3, lt // 4].astype(F32)
                                    for rt in range(4 * group, 4 * group + 4)], axis=0)
        e_user, e_pos, e_neg = rows_of(0), rows_of(1), rows_of(2)
        margin = jnp.sum(e_user * e_pos, axis=0, keepdims=True) - jnp.sum(e_user * e_neg, axis=0, keepdims=True)
        soft = jnp.maximum(-margin, 0.0) + jnp.log1p(jnp.exp(-jnp.abs(margin)))
        total = total + soft
        coef = -jax.nn.sigmoid(-margin) / n_batch
        lanes = slice(lt * 128, lt * 128 + 128)
        for ref, g in ((grad_u, coef * (e_pos - e_neg)), (grad_i, coef * e_user)):
            hi = g.astype(BF16)
            low = g - hi.astype(F32)
            mid = low.astype(BF16)
            ref[0:EMB, lanes] = hi
            ref[EMB:2 * EMB, lanes] = mid
            ref[2 * EMB:3 * EMB, lanes] = (low - mid.astype(F32)).astype(BF16)
    loss_out[...] = jnp.broadcast_to(total, loss_out.shape)
    l_sem = fresh()
    send(loss_out, loss_in, partner, l_sem)
    left(loss_out, l_sem)

    iota2 = lax.broadcasted_iota(jnp.int32, (2 * users, CHUNK), 0)
    s0 = LAYERS
    own_half = pl.multiple_of(col * (n_batch // 2), 128)

    def three(v):
        return v[0:EMB] + v[EMB:2 * EMB] + v[2 * EMB:3 * EMB]

    prod_u[...] = jnp.zeros_like(prod_u)
    for t in range(tiles // 2):
        cut = slice(t * CHUNK, (t + 1) * CHUNK)
        ids = ids_ref[0:1, pl.ds(own_half + t * CHUNK, CHUNK)]
        hot = jnp.where(iota2 == ids - row * (2 * users), 1.0, 0.0).astype(BF16)
        prod_u[...] += lax.dot_general(grad_u[:, cut], hot, NT, preferred_element_type=F32)
    seed = three(prod_u[...])
    for h in range(2):
        su[h] = seed[:, h * users:(h + 1) * users]
    su_sem = fresh()
    send(su, su_in, partner, su_sem)
    left(su, su_sem)

    def item_part(side, zz):
        base = (side * NCHUNK + zz * SIDE + y) * CHUNK
        acc = None
        for t in range(tiles // 2):
            cut = slice(t * CHUNK, (t + 1) * CHUNK)
            at_t = pl.ds(own_half + t * CHUNK, CHUNK)
            pos_hot = jnp.where(iota_i == ids_ref[1:2, at_t] - base, 1.0, 0.0)
            neg_hot = jnp.where(iota_i == ids_ref[2:3, at_t] - base, 1.0, 0.0)
            d = lax.dot_general(grad_i[:, cut], (pos_hot - neg_hot).astype(BF16), NT, preferred_element_type=F32)
            acc = d if acc is None else acc + d
        return three(acc)

    si_sem = fresh(SIDE)

    def other_seeds(zz, _):
        si[zz] = item_part(1 - col, zz)
        send(si.at[zz], si_in.at[zz], partner, plus(si_sem, zz))
        return 0

    lax.fori_loop(0, SIDE, other_seeds, 0)
    left(si, si_sem)
    arrive(su_in, su_sem)
    for h in range(2):
        v = (su[h] + su_in[h]) * 0.25
        s_user[h] = v
        ut[s0, h] = v.astype(BF16)
    item_product(s0)

    def item_seeds(zz, _):
        seed_i = item_part(col, zz)
        arrive(si_in.at[zz], plus(si_sem, zz))
        seed_i = (seed_i + si_in[zz]) * 0.25
        for part in range(2):
            for q in range(SIDE):
                block = seed_i[block_rows(part, q), block_lanes(q)]
                s_item[zz, part, q] = block
                it[s0, part, zz, y, q] = block.astype(BF16)
        ref = it.at[s0, :, zz, y]
        for k in (1, 3, 2):
            send(ref, ref, peer(1, k), plus(stage_sem[s0]['line'], k))
        return 0

    lax.fori_loop(0, SIDE, item_seeds, 0)
    left(r1.at[s0, 0], stage_sem[s0]['line'])
    arrive(loss_in, l_sem)
    loss_ref[...] = jnp.sum(total + loss_in[0:1], axis=1, keepdims=True) / n_batch

    for s in range(s0, STAGES):
        if s > s0:
            gather_last(s)
        user_own(s)
        scatter_mid(s)
        user_rest(s)
        new = scatter_end(s)
        for p in range(2):
            nxt = s_item[z, p, x] + new[p]
            if s + 1 < STAGES:
                it[s + 1, p, z, y, x] = nxt.astype(BF16)
            else:
                fin_f[p, x] = nxt
        if s + 1 < STAGES:
            gather_plane(s + 1)
        else:
            e_sem = fresh()
            send_axis(2, lambda t: fin_f.at[:, x], lambda k: fin_f.at[:, x], e_sem)
            left(fin_f.at[:, 0:3], e_sem)
        user_there(s)
        if s + 1 < STAGES:
            for h in range(2):
                ut[s + 1, h] = (s_user[h] + (up[s, h] + up_in[s, h])).astype(BF16)
            item_product(s + 1)
        else:
            gu_ref[...] = s_user[col] + (up[s, col] + up_in[s, col])
    arrive(fin_f.at[:, 0:3], e_sem)
    nat_f[...] = join_blocks(lambda part, q: fin_f[part, q]).T
    gi_ref[...] = nat_f[own, :]
    for ref, i in leaving:
        pltpu.make_async_copy(ref, ref, send_sem.at[i]).wait()


def hand_over(*refs):
    for src, dst in zip(refs[:5], refs[5:]):
        dst[...] = src[...]


def solution(mesh):
    def local_fn(mask_blk, user_emb, item_emb, triples):
        n_u, n_b = mask_blk.shape[0], triples.shape[0]
        half = n_u // 2
        vm = pltpu.VMEM
        outs = (jax.ShapeDtypeStruct((EMB, half), BF16), jax.ShapeDtypeStruct((EMB, EMB), BF16),
                jax.ShapeDtypeStruct((1, 1), F32), jax.ShapeDtypeStruct((EMB, half), F32),
                jax.ShapeDtypeStruct((EMB, EMB), F32))
        tile = (16, 128)
        S = SIDE
        scratch = [
            vm((NCHUNK, n_u, CHUNK), jnp.int32), vm((NCHUNK, n_u, CHUNK), BF16),
            vm((n_u, 128), jnp.int32), vm((n_u, 128), jnp.int32), vm((n_u, 128), F32),
            vm((2, 32, 128), jnp.int32), vm((18, 32, 128), jnp.int32), vm((32, 128), F32),
            vm((STAGES, 2, EMB, half), BF16), vm((STAGES, 2, EMB, half), F32), vm((STAGES, 2, EMB, half), F32),
            vm((2, EMB, half), F32), vm((2, EMB, half), F32),
            vm((S, EMB, EMB), BF16), vm((STAGES, 2, S, S, S) + tile, BF16), vm((STAGES, 2, S, S, S) + tile, F32),
            vm((STAGES, 2, S, S) + tile, F32),
            vm((STAGES, 2, S, 3, S) + tile, F32), vm((STAGES, 2, S * S - 1) + tile, F32),
            vm((2,) + tile, F32), vm((S, 2, S) + tile, F32),
            vm((2, S) + tile, BF16), vm((2, S) + tile, F32), vm((CHUNK, EMB), F32),
            vm((2, 3, S, S, 2) + tile, BF16), vm((3, S, S, 2) + tile, BF16), vm((3, S, S, 2) + tile, BF16),
            vm((3, 2) + tile, BF16), vm((3, S * S - 1, 2) + tile, BF16), vm((3, 3, 2) + tile, BF16),
            vm((2, 3, S, S, 2) + tile, BF16),
            vm((3 * EMB, n_b // 2), BF16), vm((3 * EMB, n_b // 2), BF16),
            vm((3 * EMB, n_u), F32), vm((2, EMB, half), F32), vm((2, EMB, half), F32),
            vm((S, EMB, CHUNK), F32), vm((S, EMB, CHUNK), F32), vm((8, 128), F32), vm((8, 128), F32),
            vm((EMB, half), BF16), vm((EMB, EMB), BF16), vm((3, n_b), jnp.int32),
            pltpu.SemaphoreType.DMA((NCHUNK + 3,)), pltpu.SemaphoreType.DMA((NSEM,)), pltpu.SemaphoreType.DMA((NSEM,)),
        ]
        spec = pl.BlockSpec(memory_space=pltpu.VMEM)
        fu, fi, loss, gu, gi = pl.pallas_call(
            kernel,
            out_shape=outs,
            in_specs=[pl.BlockSpec(memory_space=pl.ANY)] * 4,
            out_specs=(spec,) * 5,
            scratch_shapes=scratch,
            compiler_params=pltpu.CompilerParams(collective_id=0, has_side_effects=True, vmem_limit_bytes=56 * 1024 * 1024),
        )(mask_blk, user_emb.T, item_emb, triples.T)
        args = (fu, fi, loss, gu, gi)
        fu, fi, loss, gu, gi = pl.pallas_call(hand_over, out_shape=outs, in_specs=[spec] * 5, out_specs=(spec,) * 5)(*args)
        return fu.T, fi, loss[0, 0], gu.T, gi

    user_spec = P(('row', 'col'), None)
    item_spec = P(('col', 'row'), None)
    return jax.shard_map(local_fn, mesh=mesh, in_specs=(P('row', 'col'), user_spec, item_spec, P()),
                         out_specs=(user_spec, item_spec, P(), user_spec, item_spec), check_vma=False)
```
